32 devices in a mesh: tm: 4 (over y, x), space: 8 (over z, core).
Axes of the slice: x: 2, y: 2, z: 4, core: 2. Of those that a mesh axis runs over, the one named last changes fastest.
Arguments:
- source: float32 [32, 512, 1024], P('tm', 'space'), may hold values from -6 to 6
- guess: float32 [32, 512, 1024], P('tm', 'space'), may hold values from -6 to 6
- start_state: float32 [512, 1024], P('space'), may hold values from -6 to 6
- conduct: float32 [512, 1024], P('space'), may hold values from 0.5 to 4
Outputs:
- solution_field: float32 [32, 512, 1024], P('tm', 'space')
- residual: float32 [32, 512, 1024], P('tm', 'space')
The draws below stay inside these ranges and needn't reach their ends.
All inputs are finite; a program needn't handle non-finite values.
Results may differ from the reference program's by a relative error of at most 0.00002.
Values sent between devices are 32-bit elements; how exact they have to be, the bound alone decides.
A program may use at most 64 MiB of HBM per device.

```python
import math
import jax
import jax.numpy as jnp

COLS = 1024
NT = 32
NR = 512


def levels(rng, extent, cuts, smallest, high):
    loudness = 1.0
    for position, blocks in cuts:
        heights = jax.random.uniform(jax.random.fold_in(jax.random.fold_in(rng, 6), position), (blocks,), jnp.float32, smallest / len(cuts), high / len(cuts))
        loudness = loudness * jnp.repeat(jnp.exp(heights), extent[position] // blocks).reshape((-1,) + (1,) * (len(extent) - 1 - position))
    return loudness


def normal_values(rng, extent, width, reach, pieces=(), kind=jnp.bfloat16):
    entries = width * jax.random.normal(rng, extent, jnp.float32)
    if pieces:
        entries = entries * levels(rng, extent, pieces, -0.22, 0.18)
    return jnp.clip(entries, -reach, reach).astype(kind)


def setup_inputs(seed: int = 0) -> dict:
    key_list = jax.random.split(jax.random.key(seed), 5)
    source = normal_values(key_list[0], (NT, NR, COLS), 1.0, 6.0, ((0, 4), (1, 8)), jnp.float32)
    guess = normal_values(key_list[1], (NT, NR, COLS), 1.0, 6.0, ((0, 4), (1, 8)), jnp.float32)
    start_state = normal_values(key_list[2], (NR, COLS), 1.0, 6.0, ((0, 8),), jnp.float32)
    conduct = jnp.clip(jnp.exp(math.log(4.0) - 2.0794415 * jax.random.uniform(key_list[3], (NR, COLS), jnp.float32) ** levels(key_list[3], (NR, COLS), ((0, 8),), -0.2, 0.2)), 0.5, 4.0)
    return dict(source=source, guess=guess, start_state=start_state, conduct=conduct)


damping = 0.8


def apply_operator(field, conduct):
    padded = jnp.pad(field, ((0, 0), (1, 1), (1, 1)))
    beside = padded[:, 2:, 1:-1] + padded[:, :-2, 1:-1] + padded[:, 1:-1, 2:] + padded[:, 1:-1, :-2]
    return field + conduct * (4.0 * field - beside)


def approx_inverse(resid, conduct):
    diagonal = 1.0 + 4.0 * conduct
    first_sweep = resid / diagonal
    return first_sweep + (resid - apply_operator(first_sweep, conduct)) / diagonal


def fine_residual(field, before, source, conduct):
    earlier = jnp.concatenate([before[None], field[:-1]], axis=0)
    return source + earlier - apply_operator(field, conduct)


def shifted(coarse):
    return jnp.concatenate([jnp.zeros_like(coarse[:1]), coarse[:-1]], axis=0)


def reference(source, guess, start_state, conduct):
    resid0 = fine_residual(guess, start_state, source, conduct)
    smooth1 = guess + damping * approx_inverse(resid0, conduct)
    resid1 = fine_residual(smooth1, start_state, source, conduct)
    half_steps = source.shape[0] // 2
    pairs = resid1.reshape(half_steps, 2, source.shape[1], source.shape[2])
    restricted = pairs[:, 0] + pairs[:, 1]
    coarse_cond = 2.0 * conduct
    correction = damping * approx_inverse(restricted, coarse_cond)
    for sweep in range(2):
        defect = restricted + shifted(correction) - apply_operator(correction, coarse_cond)
        correction = correction + damping * approx_inverse(defect, coarse_cond)
    even_steps = 0.5 * (shifted(correction) + correction)
    fine_corr = jnp.stack([even_steps, correction], axis=1).reshape(source.shape)
    smooth2 = smooth1 + fine_corr
    resid2 = fine_residual(smooth2, start_state, source, conduct)
    smooth3 = smooth2 + damping * approx_inverse(resid2, conduct)
    resid3 = fine_residual(smooth3, start_state, source, conduct)
    return smooth3, resid3
```

```python
import functools

import jax
import jax.numpy as jnp
from jax import lax
from jax.experimental import pallas as pl
from jax.experimental.pallas import tpu as pltpu
from jax.sharding import PartitionSpec as P

damping = 0.8
MESH = pl.DeviceIdType.MESH
HALO = 8
LANES = 128

COND, F_GUESS, F_Q, F_E0, F_E1, F_E2, X_LATE, X_MID, X_EARLY = range(0, 18, 2)
T_GUESS, T_Q, T_E0, T_E1, T_E2, T_U3 = range(18, 24)
STEPS = 24


def kernel(
    tms, spaces, src_hbm, guess_hbm, start_hbm, cond_hbm, u3, rbuf,
    g, s, c, d, w, dk, wk, e, u1, er, ec, c0, c1, c2, u2, qbuf, fu,
    send_sem, recv_sem, load_sem,
):
    t = lax.axis_index("tm")
    z = lax.axis_index("space")
    has_up, has_dn = z > 0, z < spaces - 1
    has_before, has_after = t > 0, t < tms - 1
    steps, rows, cols = src_hbm.shape
    half = steps // 2
    full = rows + 2 * HALO
    mid = slice(HALO, HALO + rows)
    top, bot = slice(0, HALO), slice(HALO + rows, full)
    top_in, bot_in = slice(HALO, 2 * HALO), slice(rows, HALO + rows)
    chunks = cols // LANES
    later = slice(1, steps + 1)

    def remote(src, dst, k, dev):
        return pltpu.make_async_remote_copy(
            src_ref=src, dst_ref=dst, send_sem=send_sem.at[k], recv_sem=recv_sem.at[k],
            device_id=dev, device_id_type=MESH)

    up, dn = {"space": z - 1}, {"space": z + 1}
    sent = []

    class Edge:
        def __init__(self, k, first, last, halo_top, halo_bot):
            self.k, self.first, self.last, self.top, self.bot = k, first, last, halo_top, halo_bot

        def start(self):
            @pl.when(has_up)
            def _():
                remote(self.first, self.bot, self.k, up).start()

            @pl.when(has_dn)
            def _():
                remote(self.last, self.top, self.k + 1, dn).start()
            sent.append(self)

        def wait_recv(self):
            @pl.when(has_dn)
            def _():
                remote(self.first, self.bot, self.k, dn).wait_recv()

            @pl.when(has_up)
            def _():
                remote(self.last, self.top, self.k + 1, up).wait_recv()

        def wait_send(self):
            @pl.when(has_up)
            def _():
                remote(self.first, self.bot, self.k, up).wait_send()

            @pl.when(has_dn)
            def _():
                remote(self.last, self.top, self.k + 1, dn).wait_send()

    class Along:
        def __init__(self, k, src, dst):
            self.k, self.src, self.dst = k, src, dst

        def start(self):
            @pl.when(has_after)
            def _():
                remote(self.src, self.dst, self.k, {"tm": t + 1}).start()
            if self not in sent:
                sent.append(self)

        def wait_recv(self):
            @pl.when(has_before)
            def _():
                remote(self.src, self.dst, self.k, {"tm": t - 1}).wait_recv()

        def wait_send(self):
            @pl.when(has_after)
            def _():
                remote(self.src, self.dst, self.k, {"tm": t + 1}).wait_send()

    def within(k, ref, sl):
        return Edge(k, ref.at[sl, top_in], ref.at[sl, bot_in], ref.at[sl, top], ref.at[sl, bot])

    barrier = pltpu.get_barrier_semaphore()
    for flag, dev in ((has_up, up), (has_dn, dn), (has_before, {"tm": t - 1}), (has_after, {"tm": t + 1})):
        @pl.when(flag)
        def _(dev=dev):
            pl.semaphore_signal(barrier, inc=1, device_id=dev, device_id_type=MESH)

    loads = [
        pltpu.make_async_copy(cond_hbm, c.at[mid], load_sem.at[0]),
        pltpu.make_async_copy(guess_hbm, g.at[later, mid], load_sem.at[1]),
        pltpu.make_async_copy(src_hbm, s.at[later, mid], load_sem.at[2]),
    ]
    for load in loads:
        load.start()
    start_g = pltpu.make_async_copy(start_hbm, g.at[0, mid], load_sem.at[3])
    start_u = pltpu.make_async_copy(start_hbm, fu, load_sem.at[4])

    @pl.when(jnp.logical_not(has_before))
    def _():
        start_g.start()
        start_u.start()
        s[0, mid] = jnp.zeros((rows, cols), jnp.float32)
        for ref in (c0, c1, c2):
            ref[0, mid] = jnp.zeros((rows, cols), jnp.float32)

    for flag, edge in ((has_up, top), (has_dn, bot)):
        @pl.when(jnp.logical_not(flag))
        def _(edge=edge):
            c[edge] = jnp.zeros((HALO, cols), jnp.float32)
            for ref in (g, s, c0, c1, c2):
                if ref is g or ref is s or ref is c2:
                    ref[:, edge] = jnp.zeros((ref.shape[0], HALO, cols), jnp.float32)
                else:
                    ref[0, edge] = jnp.zeros((HALO, cols), jnp.float32)

    peers = sum(jnp.where(flag, 1, 0) for flag in (has_up, has_dn, has_before, has_after))
    pl.semaphore_wait(barrier, peers)

    along = Along(T_GUESS, guess_hbm.at[steps - 1], g.at[0, mid])
    along.start()
    a_guess = along
    x_cond = Edge(COND, cond_hbm.at[0:HALO], cond_hbm.at[rows - HALO : rows], c.at[top], c.at[bot])
    def halo(n, hbm, ref, k):
        return Edge(k, hbm.at[n - 1, 0:HALO], hbm.at[n - 1, rows - HALO : rows], ref.at[n, top], ref.at[n, bot])

    def guess_halo(n):
        return halo(n, guess_hbm, g, STEPS + 2 * (n - 1))

    def source_halo(n):
        return halo(n, src_hbm, s, STEPS + 2 * steps + 2 * (n - 1))

    x_cond.start()
    guess_halo(steps).start()
    for n in range(steps - 1, 0, -1):
        guess_halo(n).start()
        source_halo(n + 1).start()
    source_halo(1).start()
    for load in loads:
        load.wait()

    lane = lax.broadcasted_iota(jnp.int32, (full, LANES), 1)
    is_first, is_last = lane == 0, lane == LANES - 1

    def at(j):
        return slice(j * LANES, (j + 1) * LANES)

    def each(low, high, body):
        def step(i, carry):
            body(i)
            return carry
        lax.fori_loop(low, high, step, 0)

    def stencil(get, put):
        zero = jnp.zeros((full, LANES), jnp.float32)
        before, now = zero, get(0)
        for j in range(chunks):
            after = get(j + 1) if j + 1 < chunks else zero
            left = pltpu.roll(jnp.where(is_last, before, now), 1, 1)
            right = pltpu.roll(jnp.where(is_first, after, now), LANES - 1, 1)
            rim = (left + right) + (pltpu.roll(now, 1, 0) + pltpu.roll(now, full - 1, 0))
            put(j, now, rim)
            before, now = now, after

    def first_sweep(field, n, has_prev=True):
        def put(j, now, rim):
            drive = s[n, :, at(j)]
            if has_prev:
                drive = drive + field[n - 1, :, at(j)]
            e[n, :, at(j)] = d[:, at(j)] * drive + w[:, at(j)] * rim - now
        stencil(lambda j: field[n, :, at(j)], put)

    def second_sweep(field, errs, n, dst, weight, damp, inner=False):
        def put(j, now, rim):
            gain = damp * (now + weight[:, at(j)] * rim)
            if inner:
                dst[n, mid, at(j)] = field[n, mid, at(j)] + gain[mid]
            elif field is None:
                dst[n, :, at(j)] = gain
            else:
                dst[n, :, at(j)] = field[n, :, at(j)] + gain
        stencil(lambda j: errs[n, :, at(j)], put)

    def restrict(m):
        a, b = 2 * m - 1, 2 * m

        def put(j, now, rim):
            cc = c[:, at(j)]
            drive = (s[a, :, at(j)] + s[b, :, at(j)]) + (u1[a - 1, :, at(j)] + u1[a, :, at(j)])
            er[m, :, at(j)] = dk[:, at(j)] * (drive - now + cc * (rim - 4.0 * now))
        stencil(lambda j: u1[a, :, at(j)] + u1[b, :, at(j)], put)

    def coarse_defect(field, m):
        def put(j, now, rim):
            ec[m, :, at(j)] = er[m, :, at(j)] + dk[:, at(j)] * field[m - 1, :, at(j)] + wk[:, at(j)] * rim - now
        stencil(lambda j: field[m, :, at(j)], put)

    def sweep_one(low, high):
        each(low, high, lambda m: coarse_defect(c0, m))
        each(low, high, lambda m: second_sweep(c0, ec, m, c1, wk, damping))

    def sweep_two(low, high):
        each(low, high, lambda m: coarse_defect(c1, m))
        each(low, high, lambda m: second_sweep(c1, ec, m, c2, wk, damping, inner=True))

    def prolong(m):
        for j in range(chunks):
            u2[2 * m, :, at(j)] = u1[2 * m, :, at(j)] + c2[m, :, at(j)]
            u2[2 * m - 1, :, at(j)] = u1[2 * m - 1, :, at(j)] + 0.5 * (c2[m - 1, :, at(j)] + c2[m, :, at(j)])

    def last_residual(n, has_prev=True):
        def put(j, now, rim):
            flow = c[:, at(j)] * (rim - 4.0 * now) - now
            drive = s[n, mid, at(j)]
            if has_prev:
                drive = drive + u3[n - 1, mid, at(j)]
            rbuf[n - 1, :, at(j)] = flow[mid] + drive
        stencil(lambda j: u3[n, :, at(j)], put)

    for j in range(chunks):
        qbuf[:, at(j)] = s[steps, mid, at(j)] + g[steps - 1, mid, at(j)]
    a_q = Along(T_Q, qbuf, s.at[0, mid])
    a_e0 = Along(T_E0, c0.at[half, mid], c0.at[0, mid])
    a_e1 = Along(T_E1, c1.at[half, mid], c1.at[0, mid])
    a_e2 = Along(T_E2, c2.at[half, mid], c2.at[0, mid])
    a_u3 = Along(T_U3, u3.at[steps, mid], fu)

    x_cond.wait_recv()
    for j in range(chunks):
        cc = c[:, at(j)]
        dd = 1.0 / (1.0 + 4.0 * cc)
        dd2 = 1.0 / (1.0 + 8.0 * cc)
        d[:, at(j)], w[:, at(j)] = dd, cc * dd
        dk[:, at(j)], wk[:, at(j)] = dd2, 2.0 * cc * dd2
    a_q.start()
    guess_halo(steps).wait_recv()

    def local_step(i):
        n = steps - i
        guess_halo(n - 1).wait_recv()
        source_halo(n).wait_recv()

        @pl.when(i == 3)
        def _():
            a_e0.start()
        first_sweep(g, n)
        second_sweep(g, e, n, u1, w, damping)

        @pl.when(jnp.logical_and(lax.rem(i, 2) == 0, i > 0))
        def _():
            m = half + 1 - i // 2
            restrict(m)
            second_sweep(None, er, m, c0, wk, damping)

    each(0, steps - 1, local_step)

    @pl.when(jnp.logical_not(has_before))
    def _():
        start_g.wait()
        start_u.wait()
    a_guess.wait_recv()
    f_guess = within(F_GUESS, g, slice(0, 1))
    f_guess.start()
    sweep_one(3, half + 1)
    each(4, half + 1, lambda m: coarse_defect(c1, m))
    a_e1.start()
    each(4, half + 1, lambda m: second_sweep(c1, ec, m, c2, wk, damping, inner=True))
    f_guess.wait_recv()
    source_halo(1).wait_recv()
    each(1, 2, lambda n: first_sweep(g, n))
    a_e2.start()
    each(1, 2, lambda n: second_sweep(g, e, n, u1, w, damping))
    a_q.wait_recv()
    f_q = within(F_Q, s, slice(0, 1))
    f_q.start()
    f_q.wait_recv()
    each(0, 1, lambda n: first_sweep(g, n, has_prev=False))
    damp0 = jnp.where(has_before, damping, 0.0).astype(jnp.float32)
    each(0, 1, lambda n: second_sweep(g, e, n, u1, w, damp0))
    each(1, 2, restrict)
    each(1, 2, lambda m: second_sweep(None, er, m, c0, wk, damping))
    sweep_one(2, 3)
    sweep_two(3, 4)
    x_late = within(X_LATE, c2, slice(3, half + 1))
    x_late.start()
    a_e0.wait_recv()
    f_e0 = within(F_E0, c0, slice(0, 1))
    f_e0.start()
    x_late.wait_recv()
    each(half, half + 1, prolong)
    each(steps, steps + 1, lambda n: first_sweep(u2, n))
    each(steps, steps + 1, lambda n: second_sweep(u2, e, n, u3, w, damping))

    f_e0.wait_recv()
    each(1, 2, lambda m: coarse_defect(c0, m))
    a_u3.start()
    each(1, 2, lambda m: second_sweep(c0, ec, m, c1, wk, damping))
    sweep_two(2, 3)
    x_mid = within(X_MID, c2, slice(2, 3))
    x_mid.start()
    for j in range(chunks):
        u2[steps - 2, :, at(j)] = u1[steps - 2, :, at(j)] + c2[half - 1, :, at(j)]
    each(steps - 1, steps, lambda n: first_sweep(u2, n))
    each(steps - 1, steps, lambda n: second_sweep(u2, e, n, u3, w, damping))
    each(steps, steps + 1, last_residual)
    a_e1.wait_recv()
    f_e1 = within(F_E1, c1, slice(0, 1))
    f_e1.start()
    x_mid.wait_recv()
    each(3, half, prolong)
    for j in range(chunks):
        u2[4, :, at(j)] = u1[4, :, at(j)] + c2[2, :, at(j)]
    each(5, steps - 1, lambda n: first_sweep(u2, n))
    each(5, steps - 1, lambda n: second_sweep(u2, e, n, u3, w, damping))
    f_e1.wait_recv()
    sweep_two(1, 2)
    x_early = within(X_EARLY, c2, slice(1, 2))
    x_early.start()
    each(6, steps, last_residual)
    a_e2.wait_recv()
    f_e2 = within(F_E2, c2, slice(0, 1))
    f_e2.start()
    x_early.wait_recv()
    for j in range(chunks):
        u2[2, :, at(j)] = u1[2, :, at(j)] + c2[1, :, at(j)]
        u2[3, :, at(j)] = u1[3, :, at(j)] + 0.5 * (c2[1, :, at(j)] + c2[2, :, at(j)])
    each(3, 5, lambda n: first_sweep(u2, n))
    each(3, 5, lambda n: second_sweep(u2, e, n, u3, w, damping))
    each(4, 6, last_residual)
    f_e2.wait_recv()
    for j in range(chunks):
        u2[0, :, at(j)] = u1[0, :, at(j)] + c2[0, :, at(j)]
        u2[1, :, at(j)] = u1[1, :, at(j)] + 0.5 * (c2[0, :, at(j)] + c2[1, :, at(j)])
    each(1, 3, lambda n: first_sweep(u2, n))
    each(1, 3, lambda n: second_sweep(u2, e, n, u3, w, damping))
    each(2, 4, last_residual)
    each(1, 2, lambda n: last_residual(n, has_prev=False))
    for copy in sent:
        copy.wait_send()
    a_u3.wait_recv()
    rbuf[0] = rbuf[0] + fu[...]


def store(u3, rbuf, u_out, r_out, sem):
    steps, rows, _ = u_out.shape
    copies = [
        pltpu.make_async_copy(u3.at[1 : steps + 1, HALO : HALO + rows], u_out, sem.at[0]),
        pltpu.make_async_copy(rbuf, r_out, sem.at[1]),
    ]
    for copy in copies:
        copy.start()
    for copy in copies:
        copy.wait()


def solution(mesh):
    tms, spaces = mesh.shape["tm"], mesh.shape["space"]

    def shards(source, guess, start_state, conduct):
        steps, rows, cols = source.shape
        full, half = rows + 2 * HALO, steps // 2

        def buf(*lead):
            return pltpu.VMEM(lead + (full, cols), jnp.float32)

        fields = pl.pallas_call(
            functools.partial(kernel, tms, spaces),
            out_shape=(buf(steps + 1), pltpu.VMEM(source.shape, jnp.float32)),
            in_specs=[pl.BlockSpec(memory_space=pltpu.HBM)] * 4,
            out_specs=[pl.BlockSpec(memory_space=pltpu.VMEM)] * 2,
            scratch_shapes=[
                buf(steps + 1), buf(steps + 1), buf(), buf(), buf(), buf(), buf(),
                buf(steps + 1), buf(steps + 1), buf(half + 1), buf(half + 1),
                buf(half + 1), buf(half + 1), buf(half + 1), buf(steps + 1),
                pltpu.VMEM((rows, cols), jnp.float32),
                pltpu.VMEM((rows, cols), jnp.float32),
                pltpu.SemaphoreType.DMA((STEPS + 4 * steps,)),
                pltpu.SemaphoreType.DMA((STEPS + 4 * steps,)),
                pltpu.SemaphoreType.DMA((5,)),
            ],
            compiler_params=pltpu.CompilerParams(
                collective_id=0, has_side_effects=True, vmem_limit_bytes=59 * 1024 * 1024),
        )(source, guess, start_state, conduct)
        return pl.pallas_call(
            store,
            out_shape=(jax.ShapeDtypeStruct(source.shape, jnp.float32),) * 2,
            in_specs=[pl.BlockSpec(memory_space=pltpu.VMEM)] * 2,
            out_specs=[pl.BlockSpec(memory_space=pl.ANY)] * 2,
            scratch_shapes=[pltpu.SemaphoreType.DMA((2,))],
            compiler_params=pltpu.CompilerParams(vmem_limit_bytes=8 * 1024 * 1024),
        )(*fields)

    return jax.shard_map(
        shards,
        mesh=mesh,
        in_specs=(P("tm", "space", None), P("tm", "space", None), P("space", None), P("space", None)),
        out_specs=(P("tm", "space", None), P("tm", "space", None)),
        check_vma=False,
    )
```

```python
import functools

import jax
import jax.numpy as jnp
from jax import lax
from jax.experimental import pallas as pl
from jax.experimental.pallas import tpu as pltpu
from jax.sharding import PartitionSpec as P

damping = 0.8
MESH = pl.DeviceIdType.MESH
HALO = 8
LANES = 128

EARLY, SPACE, ALONG = range(0, 6, 2)
T_GUESS, T_Q, T_E0, T_E1, T_E2, T_U3 = range(6)
SETS, PLANES = 4, 6


def kernel(
    tms, spaces, src_hbm, guess_hbm, start_hbm, cond_hbm, u3, rbuf,
    g, s, c, d, w, dk, wk, e, u1, er, ec, c0, c1, c2, u2, qbuf, fu,
    send_sem, recv_sem, load_sem,
):
    t = lax.axis_index("tm")
    z = lax.axis_index("space")
    has_up, has_dn = z > 0, z < spaces - 1
    has_before, has_after = t > 0, t < tms - 1
    steps, rows, cols = src_hbm.shape
    half = steps // 2
    full = rows + 2 * HALO
    mid = slice(HALO, HALO + rows)
    top, bot = slice(0, HALO), slice(HALO + rows, full)
    top_in, bot_in = slice(HALO, 2 * HALO), slice(rows, HALO + rows)
    chunks = cols // LANES
    later = slice(1, steps + 1)

    def remote(src, dst, sent, k, dev):
        return pltpu.make_async_remote_copy(
            src_ref=src, dst_ref=dst, send_sem=send_sem.at[sent], recv_sem=recv_sem.at[k],
            device_id=dev, device_id_type=MESH)

    up, dn = {"space": z - 1}, {"space": z + 1}
    first_set = 2 * half
    first_plane = first_set + 2 * SETS

    class Edge:
        def __init__(self, sent, k, first, last, halo_top, halo_bot):
            self.sent, self.k, self.first, self.last, self.top, self.bot = sent, k, first, last, halo_top, halo_bot

        def start(self):
            @pl.when(has_up)
            def _():
                remote(self.first, self.bot, self.sent, self.k, up).start()

            @pl.when(has_dn)
            def _():
                remote(self.last, self.top, self.sent + 1, self.k + 1, dn).start()

        def wait_recv(self):
            @pl.when(has_dn)
            def _():
                remote(self.first, self.bot, self.sent, self.k, dn).wait_recv()

            @pl.when(has_up)
            def _():
                remote(self.last, self.top, self.sent + 1, self.k + 1, up).wait_recv()

        def wait_send(self):
            @pl.when(has_up)
            def _():
                remote(self.first, self.bot, self.sent, self.k, up).wait_send()

            @pl.when(has_dn)
            def _():
                remote(self.last, self.top, self.sent + 1, self.k + 1, dn).wait_send()

    class Along:
        def __init__(self, k, src, dst):
            self.k, self.src, self.dst = first_plane + k, src, dst

        def start(self):
            @pl.when(has_after)
            def _():
                remote(self.src, self.dst, ALONG, self.k, {"tm": t + 1}).start()

        def wait_recv(self):
            @pl.when(has_before)
            def _():
                remote(self.src, self.dst, ALONG, self.k, {"tm": t - 1}).wait_recv()

        def wait_send(self):
            @pl.when(has_after)
            def _():
                remote(self.src, self.dst, ALONG, self.k, {"tm": t + 1}).wait_send()

    def within(turn, ref, sl):
        return Edge(SPACE, first_set + 2 * turn, ref.at[sl, top_in], ref.at[sl, bot_in], ref.at[sl, top], ref.at[sl, bot])

    def tiles(sent, k, count):
        ref = s.at[0:1, 0 : count * HALO] if count * HALO <= full else s.at[0:2, 0 : count * HALO // 2]
        return Edge(sent, k, ref, ref, ref, ref)

    barrier = pltpu.get_barrier_semaphore()
    for flag, dev in ((has_up, up), (has_dn, dn), (has_before, {"tm": t - 1}), (has_after, {"tm": t + 1})):
        @pl.when(flag)
        def _(dev=dev):
            pl.semaphore_signal(barrier, inc=1, device_id=dev, device_id_type=MESH)

    last_guess = pltpu.make_async_copy(guess_hbm.at[steps - 1], g.at[steps, mid], load_sem.at[0])
    last_guess.start()
    loads = [
        pltpu.make_async_copy(cond_hbm, c.at[mid], load_sem.at[1]),
        pltpu.make_async_copy(src_hbm, s.at[later, mid], load_sem.at[2]),
        pltpu.make_async_copy(guess_hbm.at[0 : steps - 1], g.at[1:steps, mid], load_sem.at[3]),
    ]
    for load in loads:
        load.start()
    start_g = pltpu.make_async_copy(start_hbm, g.at[0, mid], load_sem.at[4])
    start_u = pltpu.make_async_copy(start_hbm, fu, load_sem.at[5])

    @pl.when(jnp.logical_not(has_before))
    def _():
        start_g.start()
        start_u.start()
        s[0, mid] = jnp.zeros((rows, cols), jnp.float32)
        for ref in (c0, c1, c2):
            ref[0, mid] = jnp.zeros((rows, cols), jnp.float32)

    for flag, edge in ((has_up, top), (has_dn, bot)):
        @pl.when(jnp.logical_not(flag))
        def _(edge=edge):
            c[edge] = jnp.zeros((HALO, cols), jnp.float32)
            for ref in (g, s, c0, c1, c2):
                if ref is g or ref is s or ref is c2:
                    ref[:, edge] = jnp.zeros((ref.shape[0], HALO, cols), jnp.float32)
                else:
                    ref[0, edge] = jnp.zeros((HALO, cols), jnp.float32)

    peers = sum(jnp.where(flag, 1, 0) for flag in (has_up, has_dn, has_before, has_after))
    pl.semaphore_wait(barrier, peers)

    a_guess = Along(T_GUESS, g.at[steps, mid], g.at[0, mid])
    last_guess.wait()
    a_guess.start()

    def halo(group, n, hbm, ref):
        Edge(EARLY, 2 * group, hbm.at[n - 1, 0:HALO], hbm.at[n - 1, rows - HALO : rows], ref.at[n, top], ref.at[n, bot]).start()

    Edge(SPACE, 0, cond_hbm.at[0:HALO], cond_hbm.at[rows - HALO : rows], c.at[top], c.at[bot]).start()
    halo(0, steps, guess_hbm, g)
    for i in range(steps - 1):
        n = steps - i
        halo((i + 1) // 2, n - 1, guess_hbm, g)
        halo((i + 1) // 2, n, src_hbm, s)
    halo(half - 1, 1, src_hbm, s)
    for load in loads:
        load.wait()

    lane = lax.broadcasted_iota(jnp.int32, (full, LANES), 1)
    is_first, is_last = lane == 0, lane == LANES - 1

    def at(j):
        return slice(j * LANES, (j + 1) * LANES)

    def each(low, high, body):
        def step(i, carry):
            body(i)
            return carry
        lax.fori_loop(low, high, step, 0)

    def stencil(get, put):
        zero = jnp.zeros((full, LANES), jnp.float32)
        before, now = zero, get(0)
        for j in range(chunks):
            after = get(j + 1) if j + 1 < chunks else zero
            left = pltpu.roll(jnp.where(is_last, before, now), 1, 1)
            right = pltpu.roll(jnp.where(is_first, after, now), LANES - 1, 1)
            rim = (left + right) + (pltpu.roll(now, 1, 0) + pltpu.roll(now, full - 1, 0))
            put(j, now, rim)
            before, now = now, after

    def first_sweep(field, n, has_prev=True):
        def put(j, now, rim):
            drive = s[n, :, at(j)]
            if has_prev:
                drive = drive + field[n - 1, :, at(j)]
            e[n, :, at(j)] = d[:, at(j)] * drive + w[:, at(j)] * rim - now
        stencil(lambda j: field[n, :, at(j)], put)

    def second_sweep(field, errs, n, dst, weight, damp, inner=False):
        def put(j, now, rim):
            gain = damp * (now + weight[:, at(j)] * rim)
            if inner:
                dst[n, mid, at(j)] = field[n, mid, at(j)] + gain[mid]
            elif field is None:
                dst[n, :, at(j)] = gain
            else:
                dst[n, :, at(j)] = field[n, :, at(j)] + gain
        stencil(lambda j: errs[n, :, at(j)], put)

    def restrict(m):
        a, b = 2 * m - 1, 2 * m

        def put(j, now, rim):
            cc = c[:, at(j)]
            drive = (s[a, :, at(j)] + s[b, :, at(j)]) + (u1[a - 1, :, at(j)] + u1[a, :, at(j)])
            er[m, :, at(j)] = dk[:, at(j)] * (drive - now + cc * (rim - 4.0 * now))
        stencil(lambda j: u1[a, :, at(j)] + u1[b, :, at(j)], put)

    def coarse_defect(field, m):
        def put(j, now, rim):
            ec[m, :, at(j)] = er[m, :, at(j)] + dk[:, at(j)] * field[m - 1, :, at(j)] + wk[:, at(j)] * rim - now
        stencil(lambda j: field[m, :, at(j)], put)

    def sweep_one(low, high):
        each(low, high, lambda m: coarse_defect(c0, m))
        each(low, high, lambda m: second_sweep(c0, ec, m, c1, wk, damping))

    def sweep_two(low, high):
        each(low, high, lambda m: coarse_defect(c1, m))
        each(low, high, lambda m: second_sweep(c1, ec, m, c2, wk, damping, inner=True))

    def prolong(m):
        for j in range(chunks):
            u2[2 * m, :, at(j)] = u1[2 * m, :, at(j)] + c2[m, :, at(j)]
            u2[2 * m - 1, :, at(j)] = u1[2 * m - 1, :, at(j)] + 0.5 * (c2[m - 1, :, at(j)] + c2[m, :, at(j)])

    def last_residual(n, has_prev=True):
        def put(j, now, rim):
            flow = c[:, at(j)] * (rim - 4.0 * now) - now
            drive = s[n, mid, at(j)]
            if has_prev:
                drive = drive + u3[n - 1, mid, at(j)]
            rbuf[n - 1, :, at(j)] = flow[mid] + drive
        stencil(lambda j: u3[n, :, at(j)], put)

    for j in range(chunks):
        qbuf[:, at(j)] = s[steps, mid, at(j)] + g[steps - 1, mid, at(j)]
    a_q = Along(T_Q, qbuf, s.at[0, mid])
    a_e0 = Along(T_E0, c0.at[half, mid], c0.at[0, mid])
    a_e1 = Along(T_E1, c1.at[half, mid], c1.at[0, mid])
    a_e2 = Along(T_E2, c2.at[half, mid], c2.at[0, mid])
    a_u3 = Along(T_U3, u3.at[steps, mid], fu)

    tiles(EARLY, 0, 4).wait_recv()
    for j in range(chunks):
        cc = c[:, at(j)]
        dd = 1.0 / (1.0 + 4.0 * cc)
        dd2 = 1.0 / (1.0 + 8.0 * cc)
        d[:, at(j)], w[:, at(j)] = dd, cc * dd
        dk[:, at(j)], wk[:, at(j)] = dd2, 2.0 * cc * dd2
    a_q.start()

    def local_step(i):
        n = steps - i
        odd = lax.rem(i, 2) == 1

        @pl.when(jnp.logical_and(odd, i < steps - 3))
        def _():
            tiles(EARLY, i + 1, 4).wait_recv()

        @pl.when(i == steps - 3)
        def _():
            tiles(EARLY, i + 1, 5).wait_recv()

        @pl.when(i == 3)
        def _():
            a_e0.start()
        first_sweep(g, n)
        second_sweep(g, e, n, u1, w, damping)

        @pl.when(jnp.logical_and(lax.rem(i, 2) == 0, i > 0))
        def _():
            m = half + 1 - i // 2
            restrict(m)
            second_sweep(None, er, m, c0, wk, damping)

    each(0, steps - 1, local_step)

    @pl.when(jnp.logical_not(has_before))
    def _():
        start_g.wait()
        start_u.wait()
    a_guess.wait_recv()
    f_guess = within(0, g, slice(0, 1))
    f_guess.start()
    sweep_one(3, half + 1)
    each(4, half + 1, lambda m: coarse_defect(c1, m))
    a_e1.start()
    each(4, half + 1, lambda m: second_sweep(c1, ec, m, c2, wk, damping, inner=True))
    f_guess.wait_recv()
    each(1, 2, lambda n: first_sweep(g, n))
    a_e2.start()
    each(1, 2, lambda n: second_sweep(g, e, n, u1, w, damping))
    a_q.wait_recv()
    f_q = within(1, s, slice(0, 1))
    f_q.start()
    f_q.wait_recv()
    each(0, 1, lambda n: first_sweep(g, n, has_prev=False))
    damp0 = jnp.where(has_before, damping, 0.0).astype(jnp.float32)
    each(0, 1, lambda n: second_sweep(g, e, n, u1, w, damp0))
    each(1, 2, restrict)
    each(1, 2, lambda m: second_sweep(None, er, m, c0, wk, damping))
    sweep_one(2, 3)
    sweep_two(3, 4)
    x_late = within(0, c2, slice(3, half + 1))
    x_late.start()
    a_e0.wait_recv()
    f_e0 = within(2, c0, slice(0, 1))
    f_e0.start()
    x_late.wait_recv()
    each(half, half + 1, prolong)
    each(steps, steps + 1, lambda n: first_sweep(u2, n))
    each(steps, steps + 1, lambda n: second_sweep(u2, e, n, u3, w, damping))

    f_e0.wait_recv()
    each(1, 2, lambda m: coarse_defect(c0, m))
    a_u3.start()
    each(1, 2, lambda m: second_sweep(c0, ec, m, c1, wk, damping))
    sweep_two(2, 3)
    x_mid = within(1, c2, slice(2, 3))
    x_mid.start()
    for j in range(chunks):
        u2[steps - 2, :, at(j)] = u1[steps - 2, :, at(j)] + c2[half - 1, :, at(j)]
    each(steps - 1, steps, lambda n: first_sweep(u2, n))
    each(steps - 1, steps, lambda n: second_sweep(u2, e, n, u3, w, damping))
    each(steps, steps + 1, last_residual)
    a_e1.wait_recv()
    f_e1 = within(3, c1, slice(0, 1))
    f_e1.start()
    x_mid.wait_recv()
    each(3, half, prolong)
    for j in range(chunks):
        u2[4, :, at(j)] = u1[4, :, at(j)] + c2[2, :, at(j)]
    each(5, steps - 1, lambda n: first_sweep(u2, n))
    each(5, steps - 1, lambda n: second_sweep(u2, e, n, u3, w, damping))
    f_e1.wait_recv()
    sweep_two(1, 2)
    x_early = within(0, c2, slice(1, 2))
    x_early.start()
    each(6, steps, last_residual)
    a_e2.wait_recv()
    f_e2 = within(2, c2, slice(0, 1))
    f_e2.start()
    x_early.wait_recv()
    for j in range(chunks):
        u2[2, :, at(j)] = u1[2, :, at(j)] + c2[1, :, at(j)]
        u2[3, :, at(j)] = u1[3, :, at(j)] + 0.5 * (c2[1, :, at(j)] + c2[2, :, at(j)])
    each(3, 5, lambda n: first_sweep(u2, n))
    each(3, 5, lambda n: second_sweep(u2, e, n, u3, w, damping))
    each(4, 6, last_residual)
    f_e2.wait_recv()
    for j in range(chunks):
        u2[0, :, at(j)] = u1[0, :, at(j)] + c2[0, :, at(j)]
        u2[1, :, at(j)] = u1[1, :, at(j)] + 0.5 * (c2[0, :, at(j)] + c2[1, :, at(j)])
    each(1, 3, lambda n: first_sweep(u2, n))
    each(1, 3, lambda n: second_sweep(u2, e, n, u3, w, damping))
    each(2, 4, last_residual)
    each(1, 2, lambda n: last_residual(n, has_prev=False))
    tiles(EARLY, 0, 2 * steps).wait_send()
    tiles(SPACE, 0, half + 6).wait_send()
    Along(T_U3, s.at[0:PLANES, mid], s.at[0:PLANES, mid]).wait_send()
    a_u3.wait_recv()
    rbuf[0] = rbuf[0] + fu[...]


def store(u3, rbuf, u_out, r_out, sem):
    steps, rows, _ = u_out.shape
    copies = [
        pltpu.make_async_copy(u3.at[1 : steps + 1, HALO : HALO + rows], u_out, sem.at[0]),
        pltpu.make_async_copy(rbuf, r_out, sem.at[1]),
    ]
    for copy in copies:
        copy.start()
    for copy in copies:
        copy.wait()


def solution(mesh):
    tms, spaces = mesh.shape["tm"], mesh.shape["space"]

    def shards(source, guess, start_state, conduct):
        steps, rows, cols = source.shape
        full, half = rows + 2 * HALO, steps // 2

        def buf(*lead):
            return pltpu.VMEM(lead + (full, cols), jnp.float32)

        fields = pl.pallas_call(
            functools.partial(kernel, tms, spaces),
            out_shape=(buf(steps + 1), pltpu.VMEM(source.shape, jnp.float32)),
            in_specs=[pl.BlockSpec(memory_space=pltpu.HBM)] * 4,
            out_specs=[pl.BlockSpec(memory_space=pltpu.VMEM)] * 2,
            scratch_shapes=[
                buf(steps + 1), buf(steps + 1), buf(), buf(), buf(), buf(), buf(),
                buf(steps + 1), buf(steps + 1), buf(half + 1), buf(half + 1),
                buf(half + 1), buf(half + 1), buf(half + 1), buf(steps + 1),
                pltpu.VMEM((rows, cols), jnp.float32),
                pltpu.VMEM((rows, cols), jnp.float32),
                pltpu.SemaphoreType.DMA((5,)),
                pltpu.SemaphoreType.DMA((steps + 2 * SETS + PLANES,)),
                pltpu.SemaphoreType.DMA((6,)),
            ],
            compiler_params=pltpu.CompilerParams(
                collective_id=0, has_side_effects=True, vmem_limit_bytes=59 * 1024 * 1024),
        )(source, guess, start_state, conduct)
        return pl.pallas_call(
            store,
            out_shape=(jax.ShapeDtypeStruct(source.shape, jnp.float32),) * 2,
            in_specs=[pl.BlockSpec(memory_space=pltpu.VMEM)] * 2,
            out_specs=[pl.BlockSpec(memory_space=pl.ANY)] * 2,
            scratch_shapes=[pltpu.SemaphoreType.DMA((2,))],
            compiler_params=pltpu.CompilerParams(vmem_limit_bytes=8 * 1024 * 1024),
        )(*fields)

    return jax.shard_map(
        shards,
        mesh=mesh,
        in_specs=(P("tm", "space", None), P("tm", "space", None), P("space", None), P("space", None)),
        out_specs=(P("tm", "space", None), P("tm", "space", None)),
        check_vma=False,
    )
```

```python
import functools

import jax
import jax.numpy as jnp
from jax import lax
from jax.experimental import pallas as pl
from jax.experimental.pallas import tpu as pltpu
from jax.sharding import PartitionSpec as P

damping = 0.8
MESH = pl.DeviceIdType.MESH
HALO = 8
LANES = 128

EARLY, SPACE, ALONG = range(0, 6, 2)
T_GUESS, T_Q, T_E0, T_E1_RIM, T_E1, T_E2_RIM, T_E2, T_U3 = range(8)
SETS, PLANES, PARTS = 4, 6, 8


def kernel(
    tms, spaces, src_hbm, guess_hbm, start_hbm, cond_hbm, u3, rbuf,
    g, s, c, d, w, dk, wk, e, u1, er, ec, c0, c1, c2, u2, qbuf, fu,
    send_sem, recv_sem, load_sem,
):
    t = lax.axis_index("tm")
    z = lax.axis_index("space")
    has_up, has_dn = z > 0, z < spaces - 1
    has_before, has_after = t > 0, t < tms - 1
    steps, rows, cols = src_hbm.shape
    half = steps // 2
    full = rows + 2 * HALO
    mid = slice(HALO, HALO + rows)
    top, bot = slice(0, HALO), slice(HALO + rows, full)
    top_in, bot_in = slice(HALO, 2 * HALO), slice(rows, HALO + rows)
    chunks = cols // LANES
    later = slice(1, steps + 1)

    def remote(src, dst, sent, k, dev):
        return pltpu.make_async_remote_copy(
            src_ref=src, dst_ref=dst, send_sem=send_sem.at[sent], recv_sem=recv_sem.at[k],
            device_id=dev, device_id_type=MESH)

    up, dn = {"space": z - 1}, {"space": z + 1}
    first_set = 2 * half
    first_plane = first_set + 2 * SETS

    class Edge:
        def __init__(self, sent, k, first, last, halo_top, halo_bot):
            self.sent, self.k, self.first, self.last, self.top, self.bot = sent, k, first, last, halo_top, halo_bot

        def start(self):
            @pl.when(has_up)
            def _():
                remote(self.first, self.bot, self.sent, self.k, up).start()

            @pl.when(has_dn)
            def _():
                remote(self.last, self.top, self.sent + 1, self.k + 1, dn).start()

        def wait_recv(self):
            @pl.when(has_dn)
            def _():
                remote(self.first, self.bot, self.sent, self.k, dn).wait_recv()

            @pl.when(has_up)
            def _():
                remote(self.last, self.top, self.sent + 1, self.k + 1, up).wait_recv()

        def wait_send(self):
            @pl.when(has_up)
            def _():
                remote(self.first, self.bot, self.sent, self.k, up).wait_send()

            @pl.when(has_dn)
            def _():
                remote(self.last, self.top, self.sent + 1, self.k + 1, dn).wait_send()

    class Along:
        def __init__(self, k, src, dst):
            self.k, self.src, self.dst = first_plane + k, src, dst

        def start(self):
            @pl.when(has_after)
            def _():
                remote(self.src, self.dst, ALONG, self.k, {"tm": t + 1}).start()

        def wait_recv(self):
            @pl.when(has_before)
            def _():
                remote(self.src, self.dst, ALONG, self.k, {"tm": t - 1}).wait_recv()

        def wait_send(self):
            @pl.when(has_after)
            def _():
                remote(self.src, self.dst, ALONG, self.k, {"tm": t + 1}).wait_send()

    class Split:
        def __init__(self, k, ref):
            def part(k, rows_of):
                return Along(k, ref.at[half, rows_of], ref.at[0, rows_of])
            self.rim = Along(k, s.at[0, 0 : 2 * HALO], s.at[0, 0 : 2 * HALO])
            self.rest = part(k + 1, slice(2 * HALO, rows))
            self.parts = [part(k, top_in), part(k, bot_in), self.rest]

        def start(self):
            for part in self.parts:
                part.start()

    def within(turn, ref, sl):
        return Edge(SPACE, first_set + 2 * turn, ref.at[sl, top_in], ref.at[sl, bot_in], ref.at[sl, top], ref.at[sl, bot])

    def tiles(sent, k, count):
        ref = s.at[0:1, 0 : count * HALO] if count * HALO <= full else s.at[0:2, 0 : count * HALO // 2]
        return Edge(sent, k, ref, ref, ref, ref)

    barrier = pltpu.get_barrier_semaphore()
    for flag, dev in ((has_up, up), (has_dn, dn), (has_before, {"tm": t - 1}), (has_after, {"tm": t + 1})):
        @pl.when(flag)
        def _(dev=dev):
            pl.semaphore_signal(barrier, inc=1, device_id=dev, device_id_type=MESH)

    last_guess = pltpu.make_async_copy(guess_hbm.at[steps - 1], g.at[steps, mid], load_sem.at[0])
    last_guess.start()
    loads = [
        pltpu.make_async_copy(cond_hbm, c.at[mid], load_sem.at[1]),
        pltpu.make_async_copy(src_hbm, s.at[later, mid], load_sem.at[2]),
        pltpu.make_async_copy(guess_hbm.at[0 : steps - 1], g.at[1:steps, mid], load_sem.at[3]),
    ]
    for load in loads:
        load.start()
    start_g = pltpu.make_async_copy(start_hbm, g.at[0, mid], load_sem.at[4])
    start_u = pltpu.make_async_copy(start_hbm, fu, load_sem.at[5])

    @pl.when(jnp.logical_not(has_before))
    def _():
        start_g.start()
        start_u.start()
        s[0, mid] = jnp.zeros((rows, cols), jnp.float32)
        for ref in (c0, c1, c2):
            ref[0, mid] = jnp.zeros((rows, cols), jnp.float32)

    for flag, edge in ((has_up, top), (has_dn, bot)):
        @pl.when(jnp.logical_not(flag))
        def _(edge=edge):
            c[edge] = jnp.zeros((HALO, cols), jnp.float32)
            for ref in (g, s, c0, c1, c2):
                if ref is g or ref is s or ref is c2:
                    ref[:, edge] = jnp.zeros((ref.shape[0], HALO, cols), jnp.float32)
                else:
                    ref[0, edge] = jnp.zeros((HALO, cols), jnp.float32)

    peers = sum(jnp.where(flag, 1, 0) for flag in (has_up, has_dn, has_before, has_after))
    pl.semaphore_wait(barrier, peers)

    a_guess = Along(T_GUESS, g.at[steps, mid], g.at[0, mid])
    last_guess.wait()
    a_guess.start()

    def halo(group, n, hbm, ref):
        Edge(EARLY, 2 * group, hbm.at[n - 1, 0:HALO], hbm.at[n - 1, rows - HALO : rows], ref.at[n, top], ref.at[n, bot]).start()

    Edge(SPACE, 0, cond_hbm.at[0:HALO], cond_hbm.at[rows - HALO : rows], c.at[top], c.at[bot]).start()
    halo(0, steps, guess_hbm, g)
    for i in range(steps - 1):
        n = steps - i
        halo((i + 1) // 2, n - 1, guess_hbm, g)
        halo((i + 1) // 2, n, src_hbm, s)
    halo(half - 1, 1, src_hbm, s)
    for load in loads:
        load.wait()

    lane = lax.broadcasted_iota(jnp.int32, (full, LANES), 1)
    is_first, is_last = lane == 0, lane == LANES - 1

    def at(j):
        return slice(j * LANES, (j + 1) * LANES)

    def each(low, high, body):
        def step(i, carry):
            body(i)
            return carry
        lax.fori_loop(low, high, step, 0)

    def stencil(get, put):
        zero = jnp.zeros((full, LANES), jnp.float32)
        before, now = zero, get(0)
        for j in range(chunks):
            after = get(j + 1) if j + 1 < chunks else zero
            left = pltpu.roll(jnp.where(is_last, before, now), 1, 1)
            right = pltpu.roll(jnp.where(is_first, after, now), LANES - 1, 1)
            rim = (left + right) + (pltpu.roll(now, 1, 0) + pltpu.roll(now, full - 1, 0))
            put(j, now, rim)
            before, now = now, after

    def first_sweep(field, n, has_prev=True):
        def put(j, now, rim):
            drive = s[n, :, at(j)]
            if has_prev:
                drive = drive + field[n - 1, :, at(j)]
            e[n, :, at(j)] = d[:, at(j)] * drive + w[:, at(j)] * rim - now
        stencil(lambda j: field[n, :, at(j)], put)

    def second_sweep(field, errs, n, dst, weight, damp, inner=False):
        def put(j, now, rim):
            gain = damp * (now + weight[:, at(j)] * rim)
            if inner:
                dst[n, mid, at(j)] = field[n, mid, at(j)] + gain[mid]
            elif field is None:
                dst[n, :, at(j)] = gain
            else:
                dst[n, :, at(j)] = field[n, :, at(j)] + gain
        stencil(lambda j: errs[n, :, at(j)], put)

    def restrict(m):
        a, b = 2 * m - 1, 2 * m

        def put(j, now, rim):
            cc = c[:, at(j)]
            drive = (s[a, :, at(j)] + s[b, :, at(j)]) + (u1[a - 1, :, at(j)] + u1[a, :, at(j)])
            er[m, :, at(j)] = dk[:, at(j)] * (drive - now + cc * (rim - 4.0 * now))
        stencil(lambda j: u1[a, :, at(j)] + u1[b, :, at(j)], put)

    def coarse_defect(field, m):
        def put(j, now, rim):
            ec[m, :, at(j)] = er[m, :, at(j)] + dk[:, at(j)] * field[m - 1, :, at(j)] + wk[:, at(j)] * rim - now
        stencil(lambda j: field[m, :, at(j)], put)

    def sweep_one(low, high):
        each(low, high, lambda m: coarse_defect(c0, m))
        each(low, high, lambda m: second_sweep(c0, ec, m, c1, wk, damping))

    def sweep_two(low, high):
        each(low, high, lambda m: coarse_defect(c1, m))
        each(low, high, lambda m: second_sweep(c1, ec, m, c2, wk, damping, inner=True))

    def prolong(m):
        for j in range(chunks):
            u2[2 * m, :, at(j)] = u1[2 * m, :, at(j)] + c2[m, :, at(j)]
            u2[2 * m - 1, :, at(j)] = u1[2 * m - 1, :, at(j)] + 0.5 * (c2[m - 1, :, at(j)] + c2[m, :, at(j)])

    def last_residual(n, has_prev=True):
        def put(j, now, rim):
            flow = c[:, at(j)] * (rim - 4.0 * now) - now
            drive = s[n, mid, at(j)]
            if has_prev:
                drive = drive + u3[n - 1, mid, at(j)]
            rbuf[n - 1, :, at(j)] = flow[mid] + drive
        stencil(lambda j: u3[n, :, at(j)], put)

    for j in range(chunks):
        qbuf[:, at(j)] = s[steps, mid, at(j)] + g[steps - 1, mid, at(j)]
    a_q = Along(T_Q, qbuf, s.at[0, mid])
    a_e0 = Along(T_E0, c0.at[half, mid], c0.at[0, mid])
    a_e1 = Split(T_E1_RIM, c1)
    a_e2 = Split(T_E2_RIM, c2)
    a_u3 = Along(T_U3, u3.at[steps, mid], fu)

    tiles(EARLY, 0, 4).wait_recv()
    for j in range(chunks):
        cc = c[:, at(j)]
        dd = 1.0 / (1.0 + 4.0 * cc)
        dd2 = 1.0 / (1.0 + 8.0 * cc)
        d[:, at(j)], w[:, at(j)] = dd, cc * dd
        dk[:, at(j)], wk[:, at(j)] = dd2, 2.0 * cc * dd2
    a_q.start()

    def local_step(i):
        n = steps - i
        odd = lax.rem(i, 2) == 1

        @pl.when(jnp.logical_and(odd, i < steps - 3))
        def _():
            tiles(EARLY, i + 1, 4).wait_recv()

        @pl.when(i == steps - 3)
        def _():
            tiles(EARLY, i + 1, 5).wait_recv()

        @pl.when(i == 3)
        def _():
            a_e0.start()
        first_sweep(g, n)
        second_sweep(g, e, n, u1, w, damping)

        @pl.when(jnp.logical_and(lax.rem(i, 2) == 0, i > 0))
        def _():
            m = half + 1 - i // 2
            restrict(m)
            second_sweep(None, er, m, c0, wk, damping)

    each(0, steps - 1, local_step)

    @pl.when(jnp.logical_not(has_before))
    def _():
        start_g.wait()
        start_u.wait()
    a_guess.wait_recv()
    f_guess = within(0, g, slice(0, 1))
    f_guess.start()
    sweep_one(3, half + 1)
    each(4, half + 1, lambda m: coarse_defect(c1, m))
    a_e1.start()
    each(4, half + 1, lambda m: second_sweep(c1, ec, m, c2, wk, damping, inner=True))
    f_guess.wait_recv()
    each(1, 2, lambda n: first_sweep(g, n))
    a_e2.start()
    each(1, 2, lambda n: second_sweep(g, e, n, u1, w, damping))
    a_q.wait_recv()
    f_q = within(1, s, slice(0, 1))
    f_q.start()
    f_q.wait_recv()
    each(0, 1, lambda n: first_sweep(g, n, has_prev=False))
    damp0 = jnp.where(has_before, damping, 0.0).astype(jnp.float32)
    each(0, 1, lambda n: second_sweep(g, e, n, u1, w, damp0))
    each(1, 2, restrict)
    each(1, 2, lambda m: second_sweep(None, er, m, c0, wk, damping))
    sweep_one(2, 3)
    sweep_two(3, 4)
    x_late = within(0, c2, slice(3, half + 1))
    x_late.start()
    a_e0.wait_recv()
    f_e0 = within(2, c0, slice(0, 1))
    f_e0.start()
    x_late.wait_recv()
    each(half, half + 1, prolong)
    each(steps, steps + 1, lambda n: first_sweep(u2, n))
    each(steps, steps + 1, lambda n: second_sweep(u2, e, n, u3, w, damping))

    a_e1.rim.wait_recv()
    f_e1 = within(3, c1, slice(0, 1))
    f_e1.start()
    f_e0.wait_recv()
    each(1, 2, lambda m: coarse_defect(c0, m))
    a_u3.start()
    each(1, 2, lambda m: second_sweep(c0, ec, m, c1, wk, damping))
    sweep_two(2, 3)
    x_mid = within(1, c2, slice(2, 3))
    x_mid.start()
    for j in range(chunks):
        u2[steps - 2, :, at(j)] = u1[steps - 2, :, at(j)] + c2[half - 1, :, at(j)]
    each(steps - 1, steps, lambda n: first_sweep(u2, n))
    each(steps - 1, steps, lambda n: second_sweep(u2, e, n, u3, w, damping))
    each(steps, steps + 1, last_residual)
    a_e1.rest.wait_recv()
    f_e1.wait_recv()
    sweep_two(1, 2)
    x_early = within(0, c2, slice(1, 2))
    x_early.start()
    x_mid.wait_recv()
    each(3, half, prolong)
    for j in range(chunks):
        u2[4, :, at(j)] = u1[4, :, at(j)] + c2[2, :, at(j)]
    each(5, steps - 1, lambda n: first_sweep(u2, n))
    each(5, steps - 1, lambda n: second_sweep(u2, e, n, u3, w, damping))
    a_e2.rim.wait_recv()
    f_e2 = within(2, c2, slice(0, 1))
    f_e2.start()
    each(6, steps, last_residual)
    x_early.wait_recv()
    for j in range(chunks):
        u2[2, :, at(j)] = u1[2, :, at(j)] + c2[1, :, at(j)]
        u2[3, :, at(j)] = u1[3, :, at(j)] + 0.5 * (c2[1, :, at(j)] + c2[2, :, at(j)])
    each(3, 5, lambda n: first_sweep(u2, n))
    each(3, 5, lambda n: second_sweep(u2, e, n, u3, w, damping))
    each(4, 6, last_residual)
    a_e2.rest.wait_recv()
    f_e2.wait_recv()
    for j in range(chunks):
        u2[0, :, at(j)] = u1[0, :, at(j)] + c2[0, :, at(j)]
        u2[1, :, at(j)] = u1[1, :, at(j)] + 0.5 * (c2[0, :, at(j)] + c2[1, :, at(j)])
    each(1, 3, lambda n: first_sweep(u2, n))
    each(1, 3, lambda n: second_sweep(u2, e, n, u3, w, damping))
    each(2, 4, last_residual)
    each(1, 2, lambda n: last_residual(n, has_prev=False))
    tiles(EARLY, 0, 2 * steps).wait_send()
    tiles(SPACE, 0, half + 6).wait_send()
    Along(T_U3, s.at[0:PLANES, mid], s.at[0:PLANES, mid]).wait_send()
    a_u3.wait_recv()
    rbuf[0] = rbuf[0] + fu[...]


def store(u3, rbuf, u_out, r_out, sem):
    steps, rows, _ = u_out.shape
    copies = [
        pltpu.make_async_copy(u3.at[1 : steps + 1, HALO : HALO + rows], u_out, sem.at[0]),
        pltpu.make_async_copy(rbuf, r_out, sem.at[1]),
    ]
    for copy in copies:
        copy.start()
    for copy in copies:
        copy.wait()


def solution(mesh):
    tms, spaces = mesh.shape["tm"], mesh.shape["space"]

    def shards(source, guess, start_state, conduct):
        steps, rows, cols = source.shape
        full, half = rows + 2 * HALO, steps // 2

        def buf(*lead):
            return pltpu.VMEM(lead + (full, cols), jnp.float32)

        fields = pl.pallas_call(
            functools.partial(kernel, tms, spaces),
            out_shape=(buf(steps + 1), pltpu.VMEM(source.shape, jnp.float32)),
            in_specs=[pl.BlockSpec(memory_space=pltpu.HBM)] * 4,
            out_specs=[pl.BlockSpec(memory_space=pltpu.VMEM)] * 2,
            scratch_shapes=[
                buf(steps + 1), buf(steps + 1), buf(), buf(), buf(), buf(), buf(),
                buf(steps + 1), buf(steps + 1), buf(half + 1), buf(half + 1),
                buf(half + 1), buf(half + 1), buf(half + 1), buf(steps + 1),
                pltpu.VMEM((rows, cols), jnp.float32),
                pltpu.VMEM((rows, cols), jnp.float32),
                pltpu.SemaphoreType.DMA((5,)),
                pltpu.SemaphoreType.DMA((steps + 2 * SETS + PARTS,)),
                pltpu.SemaphoreType.DMA((6,)),
            ],
            compiler_params=pltpu.CompilerParams(
                collective_id=0, has_side_effects=True, vmem_limit_bytes=59 * 1024 * 1024),
        )(source, guess, start_state, conduct)
        return pl.pallas_call(
            store,
            out_shape=(jax.ShapeDtypeStruct(source.shape, jnp.float32),) * 2,
            in_specs=[pl.BlockSpec(memory_space=pltpu.VMEM)] * 2,
            out_specs=[pl.BlockSpec(memory_space=pl.ANY)] * 2,
            scratch_shapes=[pltpu.SemaphoreType.DMA((2,))],
            compiler_params=pltpu.CompilerParams(vmem_limit_bytes=8 * 1024 * 1024),
        )(*fields)

    return jax.shard_map(
        shards,
        mesh=mesh,
        in_specs=(P("tm", "space", None), P("tm", "space", None), P("space", None), P("space", None)),
        out_specs=(P("tm", "space", None), P("tm", "space", None)),
        check_vma=False,
    )
```

```python
import functools

import jax
import jax.numpy as jnp
from jax import lax
from jax.experimental import pallas as pl
from jax.experimental.pallas import tpu as pltpu
from jax.sharding import PartitionSpec as P

damping = 0.8
MESH = pl.DeviceIdType.MESH
HALO = 8
LANES = 128

EARLY, SPACE, ALONG, RELAY = 0, 2, 4, 5
T_GUESS, T_Q, T_E0, T_E1_RIM, T_E1, T_E2_RIM, T_E2, T_U3, T_RELAY = range(9)
SETS, PLANES, PARTS = 4, 6, 9
RELAYED = 2 * HALO


def kernel(
    tms, spaces, src_hbm, guess_hbm, start_hbm, cond_hbm, u3, rbuf,
    g, s, c, d, w, dk, wk, e, u1, er, ec, c0, c1, c2, u2, qbuf, fu,
    relay, send_sem, recv_sem,
):
    t = lax.axis_index("tm")
    z = lax.axis_index("space")
    has_up, has_dn = z > 0, z < spaces - 1
    has_before, has_after = t > 0, t < tms - 1
    by_relay = jnp.logical_and(lax.rem(t, 2) == 1, t + 2 < tms)
    is_relay = jnp.logical_and(lax.rem(t, 2) == 1, t > 2)
    steps, rows, cols = src_hbm.shape
    half = steps // 2
    full = rows + 2 * HALO
    mid = slice(HALO, HALO + rows)
    top, bot = slice(0, HALO), slice(HALO + rows, full)
    top_in, bot_in = slice(HALO, 2 * HALO), slice(rows, HALO + rows)
    chunks = cols // LANES
    later = slice(1, steps + 1)

    def remote(src, dst, sent, k, dev):
        return pltpu.make_async_remote_copy(
            src_ref=src, dst_ref=dst, send_sem=send_sem.at[sent], recv_sem=recv_sem.at[k],
            device_id=dev, device_id_type=MESH)

    up, dn = {"space": z - 1}, {"space": z + 1}
    first_set = 2 * half
    first_plane = first_set + 2 * SETS

    class Edge:
        def __init__(self, sent, k, first, last, halo_top, halo_bot):
            self.sent, self.k, self.first, self.last, self.top, self.bot = sent, k, first, last, halo_top, halo_bot

        def start(self):
            @pl.when(has_up)
            def _():
                remote(self.first, self.bot, self.sent, self.k, up).start()

            @pl.when(has_dn)
            def _():
                remote(self.last, self.top, self.sent + 1, self.k + 1, dn).start()

        def wait_recv(self):
            @pl.when(has_dn)
            def _():
                remote(self.first, self.bot, self.sent, self.k, dn).wait_recv()

            @pl.when(has_up)
            def _():
                remote(self.last, self.top, self.sent + 1, self.k + 1, up).wait_recv()

        def wait_send(self):
            @pl.when(has_up)
            def _():
                remote(self.first, self.bot, self.sent, self.k, up).wait_send()

            @pl.when(has_dn)
            def _():
                remote(self.last, self.top, self.sent + 1, self.k + 1, dn).wait_send()

    class Along:
        def __init__(self, k, src, dst):
            self.k, self.src, self.dst = first_plane + k, src, dst

        def start(self):
            @pl.when(has_after)
            def _():
                remote(self.src, self.dst, ALONG, self.k, {"tm": t + 1}).start()

        def wait_recv(self):
            @pl.when(has_before)
            def _():
                remote(self.src, self.dst, ALONG, self.k, {"tm": t - 1}).wait_recv()

        def wait_send(self):
            @pl.when(has_after)
            def _():
                remote(self.src, self.dst, ALONG, self.k, {"tm": t + 1}).wait_send()

    class Split:
        def __init__(self, k, ref):
            def part(k, rows_of):
                return Along(k, ref.at[half, rows_of], ref.at[0, rows_of])
            self.rim = Along(k, s.at[0, 0 : 2 * HALO], s.at[0, 0 : 2 * HALO])
            self.rest = part(k + 1, slice(2 * HALO, rows))
            self.parts = [part(k, top_in), part(k, bot_in), self.rest]

        def start(self):
            for part in self.parts:
                part.start()

    def within(turn, ref, sl):
        return Edge(SPACE, first_set + 2 * turn, ref.at[sl, top_in], ref.at[sl, bot_in], ref.at[sl, top], ref.at[sl, bot])

    def tiles(sent, k, count):
        ref = s.at[0:1, 0 : count * HALO] if count * HALO <= full else s.at[0:2, 0 : count * HALO // 2]
        return Edge(sent, k, ref, ref, ref, ref)

    barrier = pltpu.get_barrier_semaphore()
    peers = (
        (has_up, up), (has_dn, dn), (has_before, {"tm": t - 1}), (has_after, {"tm": t + 1}),
        (is_relay, {"tm": t - 2}), (by_relay, {"tm": t + 2}))
    for flag, dev in peers:
        @pl.when(flag)
        def _(dev=dev):
            pl.semaphore_signal(barrier, inc=1, device_id=dev, device_id_type=MESH)

    last_guess = pltpu.make_async_copy(guess_hbm.at[steps - 1], g.at[steps, mid], send_sem.at[ALONG])
    last_guess.start()
    loads = [
        pltpu.make_async_copy(cond_hbm, c.at[mid], recv_sem.at[first_plane - 1]),
        pltpu.make_async_copy(src_hbm, s.at[later, mid], recv_sem.at[first_plane - 2]),
        pltpu.make_async_copy(guess_hbm.at[0 : steps - 1], g.at[1:steps, mid], recv_sem.at[first_plane - 3]),
    ]
    for load in loads:
        load.start()
    start_g = pltpu.make_async_copy(start_hbm, g.at[0, mid], recv_sem.at[first_plane + T_GUESS])
    start_u = pltpu.make_async_copy(start_hbm, fu, recv_sem.at[first_plane + T_U3])

    @pl.when(jnp.logical_not(has_before))
    def _():
        start_g.start()
        start_u.start()
        s[0, mid] = jnp.zeros((rows, cols), jnp.float32)
        for ref in (c0, c1, c2):
            ref[0, mid] = jnp.zeros((rows, cols), jnp.float32)

    for flag, edge in ((has_up, top), (has_dn, bot)):
        @pl.when(jnp.logical_not(flag))
        def _(edge=edge):
            c[edge] = jnp.zeros((HALO, cols), jnp.float32)
            for ref in (g, s, c0, c1, c2):
                if ref is g or ref is s or ref is c2:
                    ref[:, edge] = jnp.zeros((ref.shape[0], HALO, cols), jnp.float32)
                else:
                    ref[0, edge] = jnp.zeros((HALO, cols), jnp.float32)

    pl.semaphore_wait(barrier, sum(jnp.where(flag, 1, 0) for flag, _ in peers))

    a_guess = Along(T_GUESS, g.at[steps, mid], g.at[0, mid])
    last_guess.wait()
    a_guess.start()

    def halo(group, n, hbm, ref):
        Edge(EARLY, 2 * group, hbm.at[n - 1, 0:HALO], hbm.at[n - 1, rows - HALO : rows], ref.at[n, top], ref.at[n, bot]).start()

    Edge(SPACE, 0, cond_hbm.at[0:HALO], cond_hbm.at[rows - HALO : rows], c.at[top], c.at[bot]).start()
    halo(0, steps, guess_hbm, g)
    for i in range(steps - 1):
        n = steps - i
        halo((i + 1) // 2, n - 1, guess_hbm, g)
        halo((i + 1) // 2, n, src_hbm, s)
    halo(half - 1, 1, src_hbm, s)
    for load in loads:
        load.wait()

    lane = lax.broadcasted_iota(jnp.int32, (full, LANES), 1)
    is_first, is_last = lane == 0, lane == LANES - 1

    def at(j):
        return slice(j * LANES, (j + 1) * LANES)

    def each(low, high, body):
        def step(i, carry):
            body(i)
            return carry
        lax.fori_loop(low, high, step, 0)

    def stencil(get, put):
        zero = jnp.zeros((full, LANES), jnp.float32)
        before, now = zero, get(0)
        for j in range(chunks):
            after = get(j + 1) if j + 1 < chunks else zero
            left = pltpu.roll(jnp.where(is_last, before, now), 1, 1)
            right = pltpu.roll(jnp.where(is_first, after, now), LANES - 1, 1)
            rim = (left + right) + (pltpu.roll(now, 1, 0) + pltpu.roll(now, full - 1, 0))
            put(j, now, rim)
            before, now = now, after

    def first_sweep(field, n, has_prev=True):
        def put(j, now, rim):
            drive = s[n, :, at(j)]
            if has_prev:
                drive = drive + field[n - 1, :, at(j)]
            e[n, :, at(j)] = d[:, at(j)] * drive + w[:, at(j)] * rim - now
        stencil(lambda j: field[n, :, at(j)], put)

    def second_sweep(field, errs, n, dst, weight, damp, inner=False):
        def put(j, now, rim):
            gain = damp * (now + weight[:, at(j)] * rim)
            if inner:
                dst[n, mid, at(j)] = field[n, mid, at(j)] + gain[mid]
            elif field is None:
                dst[n, :, at(j)] = gain
            else:
                dst[n, :, at(j)] = field[n, :, at(j)] + gain
        stencil(lambda j: errs[n, :, at(j)], put)

    def restrict(m):
        a, b = 2 * m - 1, 2 * m

        def put(j, now, rim):
            cc = c[:, at(j)]
            drive = (s[a, :, at(j)] + s[b, :, at(j)]) + (u1[a - 1, :, at(j)] + u1[a, :, at(j)])
            er[m, :, at(j)] = dk[:, at(j)] * (drive - now + cc * (rim - 4.0 * now))
        stencil(lambda j: u1[a, :, at(j)] + u1[b, :, at(j)], put)

    def coarse_defect(field, m):
        def put(j, now, rim):
            ec[m, :, at(j)] = er[m, :, at(j)] + dk[:, at(j)] * field[m - 1, :, at(j)] + wk[:, at(j)] * rim - now
        stencil(lambda j: field[m, :, at(j)], put)

    def sweep_one(low, high):
        each(low, high, lambda m: coarse_defect(c0, m))
        each(low, high, lambda m: second_sweep(c0, ec, m, c1, wk, damping))

    def sweep_two(low, high):
        each(low, high, lambda m: coarse_defect(c1, m))
        each(low, high, lambda m: second_sweep(c1, ec, m, c2, wk, damping, inner=True))

    def prolong(m):
        for j in range(chunks):
            u2[2 * m, :, at(j)] = u1[2 * m, :, at(j)] + c2[m, :, at(j)]
            u2[2 * m - 1, :, at(j)] = u1[2 * m - 1, :, at(j)] + 0.5 * (c2[m - 1, :, at(j)] + c2[m, :, at(j)])

    def last_residual(n, has_prev=True):
        def put(j, now, rim):
            flow = c[:, at(j)] * (rim - 4.0 * now) - now
            drive = s[n, mid, at(j)]
            if has_prev:
                drive = drive + u3[n - 1, mid, at(j)]
            rbuf[n - 1, :, at(j)] = flow[mid] + drive
        stencil(lambda j: u3[n, :, at(j)], put)

    for j in range(chunks):
        qbuf[:, at(j)] = s[steps, mid, at(j)] + g[steps - 1, mid, at(j)]
    a_q = Along(T_Q, qbuf, s.at[0, mid])
    a_e0 = Along(T_E0, c0.at[half, mid], c0.at[0, mid])
    a_e1 = Split(T_E1_RIM, c1)
    a_e2 = Split(T_E2_RIM, c2)
    a_u3 = Along(T_U3, fu, fu)
    kept = rows - RELAYED
    u3_kept = Along(T_U3, u3.at[steps, HALO : HALO + kept], fu.at[0:kept])
    u3_rest = Along(T_U3, u3.at[steps, HALO + kept : HALO + rows], fu.at[kept:rows])

    def to_relay(sent, k, src, dst, step):
        return remote(src, dst, sent, first_plane + k, {"tm": t + step})

    def start_u3():
        u3_kept.start()

        @pl.when(jnp.logical_not(by_relay))
        def _():
            u3_rest.start()

        @pl.when(by_relay)
        def _():
            to_relay(ALONG, T_RELAY, u3_rest.src, relay, 2).start()

    def pass_on():
        @pl.when(is_relay)
        def _():
            to_relay(RELAY, T_RELAY, relay, relay, -2).wait_recv()
            to_relay(RELAY, T_U3, relay, u3_rest.dst, -1).start()

    tiles(EARLY, 0, 4).wait_recv()
    for j in range(chunks):
        cc = c[:, at(j)]
        dd = 1.0 / (1.0 + 4.0 * cc)
        dd2 = 1.0 / (1.0 + 8.0 * cc)
        d[:, at(j)], w[:, at(j)] = dd, cc * dd
        dk[:, at(j)], wk[:, at(j)] = dd2, 2.0 * cc * dd2
    a_q.start()

    def local_step(i):
        n = steps - i
        odd = lax.rem(i, 2) == 1

        @pl.when(jnp.logical_and(odd, i < steps - 3))
        def _():
            tiles(EARLY, i + 1, 4).wait_recv()

        @pl.when(i == steps - 3)
        def _():
            tiles(EARLY, i + 1, 5).wait_recv()

        @pl.when(i == 3)
        def _():
            a_e0.start()
        first_sweep(g, n)
        second_sweep(g, e, n, u1, w, damping)

        @pl.when(jnp.logical_and(lax.rem(i, 2) == 0, i > 0))
        def _():
            m = half + 1 - i // 2
            restrict(m)
            second_sweep(None, er, m, c0, wk, damping)

    each(0, steps - 1, local_step)

    @pl.when(jnp.logical_not(has_before))
    def _():
        start_g.wait()
        start_u.wait()
    a_guess.wait_recv()
    f_guess = within(0, g, slice(0, 1))
    f_guess.start()
    sweep_one(3, half + 1)
    each(4, half + 1, lambda m: coarse_defect(c1, m))
    a_e1.start()
    each(4, half + 1, lambda m: second_sweep(c1, ec, m, c2, wk, damping, inner=True))
    f_guess.wait_recv()
    each(1, 2, lambda n: first_sweep(g, n))
    a_e2.start()
    each(1, 2, lambda n: second_sweep(g, e, n, u1, w, damping))
    a_q.wait_recv()
    f_q = within(1, s, slice(0, 1))
    f_q.start()
    f_q.wait_recv()
    each(0, 1, lambda n: first_sweep(g, n, has_prev=False))
    damp0 = jnp.where(has_before, damping, 0.0).astype(jnp.float32)
    each(0, 1, lambda n: second_sweep(g, e, n, u1, w, damp0))
    each(1, 2, restrict)
    each(1, 2, lambda m: second_sweep(None, er, m, c0, wk, damping))
    sweep_one(2, 3)
    sweep_two(3, 4)
    x_late = within(0, c2, slice(3, half + 1))
    x_late.start()
    a_e0.wait_recv()
    f_e0 = within(2, c0, slice(0, 1))
    f_e0.start()
    x_late.wait_recv()
    each(half, half + 1, prolong)
    each(steps, steps + 1, lambda n: first_sweep(u2, n))
    each(steps, steps + 1, lambda n: second_sweep(u2, e, n, u3, w, damping))

    a_e1.rim.wait_recv()
    f_e1 = within(3, c1, slice(0, 1))
    f_e1.start()
    f_e0.wait_recv()
    each(1, 2, lambda m: coarse_defect(c0, m))
    start_u3()
    each(1, 2, lambda m: second_sweep(c0, ec, m, c1, wk, damping))
    sweep_two(2, 3)
    x_mid = within(1, c2, slice(2, 3))
    x_mid.start()
    for j in range(chunks):
        u2[steps - 2, :, at(j)] = u1[steps - 2, :, at(j)] + c2[half - 1, :, at(j)]
    each(steps - 1, steps, lambda n: first_sweep(u2, n))
    each(steps - 1, steps, lambda n: second_sweep(u2, e, n, u3, w, damping))
    each(steps, steps + 1, last_residual)
    a_e1.rest.wait_recv()
    f_e1.wait_recv()
    sweep_two(1, 2)
    x_early = within(0, c2, slice(1, 2))
    x_early.start()
    x_mid.wait_recv()
    each(3, half, prolong)
    for j in range(chunks):
        u2[4, :, at(j)] = u1[4, :, at(j)] + c2[2, :, at(j)]
    each(5, steps - 1, lambda n: first_sweep(u2, n))
    each(5, steps - 1, lambda n: second_sweep(u2, e, n, u3, w, damping))
    pass_on()
    a_e2.rim.wait_recv()
    f_e2 = within(2, c2, slice(0, 1))
    f_e2.start()
    each(6, steps, last_residual)
    x_early.wait_recv()
    for j in range(chunks):
        u2[2, :, at(j)] = u1[2, :, at(j)] + c2[1, :, at(j)]
        u2[3, :, at(j)] = u1[3, :, at(j)] + 0.5 * (c2[1, :, at(j)] + c2[2, :, at(j)])
    each(3, 5, lambda n: first_sweep(u2, n))
    each(3, 5, lambda n: second_sweep(u2, e, n, u3, w, damping))
    each(4, 6, last_residual)
    a_e2.rest.wait_recv()
    f_e2.wait_recv()
    for j in range(chunks):
        u2[0, :, at(j)] = u1[0, :, at(j)] + c2[0, :, at(j)]
        u2[1, :, at(j)] = u1[1, :, at(j)] + 0.5 * (c2[0, :, at(j)] + c2[1, :, at(j)])
    each(1, 3, lambda n: first_sweep(u2, n))
    each(1, 3, lambda n: second_sweep(u2, e, n, u3, w, damping))
    each(2, 4, last_residual)
    each(1, 2, lambda n: last_residual(n, has_prev=False))
    tiles(EARLY, 0, 2 * steps).wait_send()
    tiles(SPACE, 0, half + 6).wait_send()
    Along(T_U3, s.at[0:PLANES, mid], s.at[0:PLANES, mid]).wait_send()

    @pl.when(is_relay)
    def _():
        to_relay(RELAY, T_U3, relay, u3_rest.dst, -1).wait_send()
    a_u3.wait_recv()
    rbuf[0] = rbuf[0] + fu[...]


def store(u3, rbuf, u_out, r_out, sem):
    steps, rows, _ = u_out.shape
    copies = [
        pltpu.make_async_copy(u3.at[1 : steps + 1, HALO : HALO + rows], u_out, sem.at[0]),
        pltpu.make_async_copy(rbuf, r_out, sem.at[1]),
    ]
    for copy in copies:
        copy.start()
    for copy in copies:
        copy.wait()


def solution(mesh):
    tms, spaces = mesh.shape["tm"], mesh.shape["space"]

    def shards(source, guess, start_state, conduct):
        steps, rows, cols = source.shape
        full, half = rows + 2 * HALO, steps // 2

        def buf(*lead):
            return pltpu.VMEM(lead + (full, cols), jnp.float32)

        fields = pl.pallas_call(
            functools.partial(kernel, tms, spaces),
            out_shape=(buf(steps + 1), pltpu.VMEM(source.shape, jnp.float32)),
            in_specs=[pl.BlockSpec(memory_space=pltpu.HBM)] * 4,
            out_specs=[pl.BlockSpec(memory_space=pltpu.VMEM)] * 2,
            scratch_shapes=[
                buf(steps + 1), buf(steps + 1), buf(), buf(), buf(), buf(), buf(),
                buf(steps + 1), buf(steps + 1), buf(half + 1), buf(half + 1),
                buf(half + 1), buf(half + 1), buf(half + 1), buf(steps + 1),
                pltpu.VMEM((rows, cols), jnp.float32),
                pltpu.VMEM((rows, cols), jnp.float32),
                pltpu.VMEM((RELAYED, cols), jnp.float32),
                pltpu.SemaphoreType.DMA((6,)),
                pltpu.SemaphoreType.DMA((steps + 2 * SETS + PARTS,)),
            ],
            compiler_params=pltpu.CompilerParams(
                collective_id=0, has_side_effects=True, vmem_limit_bytes=59 * 1024 * 1024),
        )(source, guess, start_state, conduct)
        return pl.pallas_call(
            store,
            out_shape=(jax.ShapeDtypeStruct(source.shape, jnp.float32),) * 2,
            in_specs=[pl.BlockSpec(memory_space=pltpu.VMEM)] * 2,
            out_specs=[pl.BlockSpec(memory_space=pl.ANY)] * 2,
            scratch_shapes=[pltpu.SemaphoreType.DMA((2,))],
            compiler_params=pltpu.CompilerParams(vmem_limit_bytes=8 * 1024 * 1024),
        )(*fields)

    return jax.shard_map(
        shards,
        mesh=mesh,
        in_specs=(P("tm", "space", None), P("tm", "space", None), P("space", None), P("space", None)),
        out_specs=(P("tm", "space", None), P("tm", "space", None)),
        check_vma=False,
    )
```

```python
import functools

import jax
import jax.numpy as jnp
from jax import lax
from jax.experimental import pallas as pl
from jax.experimental.pallas import tpu as pltpu
from jax.sharding import PartitionSpec as P

damping = 0.8
MESH = pl.DeviceIdType.MESH
HALO = 8
LANES = 128

EARLY, SPACE, ALONG, RELAY = 0, 2, 4, 5
T_GUESS, T_Q, T_E0, T_E1_RIM, T_E1, T_E2_RIM, T_E2, T_U3, T_RELAY = range(9)
SETS, PLANES, PARTS = 4, 6, 9
RELAYED = 2 * HALO


def kernel(
    tms, spaces, src_hbm, guess_hbm, start_hbm, cond_hbm, u3, rbuf,
    g, s, c, d, w, dk, wk, e, u1, er, ec, c0, c1, c2, u2, qbuf, fu,
    relay, send_sem, recv_sem, ready,
):
    t = lax.axis_index("tm")
    z = lax.axis_index("space")
    has_up, has_dn = z > 0, z < spaces - 1
    has_before, has_after = t > 0, t < tms - 1
    by_relay = jnp.logical_and(lax.rem(t, 2) == 1, t + 2 < tms)
    is_relay = jnp.logical_and(lax.rem(t, 2) == 1, t > 2)
    from_relay = jnp.logical_and(lax.rem(t, 2) == 0, jnp.logical_and(t > 0, t + 1 < tms))
    odd_row = lax.rem(z, 2) == 1
    even_row = jnp.logical_not(odd_row)

    def count(*flags):
        return sum(jnp.where(flag, 1, 0) for flag in flags)
    steps, rows, cols = src_hbm.shape
    half = steps // 2
    full = rows + 2 * HALO
    mid = slice(HALO, HALO + rows)
    top, bot = slice(0, HALO), slice(HALO + rows, full)
    top_in, bot_in = slice(HALO, 2 * HALO), slice(rows, HALO + rows)
    chunks = cols // LANES
    later = slice(1, steps + 1)

    def remote(src, dst, sent, k, dev):
        return pltpu.make_async_remote_copy(
            src_ref=src, dst_ref=dst, send_sem=send_sem.at[sent], recv_sem=recv_sem.at[k],
            device_id=dev, device_id_type=MESH)

    up, dn = {"space": z - 1}, {"space": z + 1}
    first_set = 2 * half
    first_plane = first_set + 2 * SETS

    class Edge:
        def __init__(self, sent, k, first, last, halo_top, halo_bot):
            self.sent, self.k, self.first, self.last, self.top, self.bot = sent, k, first, last, halo_top, halo_bot

        def start(self):
            @pl.when(has_up)
            def _():
                remote(self.first, self.bot, self.sent, self.k, up).start()

            @pl.when(has_dn)
            def _():
                remote(self.last, self.top, self.sent + 1, self.k + 1, dn).start()

        def wait_recv(self):
            @pl.when(has_dn)
            def _():
                remote(self.first, self.bot, self.sent, self.k, dn).wait_recv()

            @pl.when(has_up)
            def _():
                remote(self.last, self.top, self.sent + 1, self.k + 1, up).wait_recv()

        def wait_send(self):
            @pl.when(has_up)
            def _():
                remote(self.first, self.bot, self.sent, self.k, up).wait_send()

            @pl.when(has_dn)
            def _():
                remote(self.last, self.top, self.sent + 1, self.k + 1, dn).wait_send()

    class Along:
        def __init__(self, k, src, dst):
            self.k, self.src, self.dst = first_plane + k, src, dst

        def start(self):
            @pl.when(has_after)
            def _():
                remote(self.src, self.dst, ALONG, self.k, {"tm": t + 1}).start()

        def wait_recv(self):
            @pl.when(has_before)
            def _():
                remote(self.src, self.dst, ALONG, self.k, {"tm": t - 1}).wait_recv()

        def wait_send(self):
            @pl.when(has_after)
            def _():
                remote(self.src, self.dst, ALONG, self.k, {"tm": t + 1}).wait_send()

    class Split:
        def __init__(self, k, ref):
            def part(k, rows_of):
                return Along(k, ref.at[half, rows_of], ref.at[0, rows_of])
            self.rim = Along(k, s.at[0, 0 : 2 * HALO], s.at[0, 0 : 2 * HALO])
            self.rest = part(k + 1, slice(2 * HALO, rows))
            self.parts = [part(k, top_in), part(k, bot_in), self.rest]

        def start(self):
            for part in self.parts:
                part.start()

    def within(turn, ref, sl):
        return Edge(SPACE, first_set + 2 * turn, ref.at[sl, top_in], ref.at[sl, bot_in], ref.at[sl, top], ref.at[sl, bot])

    def tiles(sent, k, count):
        ref = s.at[0:1, 0 : count * HALO] if count * HALO <= full else s.at[0:2, 0 : count * HALO // 2]
        return Edge(sent, k, ref, ref, ref, ref)

    barrier = pltpu.get_barrier_semaphore()
    greeted = (
        (has_before, {"tm": t - 1}), (is_relay, {"tm": t - 2}), (from_relay, {"tm": t + 1}),
        (jnp.logical_and(odd_row, has_up), up), (jnp.logical_and(odd_row, has_dn), dn))
    for flag, dev in greeted:
        @pl.when(flag)
        def _(dev=dev):
            pl.semaphore_signal(barrier, inc=1, device_id=dev, device_id_type=MESH)

    last_guess = pltpu.make_async_copy(guess_hbm.at[steps - 1], g.at[steps, mid], send_sem.at[ALONG])
    last_guess.start()
    loads = [
        pltpu.make_async_copy(cond_hbm, c.at[mid], recv_sem.at[first_plane - 1]),
        pltpu.make_async_copy(src_hbm, s.at[later, mid], recv_sem.at[first_plane - 2]),
        pltpu.make_async_copy(guess_hbm.at[0 : steps - 1], g.at[1:steps, mid], recv_sem.at[first_plane - 3]),
    ]
    for load in loads:
        load.start()
    start_g = pltpu.make_async_copy(start_hbm, g.at[0, mid], recv_sem.at[first_plane + T_GUESS])
    start_u = pltpu.make_async_copy(start_hbm, fu, recv_sem.at[first_plane + T_U3])

    @pl.when(jnp.logical_not(has_before))
    def _():
        start_g.start()
        start_u.start()
        s[0, mid] = jnp.zeros((rows, cols), jnp.float32)
        for ref in (c0, c1, c2):
            ref[0, mid] = jnp.zeros((rows, cols), jnp.float32)

    for flag, edge in ((has_up, top), (has_dn, bot)):
        @pl.when(jnp.logical_not(flag))
        def _(edge=edge):
            c[edge] = jnp.zeros((HALO, cols), jnp.float32)
            for ref in (g, s, c0, c1, c2):
                if ref is g or ref is s or ref is c2:
                    ref[:, edge] = jnp.zeros((ref.shape[0], HALO, cols), jnp.float32)
                else:
                    ref[0, edge] = jnp.zeros((HALO, cols), jnp.float32)

    rows_beside = count(has_up, has_dn)
    greetings = count(has_after, by_relay, is_relay) + jnp.where(even_row, rows_beside, 0)

    @pl.when(greetings > 0)
    def _():
        pl.semaphore_wait(barrier, greetings)
    for flag, dev in ((has_up, up), (has_dn, dn)):
        @pl.when(jnp.logical_and(even_row, flag))
        def _(dev=dev):
            pl.semaphore_signal(ready, inc=1, device_id=dev, device_id_type=MESH)

    a_guess = Along(T_GUESS, g.at[steps, mid], g.at[0, mid])
    last_guess.wait()
    a_guess.start()

    @pl.when(jnp.logical_and(odd_row, rows_beside > 0))
    def _():
        pl.semaphore_wait(ready, rows_beside)

    def halo(group, n, hbm, ref):
        Edge(EARLY, 2 * group, hbm.at[n - 1, 0:HALO], hbm.at[n - 1, rows - HALO : rows], ref.at[n, top], ref.at[n, bot]).start()

    Edge(SPACE, 0, cond_hbm.at[0:HALO], cond_hbm.at[rows - HALO : rows], c.at[top], c.at[bot]).start()
    halo(0, steps, guess_hbm, g)
    for i in range(steps - 1):
        n = steps - i
        halo((i + 1) // 2, n - 1, guess_hbm, g)
        halo((i + 1) // 2, n, src_hbm, s)
    halo(half - 1, 1, src_hbm, s)
    for load in loads:
        load.wait()

    lane = lax.broadcasted_iota(jnp.int32, (full, LANES), 1)
    is_first, is_last = lane == 0, lane == LANES - 1

    def at(j):
        return slice(j * LANES, (j + 1) * LANES)

    def each(low, high, body):
        def step(i, carry):
            body(i)
            return carry
        lax.fori_loop(low, high, step, 0)

    def stencil(get, put):
        zero = jnp.zeros((full, LANES), jnp.float32)
        before, now = zero, get(0)
        for j in range(chunks):
            after = get(j + 1) if j + 1 < chunks else zero
            left = pltpu.roll(jnp.where(is_last, before, now), 1, 1)
            right = pltpu.roll(jnp.where(is_first, after, now), LANES - 1, 1)
            rim = (left + right) + (pltpu.roll(now, 1, 0) + pltpu.roll(now, full - 1, 0))
            put(j, now, rim)
            before, now = now, after

    def first_sweep(field, n, has_prev=True):
        def put(j, now, rim):
            drive = s[n, :, at(j)]
            if has_prev:
                drive = drive + field[n - 1, :, at(j)]
            e[n, :, at(j)] = d[:, at(j)] * drive + w[:, at(j)] * rim - now
        stencil(lambda j: field[n, :, at(j)], put)

    def second_sweep(field, errs, n, dst, weight, damp, inner=False):
        def put(j, now, rim):
            gain = damp * (now + weight[:, at(j)] * rim)
            if inner:
                dst[n, mid, at(j)] = field[n, mid, at(j)] + gain[mid]
            elif field is None:
                dst[n, :, at(j)] = gain
            else:
                dst[n, :, at(j)] = field[n, :, at(j)] + gain
        stencil(lambda j: errs[n, :, at(j)], put)

    def restrict(m):
        a, b = 2 * m - 1, 2 * m

        def put(j, now, rim):
            cc = c[:, at(j)]
            drive = (s[a, :, at(j)] + s[b, :, at(j)]) + (u1[a - 1, :, at(j)] + u1[a, :, at(j)])
            er[m, :, at(j)] = dk[:, at(j)] * (drive - now + cc * (rim - 4.0 * now))
        stencil(lambda j: u1[a, :, at(j)] + u1[b, :, at(j)], put)

    def coarse_defect(field, m):
        def put(j, now, rim):
            ec[m, :, at(j)] = er[m, :, at(j)] + dk[:, at(j)] * field[m - 1, :, at(j)] + wk[:, at(j)] * rim - now
        stencil(lambda j: field[m, :, at(j)], put)

    def sweep_one(low, high):
        each(low, high, lambda m: coarse_defect(c0, m))
        each(low, high, lambda m: second_sweep(c0, ec, m, c1, wk, damping))

    def sweep_two(low, high):
        each(low, high, lambda m: coarse_defect(c1, m))
        each(low, high, lambda m: second_sweep(c1, ec, m, c2, wk, damping, inner=True))

    def prolong(m):
        for j in range(chunks):
            u2[2 * m, :, at(j)] = u1[2 * m, :, at(j)] + c2[m, :, at(j)]
            u2[2 * m - 1, :, at(j)] = u1[2 * m - 1, :, at(j)] + 0.5 * (c2[m - 1, :, at(j)] + c2[m, :, at(j)])

    def last_residual(n, has_prev=True):
        def put(j, now, rim):
            flow = c[:, at(j)] * (rim - 4.0 * now) - now
            drive = s[n, mid, at(j)]
            if has_prev:
                drive = drive + u3[n - 1, mid, at(j)]
            rbuf[n - 1, :, at(j)] = flow[mid] + drive
        stencil(lambda j: u3[n, :, at(j)], put)

    for j in range(chunks):
        qbuf[:, at(j)] = s[steps, mid, at(j)] + g[steps - 1, mid, at(j)]
    a_q = Along(T_Q, qbuf, s.at[0, mid])
    a_e0 = Along(T_E0, c0.at[half, mid], c0.at[0, mid])
    a_e1 = Split(T_E1_RIM, c1)
    a_e2 = Split(T_E2_RIM, c2)
    a_u3 = Along(T_U3, fu, fu)
    kept = rows - RELAYED
    u3_kept = Along(T_U3, u3.at[steps, HALO : HALO + kept], fu.at[0:kept])
    u3_rest = Along(T_U3, u3.at[steps, HALO + kept : HALO + rows], fu.at[kept:rows])

    def to_relay(sent, k, src, dst, step):
        return remote(src, dst, sent, first_plane + k, {"tm": t + step})

    def start_u3():
        u3_kept.start()

        @pl.when(jnp.logical_not(by_relay))
        def _():
            u3_rest.start()

        @pl.when(by_relay)
        def _():
            to_relay(ALONG, T_RELAY, u3_rest.src, relay, 2).start()

    def pass_on():
        @pl.when(is_relay)
        def _():
            to_relay(RELAY, T_RELAY, relay, relay, -2).wait_recv()
            to_relay(RELAY, T_U3, relay, u3_rest.dst, -1).start()

    def coefficients(part):
        for j in range(chunks):
            cc = c[part, at(j)]
            dd = 1.0 / (1.0 + 4.0 * cc)
            dd2 = 1.0 / (1.0 + 8.0 * cc)
            d[part, at(j)], w[part, at(j)] = dd, cc * dd
            dk[part, at(j)], wk[part, at(j)] = dd2, 2.0 * cc * dd2

    coefficients(mid)
    a_q.start()
    tiles(EARLY, 0, 4).wait_recv()
    coefficients(top)
    coefficients(bot)

    def local_step(i):
        n = steps - i
        odd = lax.rem(i, 2) == 1

        @pl.when(jnp.logical_and(odd, i < steps - 3))
        def _():
            tiles(EARLY, i + 1, 4).wait_recv()

        @pl.when(i == steps - 3)
        def _():
            tiles(EARLY, i + 1, 5).wait_recv()

        @pl.when(i == 3)
        def _():
            a_e0.start()
        first_sweep(g, n)
        second_sweep(g, e, n, u1, w, damping)

        @pl.when(jnp.logical_and(lax.rem(i, 2) == 0, i > 0))
        def _():
            m = half + 1 - i // 2
            restrict(m)
            second_sweep(None, er, m, c0, wk, damping)

    each(0, steps - 1, local_step)

    @pl.when(jnp.logical_not(has_before))
    def _():
        start_g.wait()
        start_u.wait()
    a_guess.wait_recv()
    f_guess = within(0, g, slice(0, 1))
    f_guess.start()
    sweep_one(3, half + 1)
    each(4, half + 1, lambda m: coarse_defect(c1, m))
    a_e1.start()
    each(4, half + 1, lambda m: second_sweep(c1, ec, m, c2, wk, damping, inner=True))
    f_guess.wait_recv()
    each(1, 2, lambda n: first_sweep(g, n))
    a_e2.start()
    each(1, 2, lambda n: second_sweep(g, e, n, u1, w, damping))
    a_q.wait_recv()
    f_q = within(1, s, slice(0, 1))
    f_q.start()
    f_q.wait_recv()
    each(0, 1, lambda n: first_sweep(g, n, has_prev=False))
    damp0 = jnp.where(has_before, damping, 0.0).astype(jnp.float32)
    each(0, 1, lambda n: second_sweep(g, e, n, u1, w, damp0))
    each(1, 2, restrict)
    each(1, 2, lambda m: second_sweep(None, er, m, c0, wk, damping))
    sweep_one(2, 3)
    sweep_two(3, 4)
    x_late = within(0, c2, slice(3, half + 1))
    x_late.start()
    a_e0.wait_recv()
    f_e0 = within(2, c0, slice(0, 1))
    f_e0.start()
    x_late.wait_recv()
    each(half, half + 1, prolong)
    each(steps, steps + 1, lambda n: first_sweep(u2, n))
    each(steps, steps + 1, lambda n: second_sweep(u2, e, n, u3, w, damping))

    a_e1.rim.wait_recv()
    f_e1 = within(3, c1, slice(0, 1))
    f_e1.start()
    f_e0.wait_recv()
    each(1, 2, lambda m: coarse_defect(c0, m))
    start_u3()
    each(1, 2, lambda m: second_sweep(c0, ec, m, c1, wk, damping))
    sweep_two(2, 3)
    x_mid = within(1, c2, slice(2, 3))
    x_mid.start()
    for j in range(chunks):
        u2[steps - 2, :, at(j)] = u1[steps - 2, :, at(j)] + c2[half - 1, :, at(j)]
    each(steps - 1, steps, lambda n: first_sweep(u2, n))
    each(steps - 1, steps, lambda n: second_sweep(u2, e, n, u3, w, damping))
    each(steps, steps + 1, last_residual)
    a_e1.rest.wait_recv()
    f_e1.wait_recv()
    sweep_two(1, 2)
    x_early = within(0, c2, slice(1, 2))
    x_early.start()
    x_mid.wait_recv()
    each(3, half, prolong)
    for j in range(chunks):
        u2[4, :, at(j)] = u1[4, :, at(j)] + c2[2, :, at(j)]
    each(5, steps - 1, lambda n: first_sweep(u2, n))
    each(5, steps - 1, lambda n: second_sweep(u2, e, n, u3, w, damping))
    pass_on()
    a_e2.rim.wait_recv()
    f_e2 = within(2, c2, slice(0, 1))
    f_e2.start()
    each(6, steps, last_residual)
    x_early.wait_recv()
    for j in range(chunks):
        u2[2, :, at(j)] = u1[2, :, at(j)] + c2[1, :, at(j)]
        u2[3, :, at(j)] = u1[3, :, at(j)] + 0.5 * (c2[1, :, at(j)] + c2[2, :, at(j)])
    each(3, 5, lambda n: first_sweep(u2, n))
    each(3, 5, lambda n: second_sweep(u2, e, n, u3, w, damping))
    each(4, 6, last_residual)
    a_e2.rest.wait_recv()
    f_e2.wait_recv()
    for j in range(chunks):
        u2[0, :, at(j)] = u1[0, :, at(j)] + c2[0, :, at(j)]
        u2[1, :, at(j)] = u1[1, :, at(j)] + 0.5 * (c2[0, :, at(j)] + c2[1, :, at(j)])
    each(1, 3, lambda n: first_sweep(u2, n))
    each(1, 3, lambda n: second_sweep(u2, e, n, u3, w, damping))
    each(2, 4, last_residual)
    each(1, 2, lambda n: last_residual(n, has_prev=False))
    tiles(EARLY, 0, 2 * steps).wait_send()
    tiles(SPACE, 0, half + 6).wait_send()
    Along(T_U3, s.at[0:PLANES, mid], s.at[0:PLANES, mid]).wait_send()

    @pl.when(is_relay)
    def _():
        to_relay(RELAY, T_U3, relay, u3_rest.dst, -1).wait_send()
    a_u3.wait_recv()
    rbuf[0] = rbuf[0] + fu[...]


def store(u3, rbuf, u_out, r_out, sem):
    steps, rows, _ = u_out.shape
    copies = [
        pltpu.make_async_copy(u3.at[1 : steps + 1, HALO : HALO + rows], u_out, sem.at[0]),
        pltpu.make_async_copy(rbuf, r_out, sem.at[1]),
    ]
    for copy in copies:
        copy.start()
    for copy in copies:
        copy.wait()


def solution(mesh):
    tms, spaces = mesh.shape["tm"], mesh.shape["space"]

    def shards(source, guess, start_state, conduct):
        steps, rows, cols = source.shape
        full, half = rows + 2 * HALO, steps // 2

        def buf(*lead):
            return pltpu.VMEM(lead + (full, cols), jnp.float32)

        fields = pl.pallas_call(
            functools.partial(kernel, tms, spaces),
            out_shape=(buf(steps + 1), pltpu.VMEM(source.shape, jnp.float32)),
            in_specs=[pl.BlockSpec(memory_space=pltpu.HBM)] * 4,
            out_specs=[pl.BlockSpec(memory_space=pltpu.VMEM)] * 2,
            scratch_shapes=[
                buf(steps + 1), buf(steps + 1), buf(), buf(), buf(), buf(), buf(),
                buf(steps + 1), buf(steps + 1), buf(half + 1), buf(half + 1),
                buf(half + 1), buf(half + 1), buf(half + 1), buf(steps + 1),
                pltpu.VMEM((rows, cols), jnp.float32),
                pltpu.VMEM((rows, cols), jnp.float32),
                pltpu.VMEM((RELAYED, cols), jnp.float32),
                pltpu.SemaphoreType.DMA((6,)),
                pltpu.SemaphoreType.DMA((steps + 2 * SETS + PARTS,)),
                pltpu.SemaphoreType.REGULAR,
            ],
            compiler_params=pltpu.CompilerParams(
                collective_id=0, has_side_effects=True, vmem_limit_bytes=59 * 1024 * 1024),
        )(source, guess, start_state, conduct)
        return pl.pallas_call(
            store,
            out_shape=(jax.ShapeDtypeStruct(source.shape, jnp.float32),) * 2,
            in_specs=[pl.BlockSpec(memory_space=pltpu.VMEM)] * 2,
            out_specs=[pl.BlockSpec(memory_space=pl.ANY)] * 2,
            scratch_shapes=[pltpu.SemaphoreType.DMA((2,))],
            compiler_params=pltpu.CompilerParams(vmem_limit_bytes=8 * 1024 * 1024),
        )(*fields)

    return jax.shard_map(
        shards,
        mesh=mesh,
        in_specs=(P("tm", "space", None), P("tm", "space", None), P("space", None), P("space", None)),
        out_specs=(P("tm", "space", None), P("tm", "space", None)),
        check_vma=False,
    )
```

```python
import functools

import jax
import jax.numpy as jnp
from jax import lax
from jax.experimental import pallas as pl
from jax.experimental.pallas import tpu as pltpu
from jax.sharding import PartitionSpec as P

damping = 0.8
MESH = pl.DeviceIdType.MESH
HALO = 8
LANES = 128

EARLY, SPACE, ALONG, RELAY = range(4)
T_GUESS, T_Q, T_E0, T_E1_RIM, T_E1, T_E2_RIM, T_E2, T_U3, T_RELAY = range(9)
SETS, PLANES, PARTS = 4, 6, 9
RELAYED = 2 * HALO


def kernel(
    tms, spaces, src_hbm, guess_hbm, start_hbm, cond_hbm, u3, rbuf,
    g, s, c, d, w, dk, wk, e, u1, er, ec, c0, c1, c2, u2, qbuf, fu,
    relay, send_sem, recv_sem, ready,
):
    t = lax.axis_index("tm")
    z = lax.axis_index("space")
    has_up, has_dn = z > 0, z < spaces - 1
    has_before, has_after = t > 0, t < tms - 1
    by_relay = jnp.logical_and(lax.rem(t, 2) == 1, t + 2 < tms)
    is_relay = jnp.logical_and(lax.rem(t, 2) == 1, t > 2)
    from_relay = jnp.logical_and(lax.rem(t, 2) == 0, jnp.logical_and(t > 0, t + 1 < tms))
    odd_row = lax.rem(z, 2) == 1
    even_row = jnp.logical_not(odd_row)

    def count(*flags):
        return sum(jnp.where(flag, 1, 0) for flag in flags)
    steps, rows, cols = src_hbm.shape
    half = steps // 2
    full = rows + 2 * HALO
    mid = slice(HALO, HALO + rows)
    top, bot = slice(0, HALO), slice(HALO + rows, full)
    top_in, bot_in = slice(HALO, 2 * HALO), slice(rows, HALO + rows)
    chunks = cols // LANES
    later = slice(1, steps + 1)

    def remote(src, dst, sent, k, dev):
        return pltpu.make_async_remote_copy(
            src_ref=src, dst_ref=dst, send_sem=send_sem.at[sent], recv_sem=recv_sem.at[k],
            device_id=dev, device_id_type=MESH)

    up, dn = {"space": z - 1}, {"space": z + 1}
    first_set = half
    first_plane = first_set + SETS
    rows_beside = count(has_up, has_dn)
    beside = {"space": jnp.where(has_up, z - 1, z + 1)}

    class Tiles:
        def __init__(self, sent, k, n):
            self.sent, self.k, self.n = sent, k, n

        def each_count(self, wait):
            for beside_count in (1, 2):
                @pl.when(rows_beside == beside_count)
                def _(n=self.n * beside_count):
                    planes = next(p for p in range(1, steps + 1) if n % p == 0 and n // p * HALO <= full)
                    ref = s.at[0:planes, 0 : n // planes * HALO]
                    wait(remote(ref, ref, self.sent, self.k, beside))

        def wait_recv(self):
            self.each_count(lambda copy: copy.wait_recv())

        def wait_send(self):
            self.each_count(lambda copy: copy.wait_send())

    class Edge(Tiles):
        def __init__(self, sent, k, first, last, halo_top, halo_bot, n=1):
            super().__init__(sent, k, n)
            self.first, self.last, self.top, self.bot = first, last, halo_top, halo_bot

        def start(self):
            @pl.when(has_up)
            def _():
                remote(self.first, self.bot, self.sent, self.k, up).start()

            @pl.when(has_dn)
            def _():
                remote(self.last, self.top, self.sent, self.k, dn).start()

    class Along:
        def __init__(self, k, src, dst):
            self.k, self.src, self.dst = first_plane + k, src, dst

        def start(self):
            @pl.when(has_after)
            def _():
                remote(self.src, self.dst, ALONG, self.k, {"tm": t + 1}).start()

        def wait_recv(self):
            @pl.when(has_before)
            def _():
                remote(self.src, self.dst, ALONG, self.k, {"tm": t - 1}).wait_recv()

        def wait_send(self):
            @pl.when(has_after)
            def _():
                remote(self.src, self.dst, ALONG, self.k, {"tm": t + 1}).wait_send()

    class Split:
        def __init__(self, k, ref):
            def part(k, rows_of):
                return Along(k, ref.at[half, rows_of], ref.at[0, rows_of])
            self.rim = Along(k, s.at[0, 0 : 2 * HALO], s.at[0, 0 : 2 * HALO])
            self.rest = part(k + 1, slice(2 * HALO, rows))
            self.parts = [part(k, top_in), part(k, bot_in), self.rest]

        def start(self):
            for part in self.parts:
                part.start()

    def within(turn, ref, sl):
        return Edge(
            SPACE, first_set + turn, ref.at[sl, top_in], ref.at[sl, bot_in], ref.at[sl, top], ref.at[sl, bot],
            sl.stop - sl.start)

    barrier = pltpu.get_barrier_semaphore()
    greeted = (
        (has_before, {"tm": t - 1}), (is_relay, {"tm": t - 2}), (from_relay, {"tm": t + 1}),
        (jnp.logical_and(odd_row, has_up), up), (jnp.logical_and(odd_row, has_dn), dn))
    for flag, dev in greeted:
        @pl.when(flag)
        def _(dev=dev):
            pl.semaphore_signal(barrier, inc=1, device_id=dev, device_id_type=MESH)

    last_guess = pltpu.make_async_copy(guess_hbm.at[steps - 1], g.at[steps, mid], send_sem.at[ALONG])
    last_guess.start()
    loads = [
        pltpu.make_async_copy(cond_hbm, c.at[mid], recv_sem.at[first_plane - 1]),
        pltpu.make_async_copy(src_hbm, s.at[later, mid], recv_sem.at[first_plane - 2]),
        pltpu.make_async_copy(guess_hbm.at[0 : steps - 1], g.at[1:steps, mid], recv_sem.at[first_plane - 3]),
    ]
    for load in loads:
        load.start()
    start_g = pltpu.make_async_copy(start_hbm, g.at[0, mid], recv_sem.at[first_plane + T_GUESS])
    start_u = pltpu.make_async_copy(start_hbm, fu, recv_sem.at[first_plane + T_U3])

    @pl.when(jnp.logical_not(has_before))
    def _():
        start_g.start()
        start_u.start()
        s[0, mid] = jnp.zeros((rows, cols), jnp.float32)
        for ref in (c0, c1, c2):
            ref[0, mid] = jnp.zeros((rows, cols), jnp.float32)

    for flag, edge in ((has_up, top), (has_dn, bot)):
        @pl.when(jnp.logical_not(flag))
        def _(edge=edge):
            c[edge] = jnp.zeros((HALO, cols), jnp.float32)
            for ref in (g, s, c0, c1, c2):
                if ref is g or ref is s or ref is c2:
                    ref[:, edge] = jnp.zeros((ref.shape[0], HALO, cols), jnp.float32)
                else:
                    ref[0, edge] = jnp.zeros((HALO, cols), jnp.float32)

    greetings = count(has_after, by_relay, is_relay) + jnp.where(even_row, rows_beside, 0)

    @pl.when(greetings > 0)
    def _():
        pl.semaphore_wait(barrier, greetings)
    for flag, dev in ((has_up, up), (has_dn, dn)):
        @pl.when(jnp.logical_and(even_row, flag))
        def _(dev=dev):
            pl.semaphore_signal(ready, inc=1, device_id=dev, device_id_type=MESH)

    a_guess = Along(T_GUESS, g.at[steps, mid], g.at[0, mid])
    last_guess.wait()
    a_guess.start()

    @pl.when(jnp.logical_and(odd_row, rows_beside > 0))
    def _():
        pl.semaphore_wait(ready, rows_beside)

    def halo(group, n, hbm, ref):
        Edge(EARLY, group, hbm.at[n - 1, 0:HALO], hbm.at[n - 1, rows - HALO : rows], ref.at[n, top], ref.at[n, bot]).start()

    Edge(SPACE, 0, cond_hbm.at[0:HALO], cond_hbm.at[rows - HALO : rows], c.at[top], c.at[bot]).start()
    halo(0, steps, guess_hbm, g)
    for i in range(steps - 1):
        n = steps - i
        halo((i + 1) // 2, n - 1, guess_hbm, g)
        halo((i + 1) // 2, n, src_hbm, s)
    halo(half - 1, 1, src_hbm, s)
    for load in loads:
        load.wait()

    lane = lax.broadcasted_iota(jnp.int32, (full, LANES), 1)
    is_first, is_last = lane == 0, lane == LANES - 1

    def at(j):
        return slice(j * LANES, (j + 1) * LANES)

    def each(low, high, body):
        def step(i, carry):
            body(i)
            return carry
        lax.fori_loop(low, high, step, 0)

    def stencil(get, put):
        zero = jnp.zeros((full, LANES), jnp.float32)
        before, now = zero, get(0)
        for j in range(chunks):
            after = get(j + 1) if j + 1 < chunks else zero
            left = pltpu.roll(jnp.where(is_last, before, now), 1, 1)
            right = pltpu.roll(jnp.where(is_first, after, now), LANES - 1, 1)
            rim = (left + right) + (pltpu.roll(now, 1, 0) + pltpu.roll(now, full - 1, 0))
            put(j, now, rim)
            before, now = now, after

    def first_sweep(field, n, has_prev=True):
        def put(j, now, rim):
            drive = s[n, :, at(j)]
            if has_prev:
                drive = drive + field[n - 1, :, at(j)]
            e[n, :, at(j)] = d[:, at(j)] * drive + w[:, at(j)] * rim - now
        stencil(lambda j: field[n, :, at(j)], put)

    def second_sweep(field, errs, n, dst, weight, damp, inner=False):
        def put(j, now, rim):
            gain = damp * (now + weight[:, at(j)] * rim)
            if inner:
                dst[n, mid, at(j)] = field[n, mid, at(j)] + gain[mid]
            elif field is None:
                dst[n, :, at(j)] = gain
            else:
                dst[n, :, at(j)] = field[n, :, at(j)] + gain
        stencil(lambda j: errs[n, :, at(j)], put)

    def restrict(m):
        a, b = 2 * m - 1, 2 * m

        def put(j, now, rim):
            cc = c[:, at(j)]
            drive = (s[a, :, at(j)] + s[b, :, at(j)]) + (u1[a - 1, :, at(j)] + u1[a, :, at(j)])
            er[m, :, at(j)] = dk[:, at(j)] * (drive - now + cc * (rim - 4.0 * now))
        stencil(lambda j: u1[a, :, at(j)] + u1[b, :, at(j)], put)

    def coarse_defect(field, m):
        def put(j, now, rim):
            ec[m, :, at(j)] = er[m, :, at(j)] + dk[:, at(j)] * field[m - 1, :, at(j)] + wk[:, at(j)] * rim - now
        stencil(lambda j: field[m, :, at(j)], put)

    def sweep_one(low, high):
        each(low, high, lambda m: coarse_defect(c0, m))
        each(low, high, lambda m: second_sweep(c0, ec, m, c1, wk, damping))

    def sweep_two(low, high):
        each(low, high, lambda m: coarse_defect(c1, m))
        each(low, high, lambda m: second_sweep(c1, ec, m, c2, wk, damping, inner=True))

    def prolong(m):
        for j in range(chunks):
            u2[2 * m, :, at(j)] = u1[2 * m, :, at(j)] + c2[m, :, at(j)]
            u2[2 * m - 1, :, at(j)] = u1[2 * m - 1, :, at(j)] + 0.5 * (c2[m - 1, :, at(j)] + c2[m, :, at(j)])

    def last_residual(n, has_prev=True):
        def put(j, now, rim):
            flow = c[:, at(j)] * (rim - 4.0 * now) - now
            drive = s[n, mid, at(j)]
            if has_prev:
                drive = drive + u3[n - 1, mid, at(j)]
            rbuf[n - 1, :, at(j)] = flow[mid] + drive
        stencil(lambda j: u3[n, :, at(j)], put)

    for j in range(chunks):
        qbuf[:, at(j)] = s[steps, mid, at(j)] + g[steps - 1, mid, at(j)]
    a_q = Along(T_Q, qbuf, s.at[0, mid])
    a_e0 = Along(T_E0, c0.at[half, mid], c0.at[0, mid])
    a_e1 = Split(T_E1_RIM, c1)
    a_e2 = Split(T_E2_RIM, c2)
    a_u3 = Along(T_U3, fu, fu)
    kept = rows - RELAYED
    u3_kept = Along(T_U3, u3.at[steps, HALO : HALO + kept], fu.at[0:kept])
    u3_rest = Along(T_U3, u3.at[steps, HALO + kept : HALO + rows], fu.at[kept:rows])

    def to_relay(sent, k, src, dst, step):
        return remote(src, dst, sent, first_plane + k, {"tm": t + step})

    def start_u3():
        u3_kept.start()

        @pl.when(jnp.logical_not(by_relay))
        def _():
            u3_rest.start()

        @pl.when(by_relay)
        def _():
            to_relay(ALONG, T_RELAY, u3_rest.src, relay, 2).start()

    def pass_on():
        @pl.when(is_relay)
        def _():
            to_relay(RELAY, T_RELAY, relay, relay, -2).wait_recv()
            to_relay(RELAY, T_U3, relay, u3_rest.dst, -1).start()

    def coefficients(part):
        for j in range(chunks):
            cc = c[part, at(j)]
            dd = 1.0 / (1.0 + 4.0 * cc)
            dd2 = 1.0 / (1.0 + 8.0 * cc)
            d[part, at(j)], w[part, at(j)] = dd, cc * dd
            dk[part, at(j)], wk[part, at(j)] = dd2, 2.0 * cc * dd2

    coefficients(mid)
    a_q.start()
    Tiles(EARLY, 0, 4).wait_recv()
    coefficients(top)
    coefficients(bot)

    def local_step(i):
        n = steps - i
        odd = lax.rem(i, 2) == 1

        @pl.when(jnp.logical_and(odd, i < steps - 3))
        def _():
            Tiles(EARLY, (i + 1) // 2, 4).wait_recv()

        @pl.when(i == steps - 3)
        def _():
            Tiles(EARLY, half - 1, 5).wait_recv()

        @pl.when(i == 3)
        def _():
            a_e0.start()
        first_sweep(g, n)
        second_sweep(g, e, n, u1, w, damping)

        @pl.when(jnp.logical_and(lax.rem(i, 2) == 0, i > 0))
        def _():
            m = half + 1 - i // 2
            restrict(m)
            second_sweep(None, er, m, c0, wk, damping)

    each(0, steps - 1, local_step)

    @pl.when(jnp.logical_not(has_before))
    def _():
        start_g.wait()
        start_u.wait()
    a_guess.wait_recv()
    f_guess = within(0, g, slice(0, 1))
    f_guess.start()
    sweep_one(3, half + 1)
    each(4, half + 1, lambda m: coarse_defect(c1, m))
    a_e1.start()
    each(4, half + 1, lambda m: second_sweep(c1, ec, m, c2, wk, damping, inner=True))
    f_guess.wait_recv()
    each(1, 2, lambda n: first_sweep(g, n))
    a_e2.start()
    each(1, 2, lambda n: second_sweep(g, e, n, u1, w, damping))
    a_q.wait_recv()
    f_q = within(1, s, slice(0, 1))
    f_q.start()
    f_q.wait_recv()
    each(0, 1, lambda n: first_sweep(g, n, has_prev=False))
    damp0 = jnp.where(has_before, damping, 0.0).astype(jnp.float32)
    each(0, 1, lambda n: second_sweep(g, e, n, u1, w, damp0))
    each(1, 2, restrict)
    each(1, 2, lambda m: second_sweep(None, er, m, c0, wk, damping))
    sweep_one(2, 3)
    sweep_two(3, 4)
    x_late = within(0, c2, slice(3, half + 1))
    x_late.start()
    a_e0.wait_recv()
    f_e0 = within(2, c0, slice(0, 1))
    f_e0.start()
    x_late.wait_recv()
    each(half, half + 1, prolong)
    each(steps, steps + 1, lambda n: first_sweep(u2, n))
    each(steps, steps + 1, lambda n: second_sweep(u2, e, n, u3, w, damping))

    a_e1.rim.wait_recv()
    f_e1 = within(3, c1, slice(0, 1))
    f_e1.start()
    f_e0.wait_recv()
    each(1, 2, lambda m: coarse_defect(c0, m))
    start_u3()
    each(1, 2, lambda m: second_sweep(c0, ec, m, c1, wk, damping))
    sweep_two(2, 3)
    x_mid = within(1, c2, slice(2, 3))
    x_mid.start()
    for j in range(chunks):
        u2[steps - 2, :, at(j)] = u1[steps - 2, :, at(j)] + c2[half - 1, :, at(j)]
    each(steps - 1, steps, lambda n: first_sweep(u2, n))
    each(steps - 1, steps, lambda n: second_sweep(u2, e, n, u3, w, damping))
    each(steps, steps + 1, last_residual)
    a_e1.rest.wait_recv()
    f_e1.wait_recv()
    sweep_two(1, 2)
    x_early = within(0, c2, slice(1, 2))
    x_early.start()
    x_mid.wait_recv()
    each(3, half, prolong)
    for j in range(chunks):
        u2[4, :, at(j)] = u1[4, :, at(j)] + c2[2, :, at(j)]
    each(5, steps - 1, lambda n: first_sweep(u2, n))
    each(5, steps - 1, lambda n: second_sweep(u2, e, n, u3, w, damping))
    pass_on()
    a_e2.rim.wait_recv()
    f_e2 = within(2, c2, slice(0, 1))
    f_e2.start()
    each(6, steps, last_residual)
    x_early.wait_recv()
    for j in range(chunks):
        u2[2, :, at(j)] = u1[2, :, at(j)] + c2[1, :, at(j)]
        u2[3, :, at(j)] = u1[3, :, at(j)] + 0.5 * (c2[1, :, at(j)] + c2[2, :, at(j)])
    each(3, 5, lambda n: first_sweep(u2, n))
    each(3, 5, lambda n: second_sweep(u2, e, n, u3, w, damping))
    each(4, 6, last_residual)
    a_e2.rest.wait_recv()
    f_e2.wait_recv()
    for j in range(chunks):
        u2[0, :, at(j)] = u1[0, :, at(j)] + c2[0, :, at(j)]
        u2[1, :, at(j)] = u1[1, :, at(j)] + 0.5 * (c2[0, :, at(j)] + c2[1, :, at(j)])
    each(1, 3, lambda n: first_sweep(u2, n))
    each(1, 3, lambda n: second_sweep(u2, e, n, u3, w, damping))
    each(2, 4, last_residual)
    each(1, 2, lambda n: last_residual(n, has_prev=False))
    @pl.when(jnp.logical_not(has_before))
    def _():
        rbuf[0] = rbuf[0] + fu[...]
    Tiles(EARLY, 0, 2 * steps).wait_send()
    Tiles(SPACE, 0, half + 6).wait_send()
    Along(T_U3, s.at[0:PLANES, mid], s.at[0:PLANES, mid]).wait_send()

    @pl.when(is_relay)
    def _():
        to_relay(RELAY, T_U3, relay, u3_rest.dst, -1).wait_send()

    @pl.when(has_before)
    def _():
        a_u3.wait_recv()
        rbuf[0] = rbuf[0] + fu[...]


def store(u3, rbuf, u_out, r_out, sem):
    steps, rows, _ = u_out.shape
    copies = [
        pltpu.make_async_copy(u3.at[1 : steps + 1, HALO : HALO + rows], u_out, sem.at[0]),
        pltpu.make_async_copy(rbuf, r_out, sem.at[1]),
    ]
    for copy in copies:
        copy.start()
    for copy in copies:
        copy.wait()


def solution(mesh):
    tms, spaces = mesh.shape["tm"], mesh.shape["space"]

    def shards(source, guess, start_state, conduct):
        steps, rows, cols = source.shape
        full, half = rows + 2 * HALO, steps // 2

        def buf(*lead):
            return pltpu.VMEM(lead + (full, cols), jnp.float32)

        fields = pl.pallas_call(
            functools.partial(kernel, tms, spaces),
            out_shape=(buf(steps + 1), pltpu.VMEM(source.shape, jnp.float32)),
            in_specs=[pl.BlockSpec(memory_space=pltpu.HBM)] * 4,
            out_specs=[pl.BlockSpec(memory_space=pltpu.VMEM)] * 2,
            scratch_shapes=[
                buf(steps + 1), buf(steps + 1), buf(), buf(), buf(), buf(), buf(),
                buf(steps + 1), buf(steps + 1), buf(half + 1), buf(half + 1),
                buf(half + 1), buf(half + 1), buf(half + 1), buf(steps + 1),
                pltpu.VMEM((rows, cols), jnp.float32),
                pltpu.VMEM((rows, cols), jnp.float32),
                pltpu.VMEM((RELAYED, cols), jnp.float32),
                pltpu.SemaphoreType.DMA((4,)),
                pltpu.SemaphoreType.DMA((half + SETS + PARTS,)),
                pltpu.SemaphoreType.REGULAR,
            ],
            compiler_params=pltpu.CompilerParams(
                collective_id=0, has_side_effects=True, vmem_limit_bytes=59 * 1024 * 1024),
        )(source, guess, start_state, conduct)
        return pl.pallas_call(
            store,
            out_shape=(jax.ShapeDtypeStruct(source.shape, jnp.float32),) * 2,
            in_specs=[pl.BlockSpec(memory_space=pltpu.VMEM)] * 2,
            out_specs=[pl.BlockSpec(memory_space=pl.ANY)] * 2,
            scratch_shapes=[pltpu.SemaphoreType.DMA((2,))],
            compiler_params=pltpu.CompilerParams(vmem_limit_bytes=8 * 1024 * 1024),
        )(*fields)

    return jax.shard_map(
        shards,
        mesh=mesh,
        in_specs=(P("tm", "space", None), P("tm", "space", None), P("space", None), P("space", None)),
        out_specs=(P("tm", "space", None), P("tm", "space", None)),
        check_vma=False,
    )
```

```python
import functools

import jax
import jax.numpy as jnp
from jax import lax
from jax.experimental import pallas as pl
from jax.experimental.pallas import tpu as pltpu
from jax.sharding import PartitionSpec as P

damping = 0.8
MESH = pl.DeviceIdType.MESH
HALO = 8
LANES = 128

EARLY, SPACE, ALONG, RELAY = range(4)
T_GUESS, T_Q, T_E0, T_E1_RIM, T_E1, T_E2_RIM, T_E2, T_U3, T_RELAY = range(9)
SETS, PLANES, PARTS = 4, 6, 9
RELAYED = 3 * HALO


def kernel(
    tms, spaces, src_hbm, guess_hbm, start_hbm, cond_hbm, u3, rbuf,
    g, s, c, d, w, dk, wk, e, u1, er, ec, c0, c1, c2, u2, qbuf, fu,
    relay, send_sem, recv_sem, ready,
):
    t = lax.axis_index("tm")
    z = lax.axis_index("space")
    has_up, has_dn = z > 0, z < spaces - 1
    has_before, has_after = t > 0, t < tms - 1
    by_relay = jnp.logical_and(lax.rem(t, 2) == 1, t + 2 < tms)
    is_relay = jnp.logical_and(lax.rem(t, 2) == 1, t > 2)
    from_relay = jnp.logical_and(lax.rem(t, 2) == 0, jnp.logical_and(t > 0, t + 1 < tms))
    odd_row = lax.rem(z, 2) == 1
    even_row = jnp.logical_not(odd_row)
    handing = jnp.logical_and(lax.rem(t, 2) == 0, has_after)
    by_hand = jnp.logical_and(handing, jnp.logical_and(even_row, has_dn))
    is_hand = jnp.logical_and(handing, odd_row)

    def count(*flags):
        return sum(jnp.where(flag, 1, 0) for flag in flags)
    steps, rows, cols = src_hbm.shape
    half = steps // 2
    full = rows + 2 * HALO
    mid = slice(HALO, HALO + rows)
    top, bot = slice(0, HALO), slice(HALO + rows, full)
    top_in, bot_in = slice(HALO, 2 * HALO), slice(rows, HALO + rows)
    chunks = cols // LANES
    later = slice(1, steps + 1)

    def remote(src, dst, sent, k, dev):
        return pltpu.make_async_remote_copy(
            src_ref=src, dst_ref=dst, send_sem=send_sem.at[sent], recv_sem=recv_sem.at[k],
            device_id=dev, device_id_type=MESH)

    up, dn = {"space": z - 1}, {"space": z + 1}
    first_set = half
    first_plane = first_set + SETS
    rows_beside = count(has_up, has_dn)
    beside = {"space": jnp.where(has_up, z - 1, z + 1)}

    class Tiles:
        def __init__(self, sent, k, n):
            self.sent, self.k, self.n = sent, k, n

        def each_count(self, wait):
            for beside_count in (1, 2):
                @pl.when(rows_beside == beside_count)
                def _(n=self.n * beside_count):
                    planes = next(p for p in range(1, steps + 1) if n % p == 0 and n // p * HALO <= full)
                    ref = s.at[0:planes, 0 : n // planes * HALO]
                    wait(remote(ref, ref, self.sent, self.k, beside))

        def wait_recv(self):
            self.each_count(lambda copy: copy.wait_recv())

        def wait_send(self):
            self.each_count(lambda copy: copy.wait_send())

    class Edge(Tiles):
        def __init__(self, sent, k, first, last, halo_top, halo_bot, n=1):
            super().__init__(sent, k, n)
            self.first, self.last, self.top, self.bot = first, last, halo_top, halo_bot

        def start(self):
            @pl.when(has_up)
            def _():
                remote(self.first, self.bot, self.sent, self.k, up).start()

            @pl.when(has_dn)
            def _():
                remote(self.last, self.top, self.sent, self.k, dn).start()

    class Along:
        def __init__(self, k, src, dst):
            self.k, self.src, self.dst = first_plane + k, src, dst

        def start(self):
            @pl.when(has_after)
            def _():
                remote(self.src, self.dst, ALONG, self.k, {"tm": t + 1}).start()

        def wait_recv(self):
            @pl.when(has_before)
            def _():
                remote(self.src, self.dst, ALONG, self.k, {"tm": t - 1}).wait_recv()

        def wait_send(self):
            @pl.when(has_after)
            def _():
                remote(self.src, self.dst, ALONG, self.k, {"tm": t + 1}).wait_send()

    class Split:
        def __init__(self, k, ref):
            def part(k, rows_of):
                return Along(k, ref.at[half, rows_of], ref.at[0, rows_of])
            self.rim = Along(k, s.at[0, 0 : 2 * HALO], s.at[0, 0 : 2 * HALO])
            self.rest = part(k + 1, slice(2 * HALO, rows))
            self.parts = [part(k, top_in), part(k, bot_in), self.rest]

        def start(self):
            for part in self.parts:
                part.start()

    def within(turn, ref, sl):
        return Edge(
            SPACE, first_set + turn, ref.at[sl, top_in], ref.at[sl, bot_in], ref.at[sl, top], ref.at[sl, bot],
            sl.stop - sl.start)

    barrier = pltpu.get_barrier_semaphore()
    greeted = (
        (has_before, {"tm": t - 1}), (is_relay, {"tm": t - 2}), (from_relay, {"tm": t + 1}),
        (jnp.logical_and(odd_row, has_up), up), (jnp.logical_and(odd_row, has_dn), dn))
    for flag, dev in greeted:
        @pl.when(flag)
        def _(dev=dev):
            pl.semaphore_signal(barrier, inc=1, device_id=dev, device_id_type=MESH)

    last_guess = pltpu.make_async_copy(guess_hbm.at[steps - 1], g.at[steps, mid], send_sem.at[ALONG])
    last_guess.start()
    loads = [
        pltpu.make_async_copy(cond_hbm, c.at[mid], recv_sem.at[first_plane - 1]),
        pltpu.make_async_copy(src_hbm, s.at[later, mid], recv_sem.at[first_plane - 2]),
        pltpu.make_async_copy(guess_hbm.at[0 : steps - 1], g.at[1:steps, mid], recv_sem.at[first_plane - 3]),
    ]
    for load in loads:
        load.start()
    start_g = pltpu.make_async_copy(start_hbm, g.at[0, mid], recv_sem.at[first_plane + T_GUESS])
    start_u = pltpu.make_async_copy(start_hbm, fu, recv_sem.at[first_plane + T_U3])

    @pl.when(jnp.logical_not(has_before))
    def _():
        start_g.start()
        start_u.start()
        s[0, mid] = jnp.zeros((rows, cols), jnp.float32)
        for ref in (c0, c1, c2):
            ref[0, mid] = jnp.zeros((rows, cols), jnp.float32)

    for flag, edge in ((has_up, top), (has_dn, bot)):
        @pl.when(jnp.logical_not(flag))
        def _(edge=edge):
            c[edge] = jnp.zeros((HALO, cols), jnp.float32)
            for ref in (g, s, c0, c1, c2):
                if ref is g or ref is s or ref is c2:
                    ref[:, edge] = jnp.zeros((ref.shape[0], HALO, cols), jnp.float32)
                else:
                    ref[0, edge] = jnp.zeros((HALO, cols), jnp.float32)

    greetings = count(has_after, by_relay, is_relay) + jnp.where(even_row, rows_beside, 0)

    @pl.when(greetings > 0)
    def _():
        pl.semaphore_wait(barrier, greetings)
    for flag, dev in ((has_up, up), (has_dn, dn)):
        @pl.when(jnp.logical_and(even_row, flag))
        def _(dev=dev):
            pl.semaphore_signal(ready, inc=1, device_id=dev, device_id_type=MESH)

    a_guess = Along(T_GUESS, g.at[steps, mid], g.at[0, mid])
    last_guess.wait()
    a_guess.start()

    @pl.when(jnp.logical_and(odd_row, rows_beside > 0))
    def _():
        pl.semaphore_wait(ready, rows_beside)

    def halo(group, n, hbm, ref):
        Edge(EARLY, group, hbm.at[n - 1, 0:HALO], hbm.at[n - 1, rows - HALO : rows], ref.at[n, top], ref.at[n, bot]).start()

    Edge(SPACE, 0, cond_hbm.at[0:HALO], cond_hbm.at[rows - HALO : rows], c.at[top], c.at[bot]).start()
    halo(0, steps, guess_hbm, g)
    for i in range(steps - 1):
        n = steps - i
        halo((i + 1) // 2, n - 1, guess_hbm, g)
        halo((i + 1) // 2, n, src_hbm, s)
    halo(half - 1, 1, src_hbm, s)
    for load in loads:
        load.wait()

    lane = lax.broadcasted_iota(jnp.int32, (full, LANES), 1)
    is_first, is_last = lane == 0, lane == LANES - 1

    def at(j):
        return slice(j * LANES, (j + 1) * LANES)

    def each(low, high, body):
        def step(i, carry):
            body(i)
            return carry
        lax.fori_loop(low, high, step, 0)

    def stencil(get, put):
        zero = jnp.zeros((full, LANES), jnp.float32)
        before, now = zero, get(0)
        for j in range(chunks):
            after = get(j + 1) if j + 1 < chunks else zero
            left = pltpu.roll(jnp.where(is_last, before, now), 1, 1)
            right = pltpu.roll(jnp.where(is_first, after, now), LANES - 1, 1)
            rim = (left + right) + (pltpu.roll(now, 1, 0) + pltpu.roll(now, full - 1, 0))
            put(j, now, rim)
            before, now = now, after

    def first_sweep(field, n, has_prev=True):
        def put(j, now, rim):
            drive = s[n, :, at(j)]
            if has_prev:
                drive = drive + field[n - 1, :, at(j)]
            e[n, :, at(j)] = d[:, at(j)] * drive + w[:, at(j)] * rim - now
        stencil(lambda j: field[n, :, at(j)], put)

    def second_sweep(field, errs, n, dst, weight, damp, inner=False):
        def put(j, now, rim):
            gain = damp * (now + weight[:, at(j)] * rim)
            if inner:
                dst[n, mid, at(j)] = field[n, mid, at(j)] + gain[mid]
            elif field is None:
                dst[n, :, at(j)] = gain
            else:
                dst[n, :, at(j)] = field[n, :, at(j)] + gain
        stencil(lambda j: errs[n, :, at(j)], put)

    def restrict(m):
        a, b = 2 * m - 1, 2 * m

        def put(j, now, rim):
            cc = c[:, at(j)]
            drive = (s[a, :, at(j)] + s[b, :, at(j)]) + (u1[a - 1, :, at(j)] + u1[a, :, at(j)])
            er[m, :, at(j)] = dk[:, at(j)] * (drive - now + cc * (rim - 4.0 * now))
        stencil(lambda j: u1[a, :, at(j)] + u1[b, :, at(j)], put)

    def coarse_defect(field, m):
        def put(j, now, rim):
            ec[m, :, at(j)] = er[m, :, at(j)] + dk[:, at(j)] * field[m - 1, :, at(j)] + wk[:, at(j)] * rim - now
        stencil(lambda j: field[m, :, at(j)], put)

    def sweep_one(low, high):
        each(low, high, lambda m: coarse_defect(c0, m))
        each(low, high, lambda m: second_sweep(c0, ec, m, c1, wk, damping))

    def sweep_two(low, high):
        each(low, high, lambda m: coarse_defect(c1, m))
        each(low, high, lambda m: second_sweep(c1, ec, m, c2, wk, damping, inner=True))

    def prolong(m):
        for j in range(chunks):
            u2[2 * m, :, at(j)] = u1[2 * m, :, at(j)] + c2[m, :, at(j)]
            u2[2 * m - 1, :, at(j)] = u1[2 * m - 1, :, at(j)] + 0.5 * (c2[m - 1, :, at(j)] + c2[m, :, at(j)])

    def last_residual(n, has_prev=True):
        def put(j, now, rim):
            flow = c[:, at(j)] * (rim - 4.0 * now) - now
            drive = s[n, mid, at(j)]
            if has_prev:
                drive = drive + u3[n - 1, mid, at(j)]
            rbuf[n - 1, :, at(j)] = flow[mid] + drive
        stencil(lambda j: u3[n, :, at(j)], put)

    for j in range(chunks):
        qbuf[:, at(j)] = s[steps, mid, at(j)] + g[steps - 1, mid, at(j)]
    a_q = Along(T_Q, qbuf, s.at[0, mid])
    a_e0 = Along(T_E0, c0.at[half, mid], c0.at[0, mid])
    a_e1 = Split(T_E1_RIM, c1)
    a_e2 = Split(T_E2_RIM, c2)
    a_u3 = Along(T_U3, fu, fu)
    kept = rows - RELAYED
    u3_kept = Along(T_U3, u3.at[steps, HALO : HALO + kept], fu.at[0:kept])
    u3_rest = Along(T_U3, u3.at[steps, HALO + kept : HALO + rows], fu.at[kept:rows])

    def give(sent, k, src, dst, step, row_step=0):
        dev = {"tm": t + step, "space": z + row_step}
        return remote(src, dst, sent, first_plane + k, dev)

    def start_u3():
        u3_kept.start()

        @pl.when(jnp.logical_not(jnp.logical_or(by_relay, by_hand)))
        def _():
            u3_rest.start()

        @pl.when(by_relay)
        def _():
            give(ALONG, T_RELAY, u3_rest.src, relay, 2).start()

        @pl.when(by_hand)
        def _():
            give(ALONG, T_RELAY, u3_rest.src, relay, 0, 1).start()

    def passed_on(act):
        for flag, source, target in ((is_relay, (-2, 0), (-1, 0)), (is_hand, (0, -1), (1, -1))):
            @pl.when(flag)
            def _(source=source, target=target):
                act(source, target)

    def forward(source, target):
        give(RELAY, T_RELAY, relay, relay, *source).wait_recv()
        give(RELAY, T_U3, relay, u3_rest.dst, *target).start()

    def forwarded(source, target):
        give(RELAY, T_U3, relay, u3_rest.dst, *target).wait_send()

    def coefficients(part):
        for j in range(chunks):
            cc = c[part, at(j)]
            dd = 1.0 / (1.0 + 4.0 * cc)
            dd2 = 1.0 / (1.0 + 8.0 * cc)
            d[part, at(j)], w[part, at(j)] = dd, cc * dd
            dk[part, at(j)], wk[part, at(j)] = dd2, 2.0 * cc * dd2

    coefficients(mid)
    a_q.start()
    Tiles(EARLY, 0, 4).wait_recv()
    coefficients(top)
    coefficients(bot)

    def local_step(i):
        n = steps - i
        odd = lax.rem(i, 2) == 1

        @pl.when(jnp.logical_and(odd, i < steps - 3))
        def _():
            Tiles(EARLY, (i + 1) // 2, 4).wait_recv()

        @pl.when(i == steps - 3)
        def _():
            Tiles(EARLY, half - 1, 5).wait_recv()

        @pl.when(i == 3)
        def _():
            a_e0.start()
        first_sweep(g, n)
        second_sweep(g, e, n, u1, w, damping)

        @pl.when(jnp.logical_and(lax.rem(i, 2) == 0, i > 0))
        def _():
            m = half + 1 - i // 2
            restrict(m)
            second_sweep(None, er, m, c0, wk, damping)

    each(0, steps - 1, local_step)

    @pl.when(jnp.logical_not(has_before))
    def _():
        start_g.wait()
        start_u.wait()
    a_guess.wait_recv()
    f_guess = within(0, g, slice(0, 1))
    f_guess.start()
    sweep_one(3, half + 1)
    each(4, half + 1, lambda m: coarse_defect(c1, m))
    a_e1.start()
    each(4, half + 1, lambda m: second_sweep(c1, ec, m, c2, wk, damping, inner=True))
    f_guess.wait_recv()
    each(1, 2, lambda n: first_sweep(g, n))
    a_e2.start()
    each(1, 2, lambda n: second_sweep(g, e, n, u1, w, damping))
    a_q.wait_recv()
    f_q = within(1, s, slice(0, 1))
    f_q.start()
    f_q.wait_recv()
    each(0, 1, lambda n: first_sweep(g, n, has_prev=False))
    damp0 = jnp.where(has_before, damping, 0.0).astype(jnp.float32)
    each(0, 1, lambda n: second_sweep(g, e, n, u1, w, damp0))
    each(1, 2, restrict)
    each(1, 2, lambda m: second_sweep(None, er, m, c0, wk, damping))
    sweep_one(2, 3)
    sweep_two(3, 4)
    x_late = within(0, c2, slice(3, half + 1))
    x_late.start()
    a_e0.wait_recv()
    f_e0 = within(2, c0, slice(0, 1))
    f_e0.start()
    x_late.wait_recv()
    each(half, half + 1, prolong)
    each(steps, steps + 1, lambda n: first_sweep(u2, n))
    each(steps, steps + 1, lambda n: second_sweep(u2, e, n, u3, w, damping))

    a_e1.rim.wait_recv()
    f_e1 = within(3, c1, slice(0, 1))
    f_e1.start()
    f_e0.wait_recv()
    each(1, 2, lambda m: coarse_defect(c0, m))
    start_u3()
    each(1, 2, lambda m: second_sweep(c0, ec, m, c1, wk, damping))
    sweep_two(2, 3)
    x_mid = within(1, c2, slice(2, 3))
    x_mid.start()
    for j in range(chunks):
        u2[steps - 2, :, at(j)] = u1[steps - 2, :, at(j)] + c2[half - 1, :, at(j)]
    each(steps - 1, steps, lambda n: first_sweep(u2, n))
    each(steps - 1, steps, lambda n: second_sweep(u2, e, n, u3, w, damping))
    each(steps, steps + 1, last_residual)
    a_e1.rest.wait_recv()
    f_e1.wait_recv()
    sweep_two(1, 2)
    x_early = within(0, c2, slice(1, 2))
    x_early.start()
    x_mid.wait_recv()
    each(3, half, prolong)
    for j in range(chunks):
        u2[4, :, at(j)] = u1[4, :, at(j)] + c2[2, :, at(j)]
    each(5, steps - 1, lambda n: first_sweep(u2, n))
    each(5, steps - 1, lambda n: second_sweep(u2, e, n, u3, w, damping))
    passed_on(forward)
    a_e2.rim.wait_recv()
    f_e2 = within(2, c2, slice(0, 1))
    f_e2.start()
    each(6, steps, last_residual)
    x_early.wait_recv()
    for j in range(chunks):
        u2[2, :, at(j)] = u1[2, :, at(j)] + c2[1, :, at(j)]
        u2[3, :, at(j)] = u1[3, :, at(j)] + 0.5 * (c2[1, :, at(j)] + c2[2, :, at(j)])
    each(3, 5, lambda n: first_sweep(u2, n))
    each(3, 5, lambda n: second_sweep(u2, e, n, u3, w, damping))
    each(4, 6, last_residual)
    a_e2.rest.wait_recv()
    f_e2.wait_recv()
    for j in range(chunks):
        u2[0, :, at(j)] = u1[0, :, at(j)] + c2[0, :, at(j)]
        u2[1, :, at(j)] = u1[1, :, at(j)] + 0.5 * (c2[0, :, at(j)] + c2[1, :, at(j)])
    each(1, 3, lambda n: first_sweep(u2, n))
    each(1, 3, lambda n: second_sweep(u2, e, n, u3, w, damping))
    each(2, 4, last_residual)
    each(1, 2, lambda n: last_residual(n, has_prev=False))
    @pl.when(jnp.logical_not(has_before))
    def _():
        rbuf[0] = rbuf[0] + fu[...]
    Tiles(EARLY, 0, 2 * steps).wait_send()
    Tiles(SPACE, 0, half + 6).wait_send()
    Along(T_U3, s.at[0:PLANES, mid], s.at[0:PLANES, mid]).wait_send()

    passed_on(forwarded)

    @pl.when(has_before)
    def _():
        a_u3.wait_recv()
        rbuf[0] = rbuf[0] + fu[...]


def store(u3, rbuf, u_out, r_out, sem):
    steps, rows, _ = u_out.shape
    copies = [
        pltpu.make_async_copy(u3.at[1 : steps + 1, HALO : HALO + rows], u_out, sem.at[0]),
        pltpu.make_async_copy(rbuf, r_out, sem.at[1]),
    ]
    for copy in copies:
        copy.start()
    for copy in copies:
        copy.wait()


def solution(mesh):
    tms, spaces = mesh.shape["tm"], mesh.shape["space"]

    def shards(source, guess, start_state, conduct):
        steps, rows, cols = source.shape
        full, half = rows + 2 * HALO, steps // 2

        def buf(*lead):
            return pltpu.VMEM(lead + (full, cols), jnp.float32)

        fields = pl.pallas_call(
            functools.partial(kernel, tms, spaces),
            out_shape=(buf(steps + 1), pltpu.VMEM(source.shape, jnp.float32)),
            in_specs=[pl.BlockSpec(memory_space=pltpu.HBM)] * 4,
            out_specs=[pl.BlockSpec(memory_space=pltpu.VMEM)] * 2,
            scratch_shapes=[
                buf(steps + 1), buf(steps + 1), buf(), buf(), buf(), buf(), buf(),
                buf(steps + 1), buf(steps + 1), buf(half + 1), buf(half + 1),
                buf(half + 1), buf(half + 1), buf(half + 1), buf(steps + 1),
                pltpu.VMEM((rows, cols), jnp.float32),
                pltpu.VMEM((rows, cols), jnp.float32),
                pltpu.VMEM((RELAYED, cols), jnp.float32),
                pltpu.SemaphoreType.DMA((4,)),
                pltpu.SemaphoreType.DMA((half + SETS + PARTS,)),
                pltpu.SemaphoreType.REGULAR,
            ],
            compiler_params=pltpu.CompilerParams(
                collective_id=0, has_side_effects=True, vmem_limit_bytes=59 * 1024 * 1024),
        )(source, guess, start_state, conduct)
        return pl.pallas_call(
            store,
            out_shape=(jax.ShapeDtypeStruct(source.shape, jnp.float32),) * 2,
            in_specs=[pl.BlockSpec(memory_space=pltpu.VMEM)] * 2,
            out_specs=[pl.BlockSpec(memory_space=pl.ANY)] * 2,
            scratch_shapes=[pltpu.SemaphoreType.DMA((2,))],
            compiler_params=pltpu.CompilerParams(vmem_limit_bytes=8 * 1024 * 1024),
        )(*fields)

    return jax.shard_map(
        shards,
        mesh=mesh,
        in_specs=(P("tm", "space", None), P("tm", "space", None), P("space", None), P("space", None)),
        out_specs=(P("tm", "space", None), P("tm", "space", None)),
        check_vma=False,
    )
```

```python
import functools

import jax
import jax.numpy as jnp
from jax import lax
from jax.experimental import pallas as pl
from jax.experimental.pallas import tpu as pltpu
from jax.sharding import PartitionSpec as P

damping = 0.8
MESH = pl.DeviceIdType.MESH
HALO = 8
LANES = 128

EARLY, SPACE, ALONG, RELAY = range(4)
T_GUESS, T_Q, T_E0, T_E1_RIM, T_E1, T_E2_RIM, T_E2, T_U3, T_RELAY = range(9)
PLANES, PARTS = 6, 9
RELAYED = 3 * HALO


def kernel(
    tms, spaces, src_hbm, guess_hbm, start_hbm, cond_hbm, u3, rbuf,
    g, s, c, d, w, dk, wk, e, u1, er, ec, c0, c1, c2, u2, qbuf, fu,
    relay, send_sem, recv_sem, ready,
):
    t = lax.axis_index("tm")
    z = lax.axis_index("space")
    has_up, has_dn = z > 0, z < spaces - 1
    has_before, has_after = t > 0, t < tms - 1
    by_relay = jnp.logical_and(lax.rem(t, 2) == 1, t + 2 < tms)
    is_relay = jnp.logical_and(lax.rem(t, 2) == 1, t > 2)
    from_relay = jnp.logical_and(lax.rem(t, 2) == 0, jnp.logical_and(t > 0, t + 1 < tms))
    odd_row = lax.rem(z, 2) == 1
    even_row = jnp.logical_not(odd_row)
    paired = jnp.logical_or(lax.rem(z, 2) == 1, has_dn)
    handing = jnp.logical_and(jnp.logical_and(lax.rem(t, 2) == 0, has_after), paired)
    by_hand = jnp.logical_and(handing, jnp.logical_and(even_row, has_dn))
    is_hand = jnp.logical_and(handing, odd_row)

    def count(*flags):
        return sum(jnp.where(flag, 1, 0) for flag in flags)
    steps, rows, cols = src_hbm.shape
    half = steps // 2
    full = rows + 2 * HALO
    mid = slice(HALO, HALO + rows)
    top, bot = slice(0, HALO), slice(HALO + rows, full)
    top_in, bot_in = slice(HALO, 2 * HALO), slice(rows, HALO + rows)
    chunks = cols // LANES
    later = slice(1, steps + 1)

    def remote(src, dst, sent, k, dev):
        return pltpu.make_async_remote_copy(
            src_ref=src, dst_ref=dst, send_sem=send_sem.at[sent], recv_sem=recv_sem.at[k],
            device_id=dev, device_id_type=MESH)

    up, dn = {"space": z - 1}, {"space": z + 1}
    alone = half
    first_plane = half + 1
    rows_beside = count(has_up, has_dn)
    beside = {"space": jnp.where(has_up, z - 1, z + 1)}

    class Tiles:
        def __init__(self, sent, k, n):
            self.sent, self.k, self.n = sent, k, n

        def each_count(self, wait):
            for beside_count in (1, 2):
                @pl.when(rows_beside == beside_count)
                def _(n=self.n * beside_count):
                    planes = next(p for p in range(1, steps + 1) if n % p == 0 and n // p * HALO <= full)
                    ref = s.at[0:planes, 0 : n // planes * HALO]
                    wait(remote(ref, ref, self.sent, self.k, beside))

        def wait_recv(self):
            self.each_count(lambda copy: copy.wait_recv())

        def wait_send(self):
            self.each_count(lambda copy: copy.wait_send())

    class Edge(Tiles):
        def __init__(self, sent, k, first, last, halo_top, halo_bot, n=1):
            super().__init__(sent, k, n)
            self.first, self.last, self.top, self.bot = first, last, halo_top, halo_bot

        def start(self):
            @pl.when(has_up)
            def _():
                remote(self.first, self.bot, self.sent, self.k, up).start()

            @pl.when(has_dn)
            def _():
                remote(self.last, self.top, self.sent, self.k, dn).start()

    class Along:
        def __init__(self, k, src, dst):
            self.k, self.src, self.dst = first_plane + k, src, dst

        def start(self):
            @pl.when(has_after)
            def _():
                remote(self.src, self.dst, ALONG, self.k, {"tm": t + 1}).start()

        def wait_recv(self):
            @pl.when(has_before)
            def _():
                remote(self.src, self.dst, ALONG, self.k, {"tm": t - 1}).wait_recv()

        def wait_send(self):
            @pl.when(has_after)
            def _():
                remote(self.src, self.dst, ALONG, self.k, {"tm": t + 1}).wait_send()

    class Split:
        def __init__(self, k, ref):
            def part(k, rows_of):
                return Along(k, ref.at[half, rows_of], ref.at[0, rows_of])
            self.rim = Along(k, s.at[0, 0 : 2 * HALO], s.at[0, 0 : 2 * HALO])
            self.rest = part(k + 1, slice(2 * HALO, rows))
            self.parts = [part(k, top_in), part(k, bot_in), self.rest]

        def start(self):
            for part in self.parts:
                part.start()

    def within(turn, ref, sl):
        return Edge(
            SPACE, turn, ref.at[sl, top_in], ref.at[sl, bot_in], ref.at[sl, top], ref.at[sl, bot],
            sl.stop - sl.start)

    barrier = pltpu.get_barrier_semaphore()
    greeted = (
        (has_before, {"tm": t - 1}), (is_relay, {"tm": t - 2}), (from_relay, {"tm": t + 1}),
        (jnp.logical_and(odd_row, has_up), up), (jnp.logical_and(odd_row, has_dn), dn))
    for flag, dev in greeted:
        @pl.when(flag)
        def _(dev=dev):
            pl.semaphore_signal(barrier, inc=1, device_id=dev, device_id_type=MESH)

    last_guess = pltpu.make_async_copy(guess_hbm.at[steps - 1], g.at[steps, mid], send_sem.at[ALONG])
    last_guess.start()
    loads = [
        pltpu.make_async_copy(cond_hbm, c.at[mid], recv_sem.at[alone]),
        pltpu.make_async_copy(src_hbm, s.at[later, mid], send_sem.at[RELAY]),
        pltpu.make_async_copy(guess_hbm.at[0 : steps - 1], g.at[1:steps, mid], recv_sem.at[alone]),
    ]
    for load in loads:
        load.start()
    loaded = [loads[1], pltpu.make_async_copy(src_hbm, s.at[later, mid], recv_sem.at[alone])]
    start_g = pltpu.make_async_copy(start_hbm, g.at[0, mid], recv_sem.at[first_plane + T_GUESS])
    start_u = pltpu.make_async_copy(start_hbm, fu, recv_sem.at[first_plane + T_U3])

    @pl.when(jnp.logical_not(has_before))
    def _():
        start_g.start()
        start_u.start()
        s[0, mid] = jnp.zeros((rows, cols), jnp.float32)
        for ref in (c0, c1, c2):
            ref[0, mid] = jnp.zeros((rows, cols), jnp.float32)

    for flag, edge in ((has_up, top), (has_dn, bot)):
        @pl.when(jnp.logical_not(flag))
        def _(edge=edge):
            c[edge] = jnp.zeros((HALO, cols), jnp.float32)
            for ref in (g, s, c0, c1, c2):
                if ref is g or ref is s or ref is c2:
                    ref[:, edge] = jnp.zeros((ref.shape[0], HALO, cols), jnp.float32)
                else:
                    ref[0, edge] = jnp.zeros((HALO, cols), jnp.float32)

    greetings = count(has_after, by_relay, is_relay) + jnp.where(even_row, rows_beside, 0)

    @pl.when(greetings > 0)
    def _():
        pl.semaphore_wait(barrier, greetings)

    a_guess = Along(T_GUESS, g.at[steps, mid], g.at[0, mid])
    last_guess.wait()
    a_guess.start()
    for flag, dev in ((has_up, up), (has_dn, dn)):
        @pl.when(jnp.logical_and(even_row, flag))
        def _(dev=dev):
            pl.semaphore_signal(ready, inc=1, device_id=dev, device_id_type=MESH)

    @pl.when(jnp.logical_and(odd_row, rows_beside > 0))
    def _():
        pl.semaphore_wait(ready, rows_beside)

    def halo(group, n, hbm, ref):
        Edge(EARLY, group, hbm.at[n - 1, 0:HALO], hbm.at[n - 1, rows - HALO : rows], ref.at[n, top], ref.at[n, bot]).start()

    Edge(SPACE, 0, cond_hbm.at[0:HALO], cond_hbm.at[rows - HALO : rows], c.at[top], c.at[bot]).start()
    halo(0, steps, guess_hbm, g)
    for i in range(steps - 1):
        n = steps - i
        halo((i + 1) // 2, n - 1, guess_hbm, g)
        halo((i + 1) // 2, n, src_hbm, s)
    for load in loaded:
        load.wait()
    halo(half - 1, 1, src_hbm, s)

    lane = lax.broadcasted_iota(jnp.int32, (full, LANES), 1)
    is_first, is_last = lane == 0, lane == LANES - 1

    def at(j):
        return slice(j * LANES, (j + 1) * LANES)

    def each(low, high, body):
        def step(i, carry):
            body(i)
            return carry
        lax.fori_loop(low, high, step, 0)

    def stencil(get, put):
        zero = jnp.zeros((full, LANES), jnp.float32)
        before, now = zero, get(0)
        for j in range(chunks):
            after = get(j + 1) if j + 1 < chunks else zero
            left = pltpu.roll(jnp.where(is_last, before, now), 1, 1)
            right = pltpu.roll(jnp.where(is_first, after, now), LANES - 1, 1)
            rim = (left + right) + (pltpu.roll(now, 1, 0) + pltpu.roll(now, full - 1, 0))
            put(j, now, rim)
            before, now = now, after

    def first_sweep(field, n, has_prev=True):
        def put(j, now, rim):
            drive = s[n, :, at(j)]
            if has_prev:
                drive = drive + field[n - 1, :, at(j)]
            e[n, :, at(j)] = d[:, at(j)] * drive + w[:, at(j)] * rim - now
        stencil(lambda j: field[n, :, at(j)], put)

    def second_sweep(field, errs, n, dst, weight, damp, inner=False):
        def put(j, now, rim):
            gain = damp * (now + weight[:, at(j)] * rim)
            if inner:
                dst[n, mid, at(j)] = field[n, mid, at(j)] + gain[mid]
            elif field is None:
                dst[n, :, at(j)] = gain
            else:
                dst[n, :, at(j)] = field[n, :, at(j)] + gain
        stencil(lambda j: errs[n, :, at(j)], put)

    def restrict(m):
        a, b = 2 * m - 1, 2 * m

        def put(j, now, rim):
            cc = c[:, at(j)]
            drive = (s[a, :, at(j)] + s[b, :, at(j)]) + (u1[a - 1, :, at(j)] + u1[a, :, at(j)])
            er[m, :, at(j)] = dk[:, at(j)] * (drive - now + cc * (rim - 4.0 * now))
        stencil(lambda j: u1[a, :, at(j)] + u1[b, :, at(j)], put)

    def coarse_defect(field, m):
        def put(j, now, rim):
            ec[m, :, at(j)] = er[m, :, at(j)] + dk[:, at(j)] * field[m - 1, :, at(j)] + wk[:, at(j)] * rim - now
        stencil(lambda j: field[m, :, at(j)], put)

    def sweep_one(low, high):
        each(low, high, lambda m: coarse_defect(c0, m))
        each(low, high, lambda m: second_sweep(c0, ec, m, c1, wk, damping))

    def sweep_two(low, high):
        each(low, high, lambda m: coarse_defect(c1, m))
        each(low, high, lambda m: second_sweep(c1, ec, m, c2, wk, damping, inner=True))

    def prolong(m):
        for j in range(chunks):
            u2[2 * m, :, at(j)] = u1[2 * m, :, at(j)] + c2[m, :, at(j)]
            u2[2 * m - 1, :, at(j)] = u1[2 * m - 1, :, at(j)] + 0.5 * (c2[m - 1, :, at(j)] + c2[m, :, at(j)])

    def last_residual(n, has_prev=True):
        def put(j, now, rim):
            flow = c[:, at(j)] * (rim - 4.0 * now) - now
            drive = s[n, mid, at(j)]
            if has_prev:
                drive = drive + u3[n - 1, mid, at(j)]
            rbuf[n - 1, :, at(j)] = flow[mid] + drive
        stencil(lambda j: u3[n, :, at(j)], put)

    for j in range(chunks):
        qbuf[:, at(j)] = s[steps, mid, at(j)] + g[steps - 1, mid, at(j)]
    a_q = Along(T_Q, qbuf, s.at[0, mid])
    a_e0 = Along(T_E0, c0.at[half, mid], c0.at[0, mid])
    a_e1 = Split(T_E1_RIM, c1)
    a_e2 = Split(T_E2_RIM, c2)
    a_u3 = Along(T_U3, fu, fu)
    kept = rows - RELAYED
    u3_kept = Along(T_U3, u3.at[steps, HALO : HALO + kept], fu.at[0:kept])
    u3_rest = Along(T_U3, u3.at[steps, HALO + kept : HALO + rows], fu.at[kept:rows])

    def give(sent, k, src, dst, step, row_step=0):
        dev = {"tm": t + step, "space": z + row_step}
        return remote(src, dst, sent, first_plane + k, dev)

    def start_u3():
        u3_kept.start()

        @pl.when(jnp.logical_not(jnp.logical_or(by_relay, handing)))
        def _():
            u3_rest.start()

        @pl.when(by_relay)
        def _():
            give(ALONG, T_RELAY, u3_rest.src, relay, 2).start()

        @pl.when(by_hand)
        def _():
            give(ALONG, T_RELAY, u3_rest.src, relay, 0, 1).start()

    def passed_on(act):
        for flag, source, target in ((is_relay, (-2, 0), (-1, 0)), (is_hand, (0, -1), (1, -1))):
            @pl.when(flag)
            def _(source=source, target=target):
                act(source, target)

    def forward(source, target):
        give(RELAY, T_RELAY, relay, relay, *source).wait_recv()
        give(RELAY, T_U3, relay, u3_rest.dst, *target).start()

        @pl.when(handing)
        def _():
            u3_rest.start()

    def forwarded(source, target):
        give(RELAY, T_U3, relay, u3_rest.dst, *target).wait_send()

    def coefficients(part):
        for j in range(chunks):
            cc = c[part, at(j)]
            dd = 1.0 / (1.0 + 4.0 * cc)
            dd2 = 1.0 / (1.0 + 8.0 * cc)
            d[part, at(j)], w[part, at(j)] = dd, cc * dd
            dk[part, at(j)], wk[part, at(j)] = dd2, 2.0 * cc * dd2

    coefficients(mid)
    a_q.start()
    Tiles(EARLY, 0, 4).wait_recv()
    coefficients(top)
    coefficients(bot)

    def local_step(i):
        n = steps - i
        odd = lax.rem(i, 2) == 1

        @pl.when(jnp.logical_and(odd, i < steps - 3))
        def _():
            Tiles(EARLY, (i + 1) // 2, 4).wait_recv()

        @pl.when(i == steps - 3)
        def _():
            Tiles(EARLY, half - 1, 5).wait_recv()

        @pl.when(i == 3)
        def _():
            a_e0.start()
        first_sweep(g, n)
        second_sweep(g, e, n, u1, w, damping)

        @pl.when(jnp.logical_and(lax.rem(i, 2) == 0, i > 0))
        def _():
            m = half + 1 - i // 2
            restrict(m)
            second_sweep(None, er, m, c0, wk, damping)

    each(0, steps - 1, local_step)

    @pl.when(jnp.logical_not(has_before))
    def _():
        start_g.wait()
        start_u.wait()
    a_guess.wait_recv()
    f_guess = within(alone, g, slice(0, 1))
    f_guess.start()
    sweep_one(3, half + 1)
    each(4, half + 1, lambda m: coarse_defect(c1, m))
    a_e1.start()
    each(4, half + 1, lambda m: second_sweep(c1, ec, m, c2, wk, damping, inner=True))
    f_guess.wait_recv()
    each(1, 2, lambda n: first_sweep(g, n))
    a_e2.start()
    each(1, 2, lambda n: second_sweep(g, e, n, u1, w, damping))
    a_q.wait_recv()
    f_q = within(0, s, slice(0, 1))
    f_q.start()
    f_q.wait_recv()
    each(0, 1, lambda n: first_sweep(g, n, has_prev=False))
    damp0 = jnp.where(has_before, damping, 0.0).astype(jnp.float32)
    each(0, 1, lambda n: second_sweep(g, e, n, u1, w, damp0))
    each(1, 2, restrict)
    each(1, 2, lambda m: second_sweep(None, er, m, c0, wk, damping))
    sweep_one(2, 3)
    sweep_two(3, 4)
    x_late = within(1, c2, slice(3, half + 1))
    x_late.start()
    a_e0.wait_recv()
    f_e0 = within(2, c0, slice(0, 1))
    f_e0.start()
    x_late.wait_recv()
    each(half, half + 1, prolong)
    each(steps, steps + 1, lambda n: first_sweep(u2, n))
    each(steps, steps + 1, lambda n: second_sweep(u2, e, n, u3, w, damping))

    a_e1.rim.wait_recv()
    f_e1 = within(3, c1, slice(0, 1))
    f_e1.start()
    f_e0.wait_recv()
    each(1, 2, lambda m: coarse_defect(c0, m))
    start_u3()
    each(1, 2, lambda m: second_sweep(c0, ec, m, c1, wk, damping))
    sweep_two(2, 3)
    x_mid = within(0, c2, slice(2, 3))
    x_mid.start()
    for j in range(chunks):
        u2[steps - 2, :, at(j)] = u1[steps - 2, :, at(j)] + c2[half - 1, :, at(j)]
    each(steps - 1, steps, lambda n: first_sweep(u2, n))
    each(steps - 1, steps, lambda n: second_sweep(u2, e, n, u3, w, damping))
    each(steps, steps + 1, last_residual)
    a_e1.rest.wait_recv()
    f_e1.wait_recv()
    sweep_two(1, 2)
    x_early = within(1, c2, slice(1, 2))
    x_early.start()
    x_mid.wait_recv()
    each(3, half, prolong)
    for j in range(chunks):
        u2[4, :, at(j)] = u1[4, :, at(j)] + c2[2, :, at(j)]
    each(5, steps - 1, lambda n: first_sweep(u2, n))
    each(5, steps - 1, lambda n: second_sweep(u2, e, n, u3, w, damping))
    passed_on(forward)
    a_e2.rim.wait_recv()
    f_e2 = within(2, c2, slice(0, 1))
    f_e2.start()
    each(6, steps, last_residual)
    x_early.wait_recv()
    for j in range(chunks):
        u2[2, :, at(j)] = u1[2, :, at(j)] + c2[1, :, at(j)]
        u2[3, :, at(j)] = u1[3, :, at(j)] + 0.5 * (c2[1, :, at(j)] + c2[2, :, at(j)])
    each(3, 5, lambda n: first_sweep(u2, n))
    each(3, 5, lambda n: second_sweep(u2, e, n, u3, w, damping))
    each(4, 6, last_residual)
    a_e2.rest.wait_recv()
    f_e2.wait_recv()
    for j in range(chunks):
        u2[0, :, at(j)] = u1[0, :, at(j)] + c2[0, :, at(j)]
        u2[1, :, at(j)] = u1[1, :, at(j)] + 0.5 * (c2[0, :, at(j)] + c2[1, :, at(j)])
    each(1, 3, lambda n: first_sweep(u2, n))
    each(1, 3, lambda n: second_sweep(u2, e, n, u3, w, damping))
    each(2, 4, last_residual)
    each(1, 2, lambda n: last_residual(n, has_prev=False))
    @pl.when(jnp.logical_not(has_before))
    def _():
        rbuf[0] = rbuf[0] + fu[...]
    Tiles(EARLY, 0, 2 * steps).wait_send()
    Tiles(SPACE, 0, half + 6).wait_send()
    Along(T_U3, s.at[0:PLANES, mid], s.at[0:PLANES, mid]).wait_send()

    passed_on(forwarded)

    @pl.when(has_before)
    def _():
        a_u3.wait_recv()
        rbuf[0] = rbuf[0] + fu[...]


def store(u3, rbuf, u_out, r_out, sem):
    steps, rows, _ = u_out.shape
    copies = [
        pltpu.make_async_copy(u3.at[1 : steps + 1, HALO : HALO + rows], u_out, sem.at[0]),
        pltpu.make_async_copy(rbuf, r_out, sem.at[1]),
    ]
    for copy in copies:
        copy.start()
    for copy in copies:
        copy.wait()


def solution(mesh):
    tms, spaces = mesh.shape["tm"], mesh.shape["space"]

    def shards(source, guess, start_state, conduct):
        steps, rows, cols = source.shape
        full, half = rows + 2 * HALO, steps // 2

        def buf(*lead):
            return pltpu.VMEM(lead + (full, cols), jnp.float32)

        fields = pl.pallas_call(
            functools.partial(kernel, tms, spaces),
            out_shape=(buf(steps + 1), pltpu.VMEM(source.shape, jnp.float32)),
            in_specs=[pl.BlockSpec(memory_space=pltpu.HBM)] * 4,
            out_specs=[pl.BlockSpec(memory_space=pltpu.VMEM)] * 2,
            scratch_shapes=[
                buf(steps + 1), buf(steps + 1), buf(), buf(), buf(), buf(), buf(),
                buf(steps + 1), buf(steps + 1), buf(half + 1), buf(half + 1),
                buf(half + 1), buf(half + 1), buf(half + 1), buf(steps + 1),
                pltpu.VMEM((rows, cols), jnp.float32),
                pltpu.VMEM((rows, cols), jnp.float32),
                pltpu.VMEM((RELAYED, cols), jnp.float32),
                pltpu.SemaphoreType.DMA((4,)),
                pltpu.SemaphoreType.DMA((half + 1 + PARTS,)),
                pltpu.SemaphoreType.REGULAR,
            ],
            compiler_params=pltpu.CompilerParams(
                collective_id=0, has_side_effects=True, vmem_limit_bytes=59 * 1024 * 1024),
        )(source, guess, start_state, conduct)
        return pl.pallas_call(
            store,
            out_shape=(jax.ShapeDtypeStruct(source.shape, jnp.float32),) * 2,
            in_specs=[pl.BlockSpec(memory_space=pltpu.VMEM)] * 2,
            out_specs=[pl.BlockSpec(memory_space=pl.ANY)] * 2,
            scratch_shapes=[pltpu.SemaphoreType.DMA((2,))],
            compiler_params=pltpu.CompilerParams(vmem_limit_bytes=8 * 1024 * 1024),
        )(*fields)

    return jax.shard_map(
        shards,
        mesh=mesh,
        in_specs=(P("tm", "space", None), P("tm", "space", None), P("space", None), P("space", None)),
        out_specs=(P("tm", "space", None), P("tm", "space", None)),
        check_vma=False,
    )
```

```python
import functools

import jax
import jax.numpy as jnp
from jax import lax
from jax.experimental import pallas as pl
from jax.experimental.pallas import tpu as pltpu
from jax.sharding import PartitionSpec as P

damping = 0.8
MESH = pl.DeviceIdType.MESH
HALO = 8
LANES = 128

EARLY, SPACE, ALONG, RELAY = range(4)
T_GUESS, T_Q, T_E0, T_E1_RIM, T_E1, T_E2_RIM, T_E2, T_KEPT, T_U3, T_RELAY = range(10)
PLANES, PARTS = 6, 10
RELAYED = 3 * HALO


def kernel(
    tms, spaces, src_hbm, guess_hbm, start_hbm, cond_hbm, u3, rbuf,
    g, s, c, d, w, dk, wk, e, u1, er, ec, c0, c1, c2, u2, qbuf, fu,
    relay, send_sem, recv_sem, ready,
):
    t = lax.axis_index("tm")
    z = lax.axis_index("space")
    has_up, has_dn = z > 0, z < spaces - 1
    has_before, has_after = t > 0, t < tms - 1
    barrier = pltpu.get_barrier_semaphore()

    @pl.when(has_before)
    def _():
        pl.semaphore_signal(barrier, inc=1, device_id={"tm": t - 1}, device_id_type=MESH)

    by_relay = jnp.logical_and(lax.rem(t, 2) == 1, t + 2 < tms)
    is_relay = jnp.logical_and(lax.rem(t, 2) == 1, t > 2)
    from_relay = jnp.logical_and(lax.rem(t, 2) == 0, jnp.logical_and(t > 0, t + 1 < tms))
    odd_row = lax.rem(z, 2) == 1
    even_row = jnp.logical_not(odd_row)
    paired = jnp.logical_or(lax.rem(z, 2) == 1, has_dn)
    handing = jnp.logical_and(jnp.logical_and(lax.rem(t, 2) == 0, has_after), paired)
    by_hand = jnp.logical_and(handing, jnp.logical_and(even_row, has_dn))
    is_hand = jnp.logical_and(handing, odd_row)

    def count(*flags):
        return sum(jnp.where(flag, 1, 0) for flag in flags)
    steps, rows, cols = src_hbm.shape
    half = steps // 2
    full = rows + 2 * HALO
    mid = slice(HALO, HALO + rows)
    top, bot = slice(0, HALO), slice(HALO + rows, full)
    top_in, bot_in = slice(HALO, 2 * HALO), slice(rows, HALO + rows)
    chunks = cols // LANES
    later = slice(1, steps + 1)

    def remote(src, dst, sent, k, dev):
        return pltpu.make_async_remote_copy(
            src_ref=src, dst_ref=dst, send_sem=send_sem.at[sent], recv_sem=recv_sem.at[k],
            device_id=dev, device_id_type=MESH)

    up, dn = {"space": z - 1}, {"space": z + 1}
    alone = half
    first_plane = half + 1
    rows_beside = count(has_up, has_dn)
    beside = {"space": jnp.where(has_up, z - 1, z + 1)}

    class Tiles:
        def __init__(self, sent, k, n):
            self.sent, self.k, self.n = sent, k, n

        def each_count(self, wait):
            for beside_count in (1, 2):
                @pl.when(rows_beside == beside_count)
                def _(n=self.n * beside_count):
                    planes = next(p for p in range(1, steps + 1) if n % p == 0 and n // p * HALO <= full)
                    ref = s.at[0:planes, 0 : n // planes * HALO]
                    wait(remote(ref, ref, self.sent, self.k, beside))

        def wait_recv(self):
            self.each_count(lambda copy: copy.wait_recv())

        def wait_send(self):
            self.each_count(lambda copy: copy.wait_send())

    class Edge(Tiles):
        def __init__(self, sent, k, first, last, halo_top, halo_bot, n=1):
            super().__init__(sent, k, n)
            self.first, self.last, self.top, self.bot = first, last, halo_top, halo_bot

        def start(self):
            @pl.when(has_up)
            def _():
                remote(self.first, self.bot, self.sent, self.k, up).start()

            @pl.when(has_dn)
            def _():
                remote(self.last, self.top, self.sent, self.k, dn).start()

    class Along:
        def __init__(self, k, src, dst):
            self.k, self.src, self.dst = first_plane + k, src, dst

        def start(self):
            @pl.when(has_after)
            def _():
                remote(self.src, self.dst, ALONG, self.k, {"tm": t + 1}).start()

        def wait_recv(self):
            @pl.when(has_before)
            def _():
                remote(self.src, self.dst, ALONG, self.k, {"tm": t - 1}).wait_recv()

        def wait_send(self):
            @pl.when(has_after)
            def _():
                remote(self.src, self.dst, ALONG, self.k, {"tm": t + 1}).wait_send()

    class Split:
        def __init__(self, k, ref):
            def part(k, rows_of):
                return Along(k, ref.at[half, rows_of], ref.at[0, rows_of])
            self.rim = Along(k, s.at[0, 0 : 2 * HALO], s.at[0, 0 : 2 * HALO])
            self.rest = part(k + 1, slice(2 * HALO, rows))
            self.parts = [part(k, top_in), part(k, bot_in), self.rest]

        def start(self):
            for part in self.parts:
                part.start()

    def within(turn, ref, sl):
        return Edge(
            SPACE, turn, ref.at[sl, top_in], ref.at[sl, bot_in], ref.at[sl, top], ref.at[sl, bot],
            sl.stop - sl.start)

    greeted = (
        (is_relay, {"tm": t - 2}), (from_relay, {"tm": t + 1}),
        (jnp.logical_and(odd_row, has_up), up), (jnp.logical_and(odd_row, has_dn), dn))
    for flag, dev in greeted:
        @pl.when(flag)
        def _(dev=dev):
            pl.semaphore_signal(barrier, inc=1, device_id=dev, device_id_type=MESH)

    last_guess = pltpu.make_async_copy(guess_hbm.at[steps - 1], g.at[steps, mid], send_sem.at[ALONG])
    last_guess.start()
    loads = [
        pltpu.make_async_copy(cond_hbm, c.at[mid], recv_sem.at[alone]),
        pltpu.make_async_copy(src_hbm, s.at[later, mid], send_sem.at[RELAY]),
        pltpu.make_async_copy(guess_hbm.at[0 : steps - 1], g.at[1:steps, mid], recv_sem.at[alone]),
    ]
    for load in loads:
        load.start()
    loaded = [loads[1], pltpu.make_async_copy(src_hbm, s.at[later, mid], recv_sem.at[alone])]
    start_g = pltpu.make_async_copy(start_hbm, g.at[0, mid], recv_sem.at[first_plane + T_GUESS])
    start_u = pltpu.make_async_copy(start_hbm, fu, recv_sem.at[first_plane + T_U3])

    @pl.when(jnp.logical_not(has_before))
    def _():
        start_g.start()
        start_u.start()
        s[0, mid] = jnp.zeros((rows, cols), jnp.float32)
        for ref in (c0, c1, c2):
            ref[0, mid] = jnp.zeros((rows, cols), jnp.float32)

    for flag, edge in ((has_up, top), (has_dn, bot)):
        @pl.when(jnp.logical_not(flag))
        def _(edge=edge):
            c[edge] = jnp.zeros((HALO, cols), jnp.float32)
            for ref in (g, s, c0, c1, c2):
                if ref is g or ref is s or ref is c2:
                    ref[:, edge] = jnp.zeros((ref.shape[0], HALO, cols), jnp.float32)
                else:
                    ref[0, edge] = jnp.zeros((HALO, cols), jnp.float32)

    greetings = count(has_after, by_relay, is_relay) + jnp.where(even_row, rows_beside, 0)

    @pl.when(greetings > 0)
    def _():
        pl.semaphore_wait(barrier, greetings)

    a_guess = Along(T_GUESS, g.at[steps, mid], g.at[0, mid])
    last_guess.wait()
    a_guess.start()
    for flag, dev in ((has_up, up), (has_dn, dn)):
        @pl.when(jnp.logical_and(even_row, flag))
        def _(dev=dev):
            pl.semaphore_signal(ready, inc=1, device_id=dev, device_id_type=MESH)

    @pl.when(jnp.logical_and(odd_row, rows_beside > 0))
    def _():
        pl.semaphore_wait(ready, rows_beside)

    def halo(group, n, hbm, ref):
        Edge(EARLY, group, hbm.at[n - 1, 0:HALO], hbm.at[n - 1, rows - HALO : rows], ref.at[n, top], ref.at[n, bot]).start()

    Edge(SPACE, 0, cond_hbm.at[0:HALO], cond_hbm.at[rows - HALO : rows], c.at[top], c.at[bot]).start()
    halo(0, steps, guess_hbm, g)
    for i in range(steps - 1):
        n = steps - i
        halo((i + 1) // 2, n - 1, guess_hbm, g)
        halo((i + 1) // 2, n, src_hbm, s)
    for load in loaded:
        load.wait()
    halo(half - 1, 1, src_hbm, s)

    lane = lax.broadcasted_iota(jnp.int32, (full, LANES), 1)
    is_first, is_last = lane == 0, lane == LANES - 1

    def at(j):
        return slice(j * LANES, (j + 1) * LANES)

    def each(low, high, body):
        def step(i, carry):
            body(i)
            return carry
        lax.fori_loop(low, high, step, 0)

    def stencil(get, put):
        zero = jnp.zeros((full, LANES), jnp.float32)
        before, now = zero, get(0)
        for j in range(chunks):
            after = get(j + 1) if j + 1 < chunks else zero
            left = pltpu.roll(jnp.where(is_last, before, now), 1, 1)
            right = pltpu.roll(jnp.where(is_first, after, now), LANES - 1, 1)
            rim = (left + right) + (pltpu.roll(now, 1, 0) + pltpu.roll(now, full - 1, 0))
            put(j, now, rim)
            before, now = now, after

    def first_sweep(field, n, has_prev=True):
        def put(j, now, rim):
            drive = s[n, :, at(j)]
            if has_prev:
                drive = drive + field[n - 1, :, at(j)]
            e[n, :, at(j)] = d[:, at(j)] * drive + w[:, at(j)] * rim - now
        stencil(lambda j: field[n, :, at(j)], put)

    def second_sweep(field, errs, n, dst, weight, damp, inner=False):
        def put(j, now, rim):
            gain = damp * (now + weight[:, at(j)] * rim)
            if inner:
                dst[n, mid, at(j)] = field[n, mid, at(j)] + gain[mid]
            elif field is None:
                dst[n, :, at(j)] = gain
            else:
                dst[n, :, at(j)] = field[n, :, at(j)] + gain
        stencil(lambda j: errs[n, :, at(j)], put)

    def restrict(m):
        a, b = 2 * m - 1, 2 * m

        def put(j, now, rim):
            cc = c[:, at(j)]
            drive = (s[a, :, at(j)] + s[b, :, at(j)]) + (u1[a - 1, :, at(j)] + u1[a, :, at(j)])
            er[m, :, at(j)] = dk[:, at(j)] * (drive - now + cc * (rim - 4.0 * now))
        stencil(lambda j: u1[a, :, at(j)] + u1[b, :, at(j)], put)

    def coarse_defect(field, m):
        def put(j, now, rim):
            ec[m, :, at(j)] = er[m, :, at(j)] + dk[:, at(j)] * field[m - 1, :, at(j)] + wk[:, at(j)] * rim - now
        stencil(lambda j: field[m, :, at(j)], put)

    def sweep_one(low, high):
        each(low, high, lambda m: coarse_defect(c0, m))
        each(low, high, lambda m: second_sweep(c0, ec, m, c1, wk, damping))

    def sweep_two(low, high):
        each(low, high, lambda m: coarse_defect(c1, m))
        each(low, high, lambda m: second_sweep(c1, ec, m, c2, wk, damping, inner=True))

    def prolong(m):
        for j in range(chunks):
            u2[2 * m, :, at(j)] = u1[2 * m, :, at(j)] + c2[m, :, at(j)]
            u2[2 * m - 1, :, at(j)] = u1[2 * m - 1, :, at(j)] + 0.5 * (c2[m - 1, :, at(j)] + c2[m, :, at(j)])

    def last_residual(n, has_prev=True):
        def put(j, now, rim):
            flow = c[:, at(j)] * (rim - 4.0 * now) - now
            drive = s[n, mid, at(j)]
            if has_prev:
                drive = drive + u3[n - 1, mid, at(j)]
            rbuf[n - 1, :, at(j)] = flow[mid] + drive
        stencil(lambda j: u3[n, :, at(j)], put)

    for j in range(chunks):
        qbuf[:, at(j)] = s[steps, mid, at(j)] + g[steps - 1, mid, at(j)]
    a_q = Along(T_Q, qbuf, s.at[0, mid])
    a_e0 = Along(T_E0, c0.at[half, mid], c0.at[0, mid])
    a_e1 = Split(T_E1_RIM, c1)
    a_e2 = Split(T_E2_RIM, c2)
    kept = rows - RELAYED
    u3_kept = Along(T_KEPT, u3.at[steps, HALO : HALO + kept], fu.at[0:kept])
    u3_rest = Along(T_U3, u3.at[steps, HALO + kept : HALO + rows], fu.at[kept:rows])

    def give(sent, k, src, dst, step, row_step=0):
        dev = {"tm": t + step, "space": z + row_step}
        return remote(src, dst, sent, first_plane + k, dev)

    def start_u3():
        u3_kept.start()

        @pl.when(jnp.logical_not(jnp.logical_or(by_relay, handing)))
        def _():
            u3_rest.start()

        @pl.when(by_relay)
        def _():
            give(ALONG, T_RELAY, u3_rest.src, relay, 2).start()

        @pl.when(by_hand)
        def _():
            give(ALONG, T_RELAY, u3_rest.src, relay, 0, 1).start()

    def passed_on(act):
        for flag, source, target in ((is_relay, (-2, 0), (-1, 0)), (is_hand, (0, -1), (1, -1))):
            @pl.when(flag)
            def _(source=source, target=target):
                act(source, target)

    def forward(source, target):
        give(RELAY, T_RELAY, relay, relay, *source).wait_recv()
        give(RELAY, T_U3, relay, u3_rest.dst, *target).start()

        @pl.when(handing)
        def _():
            u3_rest.start()

    def forwarded(source, target):
        give(RELAY, T_U3, relay, u3_rest.dst, *target).wait_send()

    def coefficients(part):
        for j in range(chunks):
            cc = c[part, at(j)]
            dd = 1.0 / (1.0 + 4.0 * cc)
            dd2 = 1.0 / (1.0 + 8.0 * cc)
            d[part, at(j)], w[part, at(j)] = dd, cc * dd
            dk[part, at(j)], wk[part, at(j)] = dd2, 2.0 * cc * dd2

    coefficients(mid)
    a_q.start()
    Tiles(EARLY, 0, 4).wait_recv()
    coefficients(top)
    coefficients(bot)

    def local_step(i):
        n = steps - i
        odd = lax.rem(i, 2) == 1

        @pl.when(jnp.logical_and(odd, i < steps - 3))
        def _():
            Tiles(EARLY, (i + 1) // 2, 4).wait_recv()

        @pl.when(i == steps - 3)
        def _():
            Tiles(EARLY, half - 1, 5).wait_recv()

        @pl.when(i == 3)
        def _():
            a_e0.start()
        first_sweep(g, n)
        second_sweep(g, e, n, u1, w, damping)

        @pl.when(jnp.logical_and(lax.rem(i, 2) == 0, i > 0))
        def _():
            m = half + 1 - i // 2
            restrict(m)
            second_sweep(None, er, m, c0, wk, damping)

    each(0, steps - 1, local_step)

    @pl.when(jnp.logical_not(has_before))
    def _():
        start_g.wait()
        start_u.wait()
    a_guess.wait_recv()
    f_guess = within(alone, g, slice(0, 1))
    f_guess.start()
    sweep_one(3, half + 1)
    each(4, half + 1, lambda m: coarse_defect(c1, m))
    a_e1.start()
    each(4, half + 1, lambda m: second_sweep(c1, ec, m, c2, wk, damping, inner=True))
    f_guess.wait_recv()
    each(1, 2, lambda n: first_sweep(g, n))
    a_e2.start()
    each(1, 2, lambda n: second_sweep(g, e, n, u1, w, damping))
    a_q.wait_recv()
    f_q = within(0, s, slice(0, 1))
    f_q.start()
    f_q.wait_recv()
    each(0, 1, lambda n: first_sweep(g, n, has_prev=False))
    damp0 = jnp.where(has_before, damping, 0.0).astype(jnp.float32)
    each(0, 1, lambda n: second_sweep(g, e, n, u1, w, damp0))
    each(1, 2, restrict)
    each(1, 2, lambda m: second_sweep(None, er, m, c0, wk, damping))
    sweep_one(2, 3)
    sweep_two(3, 4)
    x_late = within(1, c2, slice(3, half + 1))
    x_late.start()
    a_e0.wait_recv()
    f_e0 = within(2, c0, slice(0, 1))
    f_e0.start()
    x_late.wait_recv()
    each(half, half + 1, prolong)
    each(steps, steps + 1, lambda n: first_sweep(u2, n))
    each(steps, steps + 1, lambda n: second_sweep(u2, e, n, u3, w, damping))

    a_e1.rim.wait_recv()
    f_e1 = within(3, c1, slice(0, 1))
    f_e1.start()
    f_e0.wait_recv()
    each(1, 2, lambda m: coarse_defect(c0, m))
    start_u3()
    each(1, 2, lambda m: second_sweep(c0, ec, m, c1, wk, damping))
    sweep_two(2, 3)
    x_mid = within(0, c2, slice(2, 3))
    x_mid.start()
    for j in range(chunks):
        u2[steps - 2, :, at(j)] = u1[steps - 2, :, at(j)] + c2[half - 1, :, at(j)]
    each(steps - 1, steps, lambda n: first_sweep(u2, n))
    each(steps - 1, steps, lambda n: second_sweep(u2, e, n, u3, w, damping))
    each(steps, steps + 1, last_residual)
    a_e1.rest.wait_recv()
    f_e1.wait_recv()
    sweep_two(1, 2)
    x_early = within(1, c2, slice(1, 2))
    x_early.start()
    x_mid.wait_recv()
    each(3, half, prolong)
    for j in range(chunks):
        u2[4, :, at(j)] = u1[4, :, at(j)] + c2[2, :, at(j)]
    each(5, steps - 1, lambda n: first_sweep(u2, n))
    each(5, steps - 1, lambda n: second_sweep(u2, e, n, u3, w, damping))
    passed_on(forward)
    a_e2.rim.wait_recv()
    f_e2 = within(2, c2, slice(0, 1))
    f_e2.start()
    each(6, steps, last_residual)
    x_early.wait_recv()
    for j in range(chunks):
        u2[2, :, at(j)] = u1[2, :, at(j)] + c2[1, :, at(j)]
        u2[3, :, at(j)] = u1[3, :, at(j)] + 0.5 * (c2[1, :, at(j)] + c2[2, :, at(j)])
    each(3, 5, lambda n: first_sweep(u2, n))
    each(3, 5, lambda n: second_sweep(u2, e, n, u3, w, damping))
    each(4, 6, last_residual)
    a_e2.rest.wait_recv()
    f_e2.wait_recv()
    for j in range(chunks):
        u2[0, :, at(j)] = u1[0, :, at(j)] + c2[0, :, at(j)]
        u2[1, :, at(j)] = u1[1, :, at(j)] + 0.5 * (c2[0, :, at(j)] + c2[1, :, at(j)])
    each(1, 3, lambda n: first_sweep(u2, n))
    each(1, 3, lambda n: second_sweep(u2, e, n, u3, w, damping))
    each(2, 4, last_residual)
    each(1, 2, lambda n: last_residual(n, has_prev=False))
    @pl.when(jnp.logical_not(has_before))
    def _():
        rbuf[0] = rbuf[0] + fu[...]
    Tiles(EARLY, 0, 2 * steps).wait_send()
    Tiles(SPACE, 0, half + 6).wait_send()
    Along(T_U3, s.at[0:PLANES, mid], s.at[0:PLANES, mid]).wait_send()

    passed_on(forwarded)

    @pl.when(has_before)
    def _():
        for part, lines in ((u3_kept, slice(0, kept)), (u3_rest, slice(kept, rows))):
            part.wait_recv()
            rbuf[0, lines] = rbuf[0, lines] + fu[lines]


def store(u3, rbuf, u_out, r_out, sem):
    steps, rows, _ = u_out.shape
    copies = [
        pltpu.make_async_copy(u3.at[1 : steps + 1, HALO : HALO + rows], u_out, sem.at[0]),
        pltpu.make_async_copy(rbuf, r_out, sem.at[1]),
    ]
    for copy in copies:
        copy.start()
    for copy in copies:
        copy.wait()


def solution(mesh):
    tms, spaces = mesh.shape["tm"], mesh.shape["space"]

    def shards(source, guess, start_state, conduct):
        steps, rows, cols = source.shape
        full, half = rows + 2 * HALO, steps // 2

        def buf(*lead):
            return pltpu.VMEM(lead + (full, cols), jnp.float32)

        fields = pl.pallas_call(
            functools.partial(kernel, tms, spaces),
            out_shape=(buf(steps + 1), pltpu.VMEM(source.shape, jnp.float32)),
            in_specs=[pl.BlockSpec(memory_space=pltpu.HBM)] * 4,
            out_specs=[pl.BlockSpec(memory_space=pltpu.VMEM)] * 2,
            scratch_shapes=[
                buf(steps + 1), buf(steps + 1), buf(), buf(), buf(), buf(), buf(),
                buf(steps + 1), buf(steps + 1), buf(half + 1), buf(half + 1),
                buf(half + 1), buf(half + 1), buf(half + 1), buf(steps + 1),
                pltpu.VMEM((rows, cols), jnp.float32),
                pltpu.VMEM((rows, cols), jnp.float32),
                pltpu.VMEM((RELAYED, cols), jnp.float32),
                pltpu.SemaphoreType.DMA((4,)),
                pltpu.SemaphoreType.DMA((half + 1 + PARTS,)),
                pltpu.SemaphoreType.REGULAR,
            ],
            compiler_params=pltpu.CompilerParams(
                collective_id=0, has_side_effects=True, vmem_limit_bytes=59 * 1024 * 1024),
        )(source, guess, start_state, conduct)
        return pl.pallas_call(
            store,
            out_shape=(jax.ShapeDtypeStruct(source.shape, jnp.float32),) * 2,
            in_specs=[pl.BlockSpec(memory_space=pltpu.VMEM)] * 2,
            out_specs=[pl.BlockSpec(memory_space=pl.ANY)] * 2,
            scratch_shapes=[pltpu.SemaphoreType.DMA((2,))],
            compiler_params=pltpu.CompilerParams(vmem_limit_bytes=8 * 1024 * 1024),
        )(*fields)

    return jax.shard_map(
        shards,
        mesh=mesh,
        in_specs=(P("tm", "space", None), P("tm", "space", None), P("space", None), P("space", None)),
        out_specs=(P("tm", "space", None), P("tm", "space", None)),
        check_vma=False,
    )
```

```python
import functools

import jax
import jax.numpy as jnp
from jax import lax
from jax.experimental import pallas as pl
from jax.experimental.pallas import tpu as pltpu
from jax.sharding import PartitionSpec as P

damping = 0.8
MESH = pl.DeviceIdType.MESH
HALO = 8
LANES = 128

EARLY, SPACE, ALONG, RELAY = range(4)
T_GUESS, T_Q, T_E0, T_E1_RIM, T_E1, T_E2_RIM, T_E2, T_KEPT, T_U3, T_RELAY = range(10)
PLANES, PARTS = 6, 10
RELAYED = 4 * HALO


def kernel(
    tms, spaces, src_hbm, guess_hbm, start_hbm, cond_hbm, u3, rbuf,
    g, s, c, d, w, dk, wk, e, u1, er, ec, c0, c1, c2, u2, qbuf, fu,
    relay, send_sem, recv_sem, ready,
):
    t = lax.axis_index("tm")
    z = lax.axis_index("space")
    has_up, has_dn = z > 0, z < spaces - 1
    has_before, has_after = t > 0, t < tms - 1
    barrier = pltpu.get_barrier_semaphore()

    @pl.when(has_before)
    def _():
        pl.semaphore_signal(barrier, inc=1, device_id={"tm": t - 1}, device_id_type=MESH)

    by_relay = jnp.logical_and(lax.rem(t, 2) == 1, t + 2 < tms)
    is_relay = jnp.logical_and(lax.rem(t, 2) == 1, t > 2)
    from_relay = jnp.logical_and(lax.rem(t, 2) == 0, jnp.logical_and(t > 0, t + 1 < tms))
    odd_row = lax.rem(z, 2) == 1
    even_row = jnp.logical_not(odd_row)
    paired = jnp.logical_or(lax.rem(z, 2) == 1, has_dn)
    handing = jnp.logical_and(jnp.logical_and(lax.rem(t, 2) == 0, has_after), paired)
    by_hand = jnp.logical_and(handing, jnp.logical_and(even_row, has_dn))
    is_hand = jnp.logical_and(handing, odd_row)

    def count(*flags):
        return sum(jnp.where(flag, 1, 0) for flag in flags)
    steps, rows, cols = src_hbm.shape
    half = steps // 2
    full = rows + 2 * HALO
    mid = slice(HALO, HALO + rows)
    top, bot = slice(0, HALO), slice(HALO + rows, full)
    top_in, bot_in = slice(HALO, 2 * HALO), slice(rows, HALO + rows)
    chunks = cols // LANES
    later = slice(1, steps + 1)

    def remote(src, dst, sent, k, dev):
        return pltpu.make_async_remote_copy(
            src_ref=src, dst_ref=dst, send_sem=send_sem.at[sent], recv_sem=recv_sem.at[k],
            device_id=dev, device_id_type=MESH)

    up, dn = {"space": z - 1}, {"space": z + 1}
    alone = half
    first_plane = half + 1
    rows_beside = count(has_up, has_dn)
    beside = {"space": jnp.where(has_up, z - 1, z + 1)}

    class Tiles:
        def __init__(self, sent, k, n):
            self.sent, self.k, self.n = sent, k, n

        def each_count(self, wait):
            for beside_count in (1, 2):
                @pl.when(rows_beside == beside_count)
                def _(n=self.n * beside_count):
                    planes = next(p for p in range(1, steps + 1) if n % p == 0 and n // p * HALO <= full)
                    ref = s.at[0:planes, 0 : n // planes * HALO]
                    wait(remote(ref, ref, self.sent, self.k, beside))

        def wait_recv(self):
            self.each_count(lambda copy: copy.wait_recv())

        def wait_send(self):
            self.each_count(lambda copy: copy.wait_send())

    class Edge(Tiles):
        def __init__(self, sent, k, first, last, halo_top, halo_bot, n=1):
            super().__init__(sent, k, n)
            self.first, self.last, self.top, self.bot = first, last, halo_top, halo_bot

        def start(self):
            @pl.when(has_up)
            def _():
                remote(self.first, self.bot, self.sent, self.k, up).start()

            @pl.when(has_dn)
            def _():
                remote(self.last, self.top, self.sent, self.k, dn).start()

    class Along:
        def __init__(self, k, src, dst):
            self.k, self.src, self.dst = first_plane + k, src, dst

        def start(self):
            @pl.when(has_after)
            def _():
                remote(self.src, self.dst, ALONG, self.k, {"tm": t + 1}).start()

        def wait_recv(self):
            @pl.when(has_before)
            def _():
                remote(self.src, self.dst, ALONG, self.k, {"tm": t - 1}).wait_recv()

        def wait_send(self):
            @pl.when(has_after)
            def _():
                remote(self.src, self.dst, ALONG, self.k, {"tm": t + 1}).wait_send()

    class Split:
        def __init__(self, k, ref):
            def part(k, rows_of):
                return Along(k, ref.at[half, rows_of], ref.at[0, rows_of])
            self.rim = Along(k, s.at[0, 0 : 2 * HALO], s.at[0, 0 : 2 * HALO])
            self.rest = part(k + 1, slice(2 * HALO, rows))
            self.parts = [part(k, top_in), part(k, bot_in), self.rest]

        def start(self):
            for part in self.parts:
                part.start()

    def within(turn, ref, sl):
        return Edge(
            SPACE, turn, ref.at[sl, top_in], ref.at[sl, bot_in], ref.at[sl, top], ref.at[sl, bot],
            sl.stop - sl.start)

    greeted = (
        (is_relay, {"tm": t - 2}), (from_relay, {"tm": t + 1}),
        (jnp.logical_and(odd_row, has_up), up), (jnp.logical_and(odd_row, has_dn), dn))
    for flag, dev in greeted:
        @pl.when(flag)
        def _(dev=dev):
            pl.semaphore_signal(barrier, inc=1, device_id=dev, device_id_type=MESH)

    last_guess = pltpu.make_async_copy(guess_hbm.at[steps - 1], g.at[steps, mid], send_sem.at[ALONG])
    last_guess.start()
    loads = [
        pltpu.make_async_copy(cond_hbm, c.at[mid], recv_sem.at[alone]),
        pltpu.make_async_copy(src_hbm, s.at[later, mid], send_sem.at[RELAY]),
        pltpu.make_async_copy(guess_hbm.at[0 : steps - 1], g.at[1:steps, mid], recv_sem.at[alone]),
    ]
    for load in loads:
        load.start()
    loaded = [loads[1], pltpu.make_async_copy(src_hbm, s.at[later, mid], recv_sem.at[alone])]
    start_g = pltpu.make_async_copy(start_hbm, g.at[0, mid], recv_sem.at[first_plane + T_GUESS])
    start_u = pltpu.make_async_copy(start_hbm, fu, recv_sem.at[first_plane + T_U3])

    @pl.when(jnp.logical_not(has_before))
    def _():
        start_g.start()
        start_u.start()
        s[0, mid] = jnp.zeros((rows, cols), jnp.float32)
        for ref in (c0, c1, c2):
            ref[0, mid] = jnp.zeros((rows, cols), jnp.float32)

    for flag, edge in ((has_up, top), (has_dn, bot)):
        @pl.when(jnp.logical_not(flag))
        def _(edge=edge):
            c[edge] = jnp.zeros((HALO, cols), jnp.float32)
            for ref in (g, s, c0, c1, c2):
                if ref is g or ref is s or ref is c2:
                    ref[:, edge] = jnp.zeros((ref.shape[0], HALO, cols), jnp.float32)
                else:
                    ref[0, edge] = jnp.zeros((HALO, cols), jnp.float32)

    greetings = count(has_after, by_relay, is_relay) + jnp.where(even_row, rows_beside, 0)

    @pl.when(greetings > 0)
    def _():
        pl.semaphore_wait(barrier, greetings)

    a_guess = Along(T_GUESS, g.at[steps, mid], g.at[0, mid])
    last_guess.wait()
    a_guess.start()
    for flag, dev in ((has_up, up), (has_dn, dn)):
        @pl.when(jnp.logical_and(even_row, flag))
        def _(dev=dev):
            pl.semaphore_signal(ready, inc=1, device_id=dev, device_id_type=MESH)

    @pl.when(jnp.logical_and(odd_row, rows_beside > 0))
    def _():
        pl.semaphore_wait(ready, rows_beside)

    def halo(group, n, hbm, ref):
        Edge(EARLY, group, hbm.at[n - 1, 0:HALO], hbm.at[n - 1, rows - HALO : rows], ref.at[n, top], ref.at[n, bot]).start()

    Edge(SPACE, 0, cond_hbm.at[0:HALO], cond_hbm.at[rows - HALO : rows], c.at[top], c.at[bot]).start()
    halo(0, steps, guess_hbm, g)
    for i in range(steps - 1):
        n = steps - i
        halo((i + 1) // 2, n - 1, guess_hbm, g)
        halo((i + 1) // 2, n, src_hbm, s)
    for load in loaded:
        load.wait()
    halo(half - 1, 1, src_hbm, s)

    lane = lax.broadcasted_iota(jnp.int32, (full, LANES), 1)
    is_first, is_last = lane == 0, lane == LANES - 1

    def at(j):
        return slice(j * LANES, (j + 1) * LANES)

    def each(low, high, body):
        def step(i, carry):
            body(i)
            return carry
        lax.fori_loop(low, high, step, 0)

    def stencil(get, put):
        zero = jnp.zeros((full, LANES), jnp.float32)
        before, now = zero, get(0)
        for j in range(chunks):
            after = get(j + 1) if j + 1 < chunks else zero
            left = pltpu.roll(jnp.where(is_last, before, now), 1, 1)
            right = pltpu.roll(jnp.where(is_first, after, now), LANES - 1, 1)
            rim = (left + right) + (pltpu.roll(now, 1, 0) + pltpu.roll(now, full - 1, 0))
            put(j, now, rim)
            before, now = now, after

    def first_sweep(field, n, has_prev=True):
        def put(j, now, rim):
            drive = s[n, :, at(j)]
            if has_prev:
                drive = drive + field[n - 1, :, at(j)]
            e[n, :, at(j)] = d[:, at(j)] * drive + w[:, at(j)] * rim - now
        stencil(lambda j: field[n, :, at(j)], put)

    def second_sweep(field, errs, n, dst, weight, damp, inner=False):
        def put(j, now, rim):
            gain = damp * (now + weight[:, at(j)] * rim)
            if inner:
                dst[n, mid, at(j)] = field[n, mid, at(j)] + gain[mid]
            elif field is None:
                dst[n, :, at(j)] = gain
            else:
                dst[n, :, at(j)] = field[n, :, at(j)] + gain
        stencil(lambda j: errs[n, :, at(j)], put)

    def restrict(m):
        a, b = 2 * m - 1, 2 * m

        def put(j, now, rim):
            cc = c[:, at(j)]
            drive = (s[a, :, at(j)] + s[b, :, at(j)]) + (u1[a - 1, :, at(j)] + u1[a, :, at(j)])
            er[m, :, at(j)] = dk[:, at(j)] * (drive - now + cc * (rim - 4.0 * now))
        stencil(lambda j: u1[a, :, at(j)] + u1[b, :, at(j)], put)

    def coarse_defect(field, m):
        def put(j, now, rim):
            ec[m, :, at(j)] = er[m, :, at(j)] + dk[:, at(j)] * field[m - 1, :, at(j)] + wk[:, at(j)] * rim - now
        stencil(lambda j: field[m, :, at(j)], put)

    def sweep_one(low, high):
        each(low, high, lambda m: coarse_defect(c0, m))
        each(low, high, lambda m: second_sweep(c0, ec, m, c1, wk, damping))

    def sweep_two(low, high):
        each(low, high, lambda m: coarse_defect(c1, m))
        each(low, high, lambda m: second_sweep(c1, ec, m, c2, wk, damping, inner=True))

    def prolong(m):
        for j in range(chunks):
            u2[2 * m, :, at(j)] = u1[2 * m, :, at(j)] + c2[m, :, at(j)]
            u2[2 * m - 1, :, at(j)] = u1[2 * m - 1, :, at(j)] + 0.5 * (c2[m - 1, :, at(j)] + c2[m, :, at(j)])

    def last_residual(n, has_prev=True):
        def put(j, now, rim):
            flow = c[:, at(j)] * (rim - 4.0 * now) - now
            drive = s[n, mid, at(j)]
            if has_prev:
                drive = drive + u3[n - 1, mid, at(j)]
            rbuf[n - 1, :, at(j)] = flow[mid] + drive
        stencil(lambda j: u3[n, :, at(j)], put)

    for j in range(chunks):
        qbuf[:, at(j)] = s[steps, mid, at(j)] + g[steps - 1, mid, at(j)]
    a_q = Along(T_Q, qbuf, s.at[0, mid])
    a_e0 = Along(T_E0, c0.at[half, mid], c0.at[0, mid])
    a_e1 = Split(T_E1_RIM, c1)
    a_e2 = Split(T_E2_RIM, c2)
    kept = rows - RELAYED
    u3_kept = Along(T_KEPT, u3.at[steps, HALO : HALO + kept], fu.at[0:kept])
    u3_rest = Along(T_U3, u3.at[steps, HALO + kept : HALO + rows], fu.at[kept:rows])

    def give(sent, k, src, dst, step, row_step=0):
        dev = {"tm": t + step, "space": z + row_step}
        return remote(src, dst, sent, first_plane + k, dev)

    def start_u3():
        u3_kept.start()

        @pl.when(jnp.logical_not(jnp.logical_or(by_relay, handing)))
        def _():
            u3_rest.start()

        @pl.when(by_relay)
        def _():
            give(ALONG, T_RELAY, u3_rest.src, relay, 2).start()

        @pl.when(by_hand)
        def _():
            give(ALONG, T_RELAY, u3_rest.src, relay, 0, 1).start()

    def passed_on(act):
        for flag, source, target in ((is_relay, (-2, 0), (-1, 0)), (is_hand, (0, -1), (1, -1))):
            @pl.when(flag)
            def _(source=source, target=target):
                act(source, target)

    def forward(source, target):
        give(RELAY, T_RELAY, relay, relay, *source).wait_recv()
        give(RELAY, T_U3, relay, u3_rest.dst, *target).start()

        @pl.when(handing)
        def _():
            u3_rest.start()

    def forwarded(source, target):
        give(RELAY, T_U3, relay, u3_rest.dst, *target).wait_send()

    def coefficients(part):
        for j in range(chunks):
            cc = c[part, at(j)]
            dd = 1.0 / (1.0 + 4.0 * cc)
            dd2 = 1.0 / (1.0 + 8.0 * cc)
            d[part, at(j)], w[part, at(j)] = dd, cc * dd
            dk[part, at(j)], wk[part, at(j)] = dd2, 2.0 * cc * dd2

    coefficients(mid)
    a_q.start()
    Tiles(EARLY, 0, 4).wait_recv()
    coefficients(top)
    coefficients(bot)

    def local_step(i):
        n = steps - i
        odd = lax.rem(i, 2) == 1

        @pl.when(jnp.logical_and(odd, i < steps - 3))
        def _():
            Tiles(EARLY, (i + 1) // 2, 4).wait_recv()

        @pl.when(i == steps - 3)
        def _():
            Tiles(EARLY, half - 1, 5).wait_recv()

        @pl.when(i == 3)
        def _():
            a_e0.start()
        first_sweep(g, n)
        second_sweep(g, e, n, u1, w, damping)

        @pl.when(jnp.logical_and(lax.rem(i, 2) == 0, i > 0))
        def _():
            m = half + 1 - i // 2
            restrict(m)
            second_sweep(None, er, m, c0, wk, damping)

    each(0, steps - 1, local_step)

    @pl.when(jnp.logical_not(has_before))
    def _():
        start_g.wait()
        start_u.wait()
    a_guess.wait_recv()
    f_guess = within(alone, g, slice(0, 1))
    f_guess.start()
    sweep_one(3, half + 1)
    each(4, half + 1, lambda m: coarse_defect(c1, m))
    a_e1.start()
    each(4, half + 1, lambda m: second_sweep(c1, ec, m, c2, wk, damping, inner=True))
    f_guess.wait_recv()
    each(1, 2, lambda n: first_sweep(g, n))
    a_e2.start()
    each(1, 2, lambda n: second_sweep(g, e, n, u1, w, damping))
    a_q.wait_recv()
    f_q = within(0, s, slice(0, 1))
    f_q.start()
    f_q.wait_recv()
    each(0, 1, lambda n: first_sweep(g, n, has_prev=False))
    damp0 = jnp.where(has_before, damping, 0.0).astype(jnp.float32)
    each(0, 1, lambda n: second_sweep(g, e, n, u1, w, damp0))
    each(1, 2, restrict)
    each(1, 2, lambda m: second_sweep(None, er, m, c0, wk, damping))
    sweep_one(2, 3)
    sweep_two(3, 4)
    x_late = within(1, c2, slice(3, half + 1))
    x_late.start()
    a_e0.wait_recv()
    f_e0 = within(2, c0, slice(0, 1))
    f_e0.start()
    x_late.wait_recv()
    each(half, half + 1, prolong)
    each(steps, steps + 1, lambda n: first_sweep(u2, n))
    each(steps, steps + 1, lambda n: second_sweep(u2, e, n, u3, w, damping))

    a_e1.rim.wait_recv()
    f_e1 = within(3, c1, slice(0, 1))
    f_e1.start()
    f_e0.wait_recv()
    each(1, 2, lambda m: coarse_defect(c0, m))
    start_u3()
    each(1, 2, lambda m: second_sweep(c0, ec, m, c1, wk, damping))
    sweep_two(2, 3)
    x_mid = within(0, c2, slice(2, 3))
    x_mid.start()
    for j in range(chunks):
        u2[steps - 2, :, at(j)] = u1[steps - 2, :, at(j)] + c2[half - 1, :, at(j)]
    each(steps - 1, steps, lambda n: first_sweep(u2, n))
    each(steps - 1, steps, lambda n: second_sweep(u2, e, n, u3, w, damping))
    each(steps, steps + 1, last_residual)
    a_e1.rest.wait_recv()
    f_e1.wait_recv()
    sweep_two(1, 2)
    x_early = within(1, c2, slice(1, 2))
    x_early.start()
    x_mid.wait_recv()
    each(3, half, prolong)
    for j in range(chunks):
        u2[4, :, at(j)] = u1[4, :, at(j)] + c2[2, :, at(j)]
    each(5, steps - 1, lambda n: first_sweep(u2, n))
    each(5, steps - 1, lambda n: second_sweep(u2, e, n, u3, w, damping))
    passed_on(forward)
    a_e2.rim.wait_recv()
    f_e2 = within(2, c2, slice(0, 1))
    f_e2.start()
    each(6, steps, last_residual)
    x_early.wait_recv()
    for j in range(chunks):
        u2[2, :, at(j)] = u1[2, :, at(j)] + c2[1, :, at(j)]
        u2[3, :, at(j)] = u1[3, :, at(j)] + 0.5 * (c2[1, :, at(j)] + c2[2, :, at(j)])
    each(3, 5, lambda n: first_sweep(u2, n))
    each(3, 5, lambda n: second_sweep(u2, e, n, u3, w, damping))
    each(4, 6, last_residual)
    a_e2.rest.wait_recv()
    f_e2.wait_recv()
    for j in range(chunks):
        u2[0, :, at(j)] = u1[0, :, at(j)] + c2[0, :, at(j)]
        u2[1, :, at(j)] = u1[1, :, at(j)] + 0.5 * (c2[0, :, at(j)] + c2[1, :, at(j)])
    each(1, 3, lambda n: first_sweep(u2, n))
    each(1, 3, lambda n: second_sweep(u2, e, n, u3, w, damping))
    each(2, 4, last_residual)
    each(1, 2, lambda n: last_residual(n, has_prev=False))
    @pl.when(jnp.logical_not(has_before))
    def _():
        rbuf[0] = rbuf[0] + fu[...]
    Tiles(EARLY, 0, 2 * steps).wait_send()
    Tiles(SPACE, 0, half + 6).wait_send()
    Along(T_U3, s.at[0:PLANES, mid], s.at[0:PLANES, mid]).wait_send()

    passed_on(forwarded)

    @pl.when(has_before)
    def _():
        for part, lines in ((u3_kept, slice(0, kept)), (u3_rest, slice(kept, rows))):
            part.wait_recv()
            rbuf[0, lines] = rbuf[0, lines] + fu[lines]


def store(u3, rbuf, u_out, r_out, sem):
    steps, rows, _ = u_out.shape
    copies = [
        pltpu.make_async_copy(u3.at[1 : steps + 1, HALO : HALO + rows], u_out, sem.at[0]),
        pltpu.make_async_copy(rbuf, r_out, sem.at[1]),
    ]
    for copy in copies:
        copy.start()
    for copy in copies:
        copy.wait()


def solution(mesh):
    tms, spaces = mesh.shape["tm"], mesh.shape["space"]

    def shards(source, guess, start_state, conduct):
        steps, rows, cols = source.shape
        full, half = rows + 2 * HALO, steps // 2

        def buf(*lead):
            return pltpu.VMEM(lead + (full, cols), jnp.float32)

        fields = pl.pallas_call(
            functools.partial(kernel, tms, spaces),
            out_shape=(buf(steps + 1), pltpu.VMEM(source.shape, jnp.float32)),
            in_specs=[pl.BlockSpec(memory_space=pltpu.HBM)] * 4,
            out_specs=[pl.BlockSpec(memory_space=pltpu.VMEM)] * 2,
            scratch_shapes=[
                buf(steps + 1), buf(steps + 1), buf(), buf(), buf(), buf(), buf(),
                buf(steps + 1), buf(steps + 1), buf(half + 1), buf(half + 1),
                buf(half + 1), buf(half + 1), buf(half + 1), buf(steps + 1),
                pltpu.VMEM((rows, cols), jnp.float32),
                pltpu.VMEM((rows, cols), jnp.float32),
                pltpu.VMEM((RELAYED, cols), jnp.float32),
                pltpu.SemaphoreType.DMA((4,)),
                pltpu.SemaphoreType.DMA((half + 1 + PARTS,)),
                pltpu.SemaphoreType.REGULAR,
            ],
            compiler_params=pltpu.CompilerParams(
                collective_id=0, has_side_effects=True, vmem_limit_bytes=59 * 1024 * 1024),
        )(source, guess, start_state, conduct)
        return pl.pallas_call(
            store,
            out_shape=(jax.ShapeDtypeStruct(source.shape, jnp.float32),) * 2,
            in_specs=[pl.BlockSpec(memory_space=pltpu.VMEM)] * 2,
            out_specs=[pl.BlockSpec(memory_space=pl.ANY)] * 2,
            scratch_shapes=[pltpu.SemaphoreType.DMA((2,))],
            compiler_params=pltpu.CompilerParams(vmem_limit_bytes=8 * 1024 * 1024),
        )(*fields)

    return jax.shard_map(
        shards,
        mesh=mesh,
        in_specs=(P("tm", "space", None), P("tm", "space", None), P("space", None), P("space", None)),
        out_specs=(P("tm", "space", None), P("tm", "space", None)),
        check_vma=False,
    )
```

```python
import functools

import jax
import jax.numpy as jnp
from jax import lax
from jax.experimental import pallas as pl
from jax.experimental.pallas import tpu as pltpu
from jax.sharding import PartitionSpec as P

damping = 0.8
MESH = pl.DeviceIdType.MESH
HALO = 8
LANES = 128

EARLY, SPACE, ALONG, RELAY = range(4)
T_GUESS, T_Q, T_E0, T_E1_RIM, T_E1, T_E2_RIM, T_E2, T_KEPT, T_U3, T_RELAY = range(10)
PLANES, PARTS = 6, 10
RELAYED = 5 * HALO


def kernel(
    tms, spaces, src_hbm, guess_hbm, start_hbm, cond_hbm, u3, rbuf,
    g, s, c, d, w, dk, wk, e, u1, er, ec, c0, c1, c2, u2, qbuf, fu,
    relay, send_sem, recv_sem, ready,
):
    t = lax.axis_index("tm")
    z = lax.axis_index("space")
    has_up, has_dn = z > 0, z < spaces - 1
    has_before, has_after = t > 0, t < tms - 1
    barrier = pltpu.get_barrier_semaphore()

    @pl.when(has_before)
    def _():
        pl.semaphore_signal(barrier, inc=1, device_id={"tm": t - 1}, device_id_type=MESH)

    by_relay = jnp.logical_and(lax.rem(t, 2) == 1, t + 2 < tms)
    is_relay = jnp.logical_and(lax.rem(t, 2) == 1, t > 2)
    from_relay = jnp.logical_and(lax.rem(t, 2) == 0, jnp.logical_and(t > 0, t + 1 < tms))
    odd_row = lax.rem(z, 2) == 1
    even_row = jnp.logical_not(odd_row)
    paired = jnp.logical_or(lax.rem(z, 2) == 1, has_dn)
    handing = jnp.logical_and(jnp.logical_and(lax.rem(t, 2) == 0, has_after), paired)
    by_hand = jnp.logical_and(handing, jnp.logical_and(even_row, has_dn))
    is_hand = jnp.logical_and(handing, odd_row)

    def count(*flags):
        return sum(jnp.where(flag, 1, 0) for flag in flags)
    steps, rows, cols = src_hbm.shape
    half = steps // 2
    full = rows + 2 * HALO
    mid = slice(HALO, HALO + rows)
    top, bot = slice(0, HALO), slice(HALO + rows, full)
    top_in, bot_in = slice(HALO, 2 * HALO), slice(rows, HALO + rows)
    chunks = cols // LANES
    later = slice(1, steps + 1)

    def remote(src, dst, sent, k, dev):
        return pltpu.make_async_remote_copy(
            src_ref=src, dst_ref=dst, send_sem=send_sem.at[sent], recv_sem=recv_sem.at[k],
            device_id=dev, device_id_type=MESH)

    up, dn = {"space": z - 1}, {"space": z + 1}
    alone = half
    first_plane = half + 1
    rows_beside = count(has_up, has_dn)
    beside = {"space": jnp.where(has_up, z - 1, z + 1)}

    class Tiles:
        def __init__(self, sent, k, n):
            self.sent, self.k, self.n = sent, k, n

        def each_count(self, wait):
            for beside_count in (1, 2):
                @pl.when(rows_beside == beside_count)
                def _(n=self.n * beside_count):
                    planes = next(p for p in range(1, steps + 1) if n % p == 0 and n // p * HALO <= full)
                    ref = s.at[0:planes, 0 : n // planes * HALO]
                    wait(remote(ref, ref, self.sent, self.k, beside))

        def wait_recv(self):
            self.each_count(lambda copy: copy.wait_recv())

        def wait_send(self):
            self.each_count(lambda copy: copy.wait_send())

    class Edge(Tiles):
        def __init__(self, sent, k, first, last, halo_top, halo_bot, n=1):
            super().__init__(sent, k, n)
            self.first, self.last, self.top, self.bot = first, last, halo_top, halo_bot

        def start(self):
            @pl.when(has_up)
            def _():
                remote(self.first, self.bot, self.sent, self.k, up).start()

            @pl.when(has_dn)
            def _():
                remote(self.last, self.top, self.sent, self.k, dn).start()

    class Along:
        def __init__(self, k, src, dst):
            self.k, self.src, self.dst = first_plane + k, src, dst

        def start(self):
            @pl.when(has_after)
            def _():
                remote(self.src, self.dst, ALONG, self.k, {"tm": t + 1}).start()

        def wait_recv(self):
            @pl.when(has_before)
            def _():
                remote(self.src, self.dst, ALONG, self.k, {"tm": t - 1}).wait_recv()

        def wait_send(self):
            @pl.when(has_after)
            def _():
                remote(self.src, self.dst, ALONG, self.k, {"tm": t + 1}).wait_send()

    class Split:
        def __init__(self, k, ref):
            def part(k, rows_of):
                return Along(k, ref.at[half, rows_of], ref.at[0, rows_of])
            self.rim = Along(k, s.at[0, 0 : 2 * HALO], s.at[0, 0 : 2 * HALO])
            self.rest = part(k + 1, slice(2 * HALO, rows))
            self.parts = [part(k, top_in), part(k, bot_in), self.rest]

        def start(self):
            for part in self.parts:
                part.start()

    def within(turn, ref, sl):
        return Edge(
            SPACE, turn, ref.at[sl, top_in], ref.at[sl, bot_in], ref.at[sl, top], ref.at[sl, bot],
            sl.stop - sl.start)

    greeted = (
        (is_relay, {"tm": t - 2}), (from_relay, {"tm": t + 1}),
        (jnp.logical_and(odd_row, has_up), up), (jnp.logical_and(odd_row, has_dn), dn))
    for flag, dev in greeted:
        @pl.when(flag)
        def _(dev=dev):
            pl.semaphore_signal(barrier, inc=1, device_id=dev, device_id_type=MESH)

    last_guess = pltpu.make_async_copy(guess_hbm.at[steps - 1], g.at[steps, mid], send_sem.at[ALONG])
    last_guess.start()
    loads = [
        pltpu.make_async_copy(cond_hbm, c.at[mid], recv_sem.at[alone]),
        pltpu.make_async_copy(src_hbm, s.at[later, mid], send_sem.at[RELAY]),
        pltpu.make_async_copy(guess_hbm.at[0 : steps - 1], g.at[1:steps, mid], recv_sem.at[alone]),
    ]
    for load in loads:
        load.start()
    loaded = [loads[1], pltpu.make_async_copy(src_hbm, s.at[later, mid], recv_sem.at[alone])]
    start_g = pltpu.make_async_copy(start_hbm, g.at[0, mid], recv_sem.at[first_plane + T_GUESS])
    start_u = pltpu.make_async_copy(start_hbm, fu, recv_sem.at[first_plane + T_U3])

    @pl.when(jnp.logical_not(has_before))
    def _():
        start_g.start()
        start_u.start()
        s[0, mid] = jnp.zeros((rows, cols), jnp.float32)
        for ref in (c0, c1, c2):
            ref[0, mid] = jnp.zeros((rows, cols), jnp.float32)

    for flag, edge in ((has_up, top), (has_dn, bot)):
        @pl.when(jnp.logical_not(flag))
        def _(edge=edge):
            c[edge] = jnp.zeros((HALO, cols), jnp.float32)
            for ref in (g, s, c0, c1, c2):
                if ref is g or ref is s or ref is c2:
                    ref[:, edge] = jnp.zeros((ref.shape[0], HALO, cols), jnp.float32)
                else:
                    ref[0, edge] = jnp.zeros((HALO, cols), jnp.float32)

    greetings = count(has_after, by_relay, is_relay) + jnp.where(even_row, rows_beside, 0)

    @pl.when(greetings > 0)
    def _():
        pl.semaphore_wait(barrier, greetings)

    a_guess = Along(T_GUESS, g.at[steps, mid], g.at[0, mid])
    last_guess.wait()
    a_guess.start()
    for flag, dev in ((has_up, up), (has_dn, dn)):
        @pl.when(jnp.logical_and(even_row, flag))
        def _(dev=dev):
            pl.semaphore_signal(ready, inc=1, device_id=dev, device_id_type=MESH)

    @pl.when(jnp.logical_and(odd_row, rows_beside > 0))
    def _():
        pl.semaphore_wait(ready, rows_beside)

    def halo(group, n, hbm, ref):
        Edge(EARLY, group, hbm.at[n - 1, 0:HALO], hbm.at[n - 1, rows - HALO : rows], ref.at[n, top], ref.at[n, bot]).start()

    Edge(SPACE, 0, cond_hbm.at[0:HALO], cond_hbm.at[rows - HALO : rows], c.at[top], c.at[bot]).start()
    halo(0, steps, guess_hbm, g)
    for i in range(steps - 1):
        n = steps - i
        halo((i + 1) // 2, n - 1, guess_hbm, g)
        halo((i + 1) // 2, n, src_hbm, s)
    for load in loaded:
        load.wait()
    halo(half - 1, 1, src_hbm, s)

    lane = lax.broadcasted_iota(jnp.int32, (full, LANES), 1)
    is_first, is_last = lane == 0, lane == LANES - 1

    def at(j):
        return slice(j * LANES, (j + 1) * LANES)

    def each(low, high, body):
        def step(i, carry):
            body(i)
            return carry
        lax.fori_loop(low, high, step, 0)

    def stencil(get, put):
        zero = jnp.zeros((full, LANES), jnp.float32)
        before, now = zero, get(0)
        for j in range(chunks):
            after = get(j + 1) if j + 1 < chunks else zero
            left = pltpu.roll(jnp.where(is_last, before, now), 1, 1)
            right = pltpu.roll(jnp.where(is_first, after, now), LANES - 1, 1)
            rim = (left + right) + (pltpu.roll(now, 1, 0) + pltpu.roll(now, full - 1, 0))
            put(j, now, rim)
            before, now = now, after

    def first_sweep(field, n, has_prev=True):
        def put(j, now, rim):
            drive = s[n, :, at(j)]
            if has_prev:
                drive = drive + field[n - 1, :, at(j)]
            e[n, :, at(j)] = d[:, at(j)] * drive + w[:, at(j)] * rim - now
        stencil(lambda j: field[n, :, at(j)], put)

    def second_sweep(field, errs, n, dst, weight, damp, inner=False):
        def put(j, now, rim):
            gain = damp * (now + weight[:, at(j)] * rim)
            if inner:
                dst[n, mid, at(j)] = field[n, mid, at(j)] + gain[mid]
            elif field is None:
                dst[n, :, at(j)] = gain
            else:
                dst[n, :, at(j)] = field[n, :, at(j)] + gain
        stencil(lambda j: errs[n, :, at(j)], put)

    def restrict(m):
        a, b = 2 * m - 1, 2 * m

        def put(j, now, rim):
            cc = c[:, at(j)]
            drive = (s[a, :, at(j)] + s[b, :, at(j)]) + (u1[a - 1, :, at(j)] + u1[a, :, at(j)])
            er[m, :, at(j)] = dk[:, at(j)] * (drive - now + cc * (rim - 4.0 * now))
        stencil(lambda j: u1[a, :, at(j)] + u1[b, :, at(j)], put)

    def coarse_defect(field, m):
        def put(j, now, rim):
            ec[m, :, at(j)] = er[m, :, at(j)] + dk[:, at(j)] * field[m - 1, :, at(j)] + wk[:, at(j)] * rim - now
        stencil(lambda j: field[m, :, at(j)], put)

    def sweep_one(low, high):
        each(low, high, lambda m: coarse_defect(c0, m))
        each(low, high, lambda m: second_sweep(c0, ec, m, c1, wk, damping))

    def sweep_two(low, high):
        each(low, high, lambda m: coarse_defect(c1, m))
        each(low, high, lambda m: second_sweep(c1, ec, m, c2, wk, damping, inner=True))

    def prolong(m):
        for j in range(chunks):
            u2[2 * m, :, at(j)] = u1[2 * m, :, at(j)] + c2[m, :, at(j)]
            u2[2 * m - 1, :, at(j)] = u1[2 * m - 1, :, at(j)] + 0.5 * (c2[m - 1, :, at(j)] + c2[m, :, at(j)])

    def last_residual(n, has_prev=True):
        def put(j, now, rim):
            flow = c[:, at(j)] * (rim - 4.0 * now) - now
            drive = s[n, mid, at(j)]
            if has_prev:
                drive = drive + u3[n - 1, mid, at(j)]
            rbuf[n - 1, :, at(j)] = flow[mid] + drive
        stencil(lambda j: u3[n, :, at(j)], put)

    for j in range(chunks):
        qbuf[:, at(j)] = s[steps, mid, at(j)] + g[steps - 1, mid, at(j)]
    a_q = Along(T_Q, qbuf, s.at[0, mid])
    a_e0 = Along(T_E0, c0.at[half, mid], c0.at[0, mid])
    a_e1 = Split(T_E1_RIM, c1)
    a_e2 = Split(T_E2_RIM, c2)
    kept = rows - RELAYED
    u3_kept = Along(T_KEPT, u3.at[steps, HALO : HALO + kept], fu.at[0:kept])
    u3_rest = Along(T_U3, u3.at[steps, HALO + kept : HALO + rows], fu.at[kept:rows])

    def give(sent, k, src, dst, step, row_step=0):
        dev = {"tm": t + step, "space": z + row_step}
        return remote(src, dst, sent, first_plane + k, dev)

    def start_u3():
        u3_kept.start()

        @pl.when(jnp.logical_not(jnp.logical_or(by_relay, handing)))
        def _():
            u3_rest.start()

        @pl.when(by_relay)
        def _():
            give(ALONG, T_RELAY, u3_rest.src, relay, 2).start()

        @pl.when(by_hand)
        def _():
            give(ALONG, T_RELAY, u3_rest.src, relay, 0, 1).start()

    def passed_on(act):
        for flag, source, target in ((is_relay, (-2, 0), (-1, 0)), (is_hand, (0, -1), (1, -1))):
            @pl.when(flag)
            def _(source=source, target=target):
                act(source, target)

    def forward(source, target):
        give(RELAY, T_RELAY, relay, relay, *source).wait_recv()
        give(RELAY, T_U3, relay, u3_rest.dst, *target).start()

        @pl.when(handing)
        def _():
            u3_rest.start()

    def forwarded(source, target):
        give(RELAY, T_U3, relay, u3_rest.dst, *target).wait_send()

    def coefficients(part):
        for j in range(chunks):
            cc = c[part, at(j)]
            dd = 1.0 / (1.0 + 4.0 * cc)
            dd2 = 1.0 / (1.0 + 8.0 * cc)
            d[part, at(j)], w[part, at(j)] = dd, cc * dd
            dk[part, at(j)], wk[part, at(j)] = dd2, 2.0 * cc * dd2

    coefficients(mid)
    a_q.start()
    Tiles(EARLY, 0, 4).wait_recv()
    coefficients(top)
    coefficients(bot)

    def local_step(i):
        n = steps - i
        odd = lax.rem(i, 2) == 1

        @pl.when(jnp.logical_and(odd, i < steps - 3))
        def _():
            Tiles(EARLY, (i + 1) // 2, 4).wait_recv()

        @pl.when(i == steps - 3)
        def _():
            Tiles(EARLY, half - 1, 5).wait_recv()

        @pl.when(i == 3)
        def _():
            a_e0.start()
        first_sweep(g, n)
        second_sweep(g, e, n, u1, w, damping)

        @pl.when(jnp.logical_and(lax.rem(i, 2) == 0, i > 0))
        def _():
            m = half + 1 - i // 2
            restrict(m)
            second_sweep(None, er, m, c0, wk, damping)

    each(0, steps - 1, local_step)

    @pl.when(jnp.logical_not(has_before))
    def _():
        start_g.wait()
        start_u.wait()
    a_guess.wait_recv()
    f_guess = within(alone, g, slice(0, 1))
    f_guess.start()
    sweep_one(3, half + 1)
    each(4, half + 1, lambda m: coarse_defect(c1, m))
    a_e1.start()
    each(4, half + 1, lambda m: second_sweep(c1, ec, m, c2, wk, damping, inner=True))
    f_guess.wait_recv()
    each(1, 2, lambda n: first_sweep(g, n))
    a_e2.start()
    each(1, 2, lambda n: second_sweep(g, e, n, u1, w, damping))
    a_q.wait_recv()
    f_q = within(0, s, slice(0, 1))
    f_q.start()
    f_q.wait_recv()
    each(0, 1, lambda n: first_sweep(g, n, has_prev=False))
    damp0 = jnp.where(has_before, damping, 0.0).astype(jnp.float32)
    each(0, 1, lambda n: second_sweep(g, e, n, u1, w, damp0))
    each(1, 2, restrict)
    each(1, 2, lambda m: second_sweep(None, er, m, c0, wk, damping))
    sweep_one(2, 3)
    sweep_two(3, 4)
    x_late = within(1, c2, slice(3, half + 1))
    x_late.start()
    a_e0.wait_recv()
    f_e0 = within(2, c0, slice(0, 1))
    f_e0.start()
    x_late.wait_recv()
    each(half, half + 1, prolong)
    each(steps, steps + 1, lambda n: first_sweep(u2, n))
    each(steps, steps + 1, lambda n: second_sweep(u2, e, n, u3, w, damping))

    a_e1.rim.wait_recv()
    f_e1 = within(3, c1, slice(0, 1))
    f_e1.start()
    f_e0.wait_recv()
    each(1, 2, lambda m: coarse_defect(c0, m))
    start_u3()
    each(1, 2, lambda m: second_sweep(c0, ec, m, c1, wk, damping))
    sweep_two(2, 3)
    x_mid = within(0, c2, slice(2, 3))
    x_mid.start()
    for j in range(chunks):
        u2[steps - 2, :, at(j)] = u1[steps - 2, :, at(j)] + c2[half - 1, :, at(j)]
    each(steps - 1, steps, lambda n: first_sweep(u2, n))
    each(steps - 1, steps, lambda n: second_sweep(u2, e, n, u3, w, damping))
    each(steps, steps + 1, last_residual)
    a_e1.rest.wait_recv()
    f_e1.wait_recv()
    sweep_two(1, 2)
    x_early = within(1, c2, slice(1, 2))
    x_early.start()
    x_mid.wait_recv()
    each(3, half, prolong)
    for j in range(chunks):
        u2[4, :, at(j)] = u1[4, :, at(j)] + c2[2, :, at(j)]
    each(5, steps - 1, lambda n: first_sweep(u2, n))
    each(5, steps - 1, lambda n: second_sweep(u2, e, n, u3, w, damping))
    passed_on(forward)
    a_e2.rim.wait_recv()
    f_e2 = within(2, c2, slice(0, 1))
    f_e2.start()
    each(6, steps, last_residual)
    x_early.wait_recv()
    for j in range(chunks):
        u2[2, :, at(j)] = u1[2, :, at(j)] + c2[1, :, at(j)]
        u2[3, :, at(j)] = u1[3, :, at(j)] + 0.5 * (c2[1, :, at(j)] + c2[2, :, at(j)])
    each(3, 5, lambda n: first_sweep(u2, n))
    each(3, 5, lambda n: second_sweep(u2, e, n, u3, w, damping))
    each(4, 6, last_residual)
    a_e2.rest.wait_recv()
    f_e2.wait_recv()
    for j in range(chunks):
        u2[0, :, at(j)] = u1[0, :, at(j)] + c2[0, :, at(j)]
        u2[1, :, at(j)] = u1[1, :, at(j)] + 0.5 * (c2[0, :, at(j)] + c2[1, :, at(j)])
    each(1, 3, lambda n: first_sweep(u2, n))
    each(1, 3, lambda n: second_sweep(u2, e, n, u3, w, damping))
    each(2, 4, last_residual)
    each(1, 2, lambda n: last_residual(n, has_prev=False))
    @pl.when(jnp.logical_not(has_before))
    def _():
        rbuf[0] = rbuf[0] + fu[...]
    Tiles(EARLY, 0, 2 * steps).wait_send()
    Tiles(SPACE, 0, half + 6).wait_send()
    Along(T_U3, s.at[0:PLANES, mid], s.at[0:PLANES, mid]).wait_send()

    passed_on(forwarded)

    @pl.when(has_before)
    def _():
        for part, lines in ((u3_kept, slice(0, kept)), (u3_rest, slice(kept, rows))):
            part.wait_recv()
            rbuf[0, lines] = rbuf[0, lines] + fu[lines]


def store(u3, rbuf, u_out, r_out, sem):
    steps, rows, _ = u_out.shape
    copies = [
        pltpu.make_async_copy(u3.at[1 : steps + 1, HALO : HALO + rows], u_out, sem.at[0]),
        pltpu.make_async_copy(rbuf, r_out, sem.at[1]),
    ]
    for copy in copies:
        copy.start()
    for copy in copies:
        copy.wait()


def solution(mesh):
    tms, spaces = mesh.shape["tm"], mesh.shape["space"]

    def shards(source, guess, start_state, conduct):
        steps, rows, cols = source.shape
        full, half = rows + 2 * HALO, steps // 2

        def buf(*lead):
            return pltpu.VMEM(lead + (full, cols), jnp.float32)

        fields = pl.pallas_call(
            functools.partial(kernel, tms, spaces),
            out_shape=(buf(steps + 1), pltpu.VMEM(source.shape, jnp.float32)),
            in_specs=[pl.BlockSpec(memory_space=pltpu.HBM)] * 4,
            out_specs=[pl.BlockSpec(memory_space=pltpu.VMEM)] * 2,
            scratch_shapes=[
                buf(steps + 1), buf(steps + 1), buf(), buf(), buf(), buf(), buf(),
                buf(steps + 1), buf(steps + 1), buf(half + 1), buf(half + 1),
                buf(half + 1), buf(half + 1), buf(half + 1), buf(steps + 1),
                pltpu.VMEM((rows, cols), jnp.float32),
                pltpu.VMEM((rows, cols), jnp.float32),
                pltpu.VMEM((RELAYED, cols), jnp.float32),
                pltpu.SemaphoreType.DMA((4,)),
                pltpu.SemaphoreType.DMA((half + 1 + PARTS,)),
                pltpu.SemaphoreType.REGULAR,
            ],
            compiler_params=pltpu.CompilerParams(
                collective_id=0, has_side_effects=True, vmem_limit_bytes=59 * 1024 * 1024),
        )(source, guess, start_state, conduct)
        return pl.pallas_call(
            store,
            out_shape=(jax.ShapeDtypeStruct(source.shape, jnp.float32),) * 2,
            in_specs=[pl.BlockSpec(memory_space=pltpu.VMEM)] * 2,
            out_specs=[pl.BlockSpec(memory_space=pl.ANY)] * 2,
            scratch_shapes=[pltpu.SemaphoreType.DMA((2,))],
            compiler_params=pltpu.CompilerParams(vmem_limit_bytes=8 * 1024 * 1024),
        )(*fields)

    return jax.shard_map(
        shards,
        mesh=mesh,
        in_specs=(P("tm", "space", None), P("tm", "space", None), P("space", None), P("space", None)),
        out_specs=(P("tm", "space", None), P("tm", "space", None)),
        check_vma=False,
    )
```
